128 devices in a mesh: fsdp: 128 (over z, y, x, core).
Axes of the slice: x: 4, y: 4, z: 4, core: 2. Of those that a mesh axis runs over, the one named last changes fastest.
Arguments:
- x_saved: bfloat16 [2, 128, 384, 1280], P(None, 'fsdp')
- grad_out: bfloat16 [128, 384, 1280], P('fsdp')
- x_next: bfloat16 [128, 384, 1280], P('fsdp')
- w_up: bfloat16 [2, 1280, 5120], replicated
- w_down: bfloat16 [2, 5120, 1280], replicated
- gacc_up: float32 [2, 1280, 5120], P(None, 'fsdp')
- gacc_down: float32 [2, 5120, 1280], P(None, 'fsdp')
- master_up: float32 [2, 1280, 5120], P(None, 'fsdp')
- master_down: float32 [2, 5120, 1280], P(None, 'fsdp')
- mom1_up: float32 [2, 1280, 5120], P(None, 'fsdp')
- mom1_down: float32 [2, 5120, 1280], P(None, 'fsdp')
- mom2_up: float32 [2, 1280, 5120], P(None, 'fsdp')
- mom2_down: float32 [2, 5120, 1280], P(None, 'fsdp')
Outputs:
- output 1: bfloat16 [128, 384, 1280], P('fsdp')
- output 2: float32 [2, 1280, 5120], P(None, 'fsdp')
- output 3: float32 [2, 5120, 1280], P(None, 'fsdp')
- output 4: float32 [2, 1280, 5120], P(None, 'fsdp')
- output 5: float32 [2, 5120, 1280], P(None, 'fsdp')
- output 6: float32 [2, 1280, 5120], P(None, 'fsdp')
- output 7: float32 [2, 5120, 1280], P(None, 'fsdp')
All inputs are finite; a program needn't handle non-finite values.
Results may differ from the reference program's by a relative error of at most 0.00841215.
Values are sent between devices in bfloat16 or wider.
A program may use at most 1 GiB of HBM per device.

```python
import math
import jax
import jax.numpy as jnp
from jax import lax

LAYERS = 2
ADAM_STEP = 3
MICRO_STEPS = 2
GROUP_DEVS = 128
GLOBAL_BATCH = 128
SEQ_LEN = 384
D_MODEL = 1280
D_FF = 5120

DEV_BATCH = GLOBAL_BATCH // GROUP_DEVS
LEARN_RATE = 0.001
BETA_ONE = 0.9
BETA_TWO = 0.95
ADAM_EPS = 1e-8
WEIGHT_DECAY = 0.1
CLIP_NORM = 0.1 * math.sqrt(2 * LAYERS * D_MODEL * D_FF)


def setup_inputs(seed: int = 0) -> dict:
    key_list = jax.random.split(jax.random.key(seed), 13)
    up_scale = D_MODEL ** -0.5
    down_scale = D_FF ** -0.5
    tok_shape = (GLOBAL_BATCH, SEQ_LEN, D_MODEL)
    up_shape = (LAYERS, D_MODEL, D_FF)
    down_shape = (LAYERS, D_FF, D_MODEL)
    master_up = jax.random.normal(key_list[3], up_shape, jnp.float32) * up_scale
    master_down = jax.random.normal(key_list[4], down_shape, jnp.float32) * down_scale
    w_up = master_up + 0.3 * up_scale * jax.random.normal(key_list[5], up_shape, jnp.float32)
    w_down = master_down + 0.3 * down_scale * jax.random.normal(key_list[6], down_shape, jnp.float32)
    grad_scale = (GLOBAL_BATCH * SEQ_LEN) ** -0.5
    return {
        "x_saved": jax.random.normal(key_list[0], (LAYERS,) + tok_shape, jnp.float32).astype(jnp.bfloat16),
        "grad_out": (grad_scale * jax.random.normal(key_list[1], tok_shape, jnp.float32)).astype(jnp.bfloat16),
        "x_next": jax.random.normal(key_list[2], tok_shape, jnp.float32).astype(jnp.bfloat16),
        "w_up": w_up.astype(jnp.bfloat16),
        "w_down": w_down.astype(jnp.bfloat16),
        "gacc_up": 0.3 * jax.random.normal(key_list[7], up_shape, jnp.float32),
        "gacc_down": 0.6 * jax.random.normal(key_list[8], down_shape, jnp.float32),
        "master_up": master_up,
        "master_down": master_down,
        "mom1_up": 0.01 * jax.random.normal(key_list[9], up_shape, jnp.float32),
        "mom1_down": 0.01 * jax.random.normal(key_list[10], down_shape, jnp.float32),
        "mom2_up": 0.0004 * (0.5 + jax.random.uniform(key_list[11], up_shape, jnp.float32)),
        "mom2_down": 0.0004 * (0.5 + jax.random.uniform(key_list[12], down_shape, jnp.float32)),
    }


def gelu_fn(pre_act):
    return jax.nn.gelu(pre_act, approximate=True)


def seq_backward(w_up, w_down, x_layers, grad_seq):
    grads_up = []
    grads_down = []
    grad_cur = grad_seq
    for layer_idx in range(LAYERS - 1, -1, -1):
        x_in = x_layers[layer_idx]
        pre_act = jnp.dot(x_in, w_up[layer_idx], preferred_element_type=jnp.float32)
        hidden_act, gelu_vjp = jax.vjp(gelu_fn, pre_act)
        d_act = jnp.dot(grad_cur, w_down[layer_idx].T, preferred_element_type=jnp.float32)
        d_pre = gelu_vjp(d_act)[0].astype(jnp.bfloat16)
        grads_down.append(jnp.dot(hidden_act.astype(jnp.bfloat16).T, grad_cur, preferred_element_type=jnp.float32))
        grads_up.append(jnp.dot(x_in.T, d_pre, preferred_element_type=jnp.float32))
        if layer_idx > 0:
            grad_cur = (grad_cur.astype(jnp.float32) + jnp.dot(d_pre, w_up[layer_idx].T, preferred_element_type=jnp.float32)).astype(jnp.bfloat16)
    return jnp.stack(grads_up[::-1]), jnp.stack(grads_down[::-1])


def device_partials(w_up, w_down, x_dev, grad_dev):
    def scan_body(acc_in, seq_idx):
        up_grad, down_grad = seq_backward(w_up, w_down, x_dev[:, seq_idx], grad_dev[seq_idx])
        return (acc_in[0] + up_grad, acc_in[1] + down_grad), None
    start_acc = (jnp.zeros((LAYERS, D_MODEL, D_FF), jnp.float32), jnp.zeros((LAYERS, D_FF, D_MODEL), jnp.float32))
    acc_pair, _ = lax.scan(scan_body, start_acc, jnp.arange(DEV_BATCH))
    return acc_pair[0].astype(jnp.bfloat16), acc_pair[1].astype(jnp.bfloat16)


def adamw_update(master_old, mom_one, mom_two, grad_clip):
    mom_one_new = BETA_ONE * mom_one + (1.0 - BETA_ONE) * grad_clip
    mom_two_new = BETA_TWO * mom_two + (1.0 - BETA_TWO) * grad_clip * grad_clip
    first_hat = mom_one_new / (1.0 - BETA_ONE ** ADAM_STEP)
    second_hat = mom_two_new / (1.0 - BETA_TWO ** ADAM_STEP)
    master_new = master_old - LEARN_RATE * (first_hat / (jnp.sqrt(second_hat) + ADAM_EPS) + WEIGHT_DECAY * master_old)
    return master_new, mom_one_new, mom_two_new


def seq_forward(w_up_new, w_down_new, x_seq):
    hidden_state = x_seq
    for layer_idx in range(LAYERS):
        pre_act = jnp.dot(hidden_state, w_up_new[layer_idx], preferred_element_type=jnp.float32)
        hidden_act = gelu_fn(pre_act).astype(jnp.bfloat16)
        hidden_state = (hidden_state.astype(jnp.float32) + jnp.dot(hidden_act, w_down_new[layer_idx], preferred_element_type=jnp.float32)).astype(jnp.bfloat16)
    return hidden_state


def reference(x_saved, grad_out, x_next, w_up, w_down, gacc_up, gacc_down, master_up, master_down, mom1_up, mom1_down, mom2_up, mom2_down):
    x_groups = x_saved.reshape(LAYERS, GROUP_DEVS, DEV_BATCH, SEQ_LEN, D_MODEL)
    grad_groups = grad_out.reshape(GROUP_DEVS, DEV_BATCH, SEQ_LEN, D_MODEL)

    def dev_body(acc_in, dev_idx):
        part_up, part_down = device_partials(w_up, w_down, x_groups[:, dev_idx], grad_groups[dev_idx])
        return (acc_in[0] + part_up.astype(jnp.float32), acc_in[1] + part_down.astype(jnp.float32)), None

    start_acc = (jnp.zeros((LAYERS, D_MODEL, D_FF), jnp.float32), jnp.zeros((LAYERS, D_FF, D_MODEL), jnp.float32))
    acc_pair, _ = lax.scan(dev_body, start_acc, jnp.arange(GROUP_DEVS))
    grad_up = (gacc_up + acc_pair[0]) / MICRO_STEPS
    grad_down = (gacc_down + acc_pair[1]) / MICRO_STEPS
    total_norm = jnp.sqrt(jnp.sum(grad_up * grad_up) + jnp.sum(grad_down * grad_down))
    clip_factor = jnp.minimum(1.0, CLIP_NORM / total_norm)
    new_up = adamw_update(master_up, mom1_up, mom2_up, grad_up * clip_factor)
    new_down = adamw_update(master_down, mom1_down, mom2_down, grad_down * clip_factor)
    w_up_new = new_up[0].astype(jnp.bfloat16)
    w_down_new = new_down[0].astype(jnp.bfloat16)
    x_out = lax.map(lambda x_seq: seq_forward(w_up_new, w_down_new, x_seq), x_next)
    return (x_out, new_up[0], new_down[0], new_up[1], new_down[1], new_up[2], new_down[2])
```

```python
import functools
import math

import jax
import jax.numpy as jnp
from jax import lax
from jax.experimental import pallas as pl
from jax.experimental.pallas import tpu as pltpu
from jax.sharding import PartitionSpec as P

LEARN_RATE = 0.001
BETA_ONE = 0.9
BETA_TWO = 0.95
ADAM_EPS = 1e-8
WEIGHT_DECAY = 0.1
ADAM_STEP = 3
MICRO_STEPS = 2

MESH = pl.DeviceIdType.MESH
BF16 = jnp.bfloat16
F32 = jnp.float32
VMEM_LIMIT = 67_000_000
LAYERS = 2
RING = 4
WIDTH = 1280
FF = 5120
UP_ROWS = 10
DOWN_ROWS = 40
BLOCK = 80
COLS = 640
PAIR_ROWS = 2 * BLOCK
ROWS = LAYERS * PAIR_ROWS
LANES = 128
OCTET = 8
CHUNK = 8
SEMS = pltpu.SemaphoreType.DMA

BATCH_CHUNKS = PAIR_ROWS // CHUNK
ORDERS = ((0, 1, 2), (1, 2, 0), (2, 0, 1))
N_FLOWS = 6
FLOWS = range(N_FLOWS)
TICKS = RING
STEPS = RING - 1
BATCH_LEN = [[TICKS if f // 2 == b else TICKS - 1 for f in FLOWS] for b in range(LAYERS)]
BATCH_START = [[sum(lens[:f]) for f in FLOWS] for lens in BATCH_LEN]
OWN_SLOTS = 3
UP_TILES = 8
TILES = 16


def up_base(layer):
    return (LAYERS - 1 - layer) * PAIR_ROWS


def down_base(layer):
    return up_base(layer) + BLOCK


def comm_params(collective_id):
    return pltpu.CompilerParams(collective_id=collective_id, has_side_effects=True, vmem_limit_bytes=VMEM_LIMIT)


def plain_params(dims):
    return pltpu.CompilerParams(dimension_semantics=("arbitrary",) * dims, vmem_limit_bytes=VMEM_LIMIT)


def in_vmem():
    return pl.BlockSpec(memory_space=pltpu.VMEM)


def in_hbm():
    return pl.BlockSpec(memory_space=pl.ANY)


def aligned(start, size):
    return pl.ds(pl.multiple_of(start, CHUNK), size)


def aligned_lanes(start, size):
    return pl.ds(pl.multiple_of(start, LANES), size)


def remote(src, dst, send, got, device):
    return pltpu.make_async_remote_copy(
        src_ref=src, dst_ref=dst, send_sem=send, recv_sem=got, device_id=(device,), device_id_type=MESH
    )

def flow_dims(flow):
    return ORDERS[flow // 2]


def flow_sign(flow):
    return 1 - 2 * (flow % 2)


def my_place():
    me = lax.axis_index("fsdp")
    core, chip = lax.rem(me, 2), lax.div(me, 2)
    line = lax.div(chip, RING)
    return core, (lax.div(line, RING), lax.rem(line, RING), lax.rem(chip, RING))


def device_at(pos, core):
    return ((pos[0] * RING + pos[1]) * RING + pos[2]) * 2 + core


def neighbor(pos, core, dim, sign):
    moved = list(pos)
    moved[dim] = lax.rem(pos[dim] + RING + sign, RING)
    return device_at(moved, core)


def all_neighbors(pos, core):
    return [neighbor(pos, core, dim, sign) for dim in range(3) for sign in (1, -1)]


def entry_barrier(peers):
    barrier = pltpu.get_barrier_semaphore()
    for peer in peers:
        pl.semaphore_signal(barrier, inc=1, device_id=(peer,), device_id_type=MESH)
    pl.semaphore_wait(barrier, len(peers))


def rounded_product(left, right):
    return lax.dot_general(left, right, (((0,), (0,)), ((), ())), preferred_element_type=F32).astype(BF16).astype(F32)


def reduce_kernel(
    s_last, x_own, d_own, a_own, g_own, out_ref, s_first, x_pair, d_pair, a_pair, g_pair,
    recv1, recv2, recv3, own, left, left_pair, right, right_pair, tile, own_sem, tile_in, tile_out, pair_send, pair_got, credit,
    send1, got1, send2, got2, send3, got3,
):
    core, pos = my_place()
    partner = device_at(pos, 1 - core)
    entry_barrier([partner] + all_neighbors(pos, core))
    target = [[neighbor(pos, core, dim, flow_sign(f)) for dim in flow_dims(f)] for f in FLOWS]
    source = [neighbor(pos, core, flow_dims(f)[0], -flow_sign(f)) for f in FLOWS]
    sums = (s_last, s_first)

    def seg(flow, phase, step):
        at = pos[flow_dims(flow)[phase]]
        return lax.rem(at + 2 * RING - flow_sign(flow) * (1 + step), RING)

    def s_slice(b, flow, j, chunk):
        index = [slice(None)] * 3
        index[flow_dims(flow)[0]] = j
        return sums[b].at[(*index, aligned(chunk * CHUNK, CHUNK), slice(None))]

    def part2(flow, ref, j):
        second, third = flow_dims(flow)[1:]
        return ref.at[j] if second < third else ref.at[:, j]

    def slot1(b, step):
        return step + b * 2 * ((step + 1) // 2)

    def land1(b, step, chunk):
        return recv1.at[slot1(b, step), chunk]

    def land2(b, step, chunk):
        return recv2.at[b, step, chunk]

    def land3(b, step, chunk):
        return recv3.at[b, step, chunk]

    lands, sends, gots = (land1, land2, land3), (send1, send2, send3), (got1, got2, got3)

    def copy(phase, b, flow, step, chunk, src):
        dst = lands[phase](b, step, chunk)
        return remote(dst if src is None else src, dst, sends[phase].at[b, step, chunk], gots[phase].at[b, step, chunk], target[flow][phase])

    def first_copy(phase, b, flow, chunk):
        j = seg(flow, phase, 0)
        if phase == 0:
            src = s_slice(b, flow, j, chunk)
        elif phase == 1:
            src = part2(flow, land1(b, STEPS - 1, chunk), j)
        else:
            src = recv2.at[b, STEPS - 1, chunk, j]
        return copy(phase, b, flow, 0, chunk, src)

    def next_copy(phase, b, flow, step, chunk):
        return copy(phase, b, flow, step + 1, chunk, lands[phase](b, step, chunk))

    def own_copy(b, flow, n):
        step, k = lax.div(n, TICKS), lax.rem(n, TICKS)
        slot = lax.rem(n, OWN_SLOTS)
        src = s_slice(b, flow, seg(flow, 0, step + 1), BATCH_START[b][flow] + k)
        return pltpu.make_async_copy(src, own.at[flow, slot], own_sem.at[flow, slot])

    def start_batch(b):
        for k in range(TICKS):
            for f in FLOWS:
                if k < BATCH_LEN[b][f]:
                    first_copy(0, b, f, BATCH_START[b][f] + k).start()
        for n in range(OWN_SLOTS - 1):
            for f in FLOWS:
                own_copy(b, f, n).start()

    def tick(phase, b, n):
        step, k = lax.div(n, TICKS), lax.rem(n, TICKS)

        def each(body):
            for f in FLOWS:
                if BATCH_LEN[b][f] == TICKS:
                    body(f, BATCH_START[b][f] + k)
                else:
                    pl.when(k < BATCH_LEN[b][f])(functools.partial(body, f, BATCH_START[b][f] + k))

        def add(f, chunk):
            copy(phase, b, f, step, chunk, None).wait_recv()
            landed = lands[phase](b, step, chunk)
            if phase == 0:
                own_copy(b, f, n).wait()
                landed[...] = landed[...] + own[f, lax.rem(n, OWN_SLOTS)]
            elif phase == 1:
                landed[...] = landed[...] + part2(f, land1(b, STEPS - 1, chunk), seg(f, 1, step + 1))[...]
            else:
                landed[...] = landed[...] + recv2[b, STEPS - 1, chunk, seg(f, 2, step + 1)]

        def pass_on(f, chunk):
            @pl.when(step < STEPS - 1)
            def _():
                next_copy(phase, b, f, step, chunk).start()

            @pl.when(step == STEPS - 1)
            def _():
                if phase < 2:
                    first_copy(phase + 1, b, f, chunk).start()
                else:
                    out_ref[aligned((b * BATCH_CHUNKS + chunk) * CHUNK, CHUNK), :] = recv3[b, STEPS - 1, chunk]

        if phase == 0:
            later = n + OWN_SLOTS - 1
            for f in FLOWS:
                @pl.when((later < STEPS * TICKS) & (lax.rem(later, TICKS) < BATCH_LEN[b][f]))
                def _():
                    own_copy(b, f, later).start()

        each(add)
        each(pass_on)

    def tile_reads(job, up):
        slot = lax.rem(job, 2)
        if up:
            rows = aligned_lanes(lax.div(job, RING) * COLS, COLS)
            cols = lax.rem(job, RING) * COLS
            reads = (x_own.at[:, rows], x_pair.at[:, rows], d_own.at[:, aligned_lanes(core * (FF // 2) + cols, COLS)], d_pair.at[:, aligned_lanes(cols, COLS)])
        else:
            rows = aligned_lanes((job - UP_TILES) * COLS, COLS)
            reads = (a_own.at[:, rows], a_pair.at[:, rows], g_own.at[:, aligned_lanes(core * COLS, COLS)], g_pair)
        return [
            pltpu.make_async_copy(src, dst.at[slot], tile_in.at[i, slot])
            for i, (src, dst) in enumerate(zip(reads, (left, left_pair, right, right_pair)))
        ]

    def start_reads(job):
        for up in (True, False):
            @pl.when((job < UP_TILES) if up else (job >= UP_TILES) & (job < TILES))
            def _():
                for read in tile_reads(job, up):
                    read.start()

    def tile_write(job, up):
        slot = lax.rem(job, 2)
        if up:
            dst = s_first.at[pl.ds(lax.div(job, RING) * 2, 2), :, lax.rem(job, RING), pl.ds(0, BLOCK)]
        else:
            i = job - UP_TILES
            dst = s_first.at[lax.div(i, 2), pl.ds(lax.rem(i, 2) * 2, 2), :, pl.ds(BLOCK, BLOCK)]
        return pltpu.make_async_copy(tile.at[slot], dst, tile_out.at[slot])

    def compute(job):
        slot = lax.rem(job, 2)
        start_reads(job + 1)
        for read in tile_reads(UP_TILES + slot, False):
            read.wait()

        @pl.when(job >= 2)
        def _():
            tile_write(UP_TILES + slot, False).wait()

        total = rounded_product(left[slot], right[slot]) + rounded_product(left_pair[slot], right_pair[slot])
        tile[slot] = total.reshape(tile.shape[1:])
        for up in (True, False):
            @pl.when((job < UP_TILES) if up else (job >= UP_TILES))
            def _():
                tile_write(job, up).start()

    start_batch(0)
    other = 1 - core
    gives = (x_own, d_own.at[:, aligned_lanes(other * (FF // 2), FF // 2)], a_own, g_own.at[:, aligned_lanes(other * COLS, COLS)])
    exchange = [
        remote(src, dst, pair_send.at[i], pair_got.at[i], partner)
        for i, (src, dst) in enumerate(zip(gives, (x_pair, d_pair, a_pair, g_pair)))
    ]
    for give in exchange:
        give.start()
    for give in exchange:
        give.wait_recv()
    start_reads(0)

    @pl.loop(0, 2 * TICKS)
    def _(n):
        tick(0, 0, n)

        @pl.loop(0, 2)
        def _(i):
            compute(2 * n + i)

    for slot in range(2):
        tile_write(UP_TILES + slot, False).wait()
    for f in FLOWS:
        for k in range(BATCH_LEN[0][f]):
            copy(0, 0, f, 1, BATCH_START[0][f] + k, None).wait_send()
        pl.semaphore_signal(credit.at[f], inc=1, device_id=(source[f],), device_id_type=MESH)
    for f in FLOWS:
        pl.semaphore_wait(credit.at[f], 1)
    for k in range(TICKS):
        for f in FLOWS:
            if k < BATCH_LEN[1][f]:
                first_copy(0, 1, f, BATCH_START[1][f] + k).start()

    @pl.loop(2 * TICKS, STEPS * TICKS)
    def _(n):
        tick(0, 0, n)

    for n in range(OWN_SLOTS - 1):
        for f in FLOWS:
            own_copy(1, f, n).start()

    @pl.loop(0, STEPS * TICKS)
    def _(n):
        tick(0, 1, n)
        tick(1, 0, n)

    @pl.loop(0, STEPS * TICKS)
    def _(n):
        tick(1, 1, n)
        tick(2, 0, n)

    @pl.loop(0, STEPS * TICKS)
    def _(n):
        tick(2, 1, n)

    for give in exchange:
        give.wait_send()
    for b in range(LAYERS):
        for f in FLOWS:
            @pl.loop(BATCH_START[b][f], BATCH_START[b][f] + BATCH_LEN[b][f])
            def _(chunk):
                for phase in range(3):
                    for step in range(STEPS):
                        if (phase, b, step) != (0, 0, 1):
                            copy(phase, b, f, step, chunk, None).wait_send()


def reduce_blocks(s_last, x_first, d_first, a_first, g_first):
    tokens = x_first.shape[0]

    def half(width):
        return jax.ShapeDtypeStruct((tokens, width), BF16)

    piece = pltpu.VMEM((2, tokens, COLS), BF16)
    sems = SEMS((LAYERS, STEPS, BATCH_CHUNKS))
    return pl.pallas_call(
        reduce_kernel,
        out_shape=[jax.ShapeDtypeStruct((ROWS, COLS), F32), jax.ShapeDtypeStruct(s_last.shape, F32), half(WIDTH), half(FF // 2), half(FF), half(COLS)],
        in_specs=[in_hbm()] * 5,
        out_specs=[in_vmem()] + [in_hbm()] * 5,
        scratch_shapes=[
            pltpu.VMEM((5, BATCH_CHUNKS, RING, RING, CHUNK, COLS), F32),
            pltpu.VMEM((LAYERS, STEPS, BATCH_CHUNKS, RING, CHUNK, COLS), F32),
            pltpu.VMEM((LAYERS, STEPS, BATCH_CHUNKS, CHUNK, COLS), F32),
            pltpu.VMEM((N_FLOWS, OWN_SLOTS, RING, RING, CHUNK, COLS), F32),
            piece, piece, piece, piece,
            pltpu.VMEM((2, 2, RING, BLOCK, COLS), F32),
            SEMS((N_FLOWS, OWN_SLOTS)), SEMS((4, 2)), SEMS((2,)), SEMS((4,)), SEMS((4,)), pltpu.SemaphoreType.REGULAR((N_FLOWS,)),
            sems, sems, sems, sems, sems, sems,
        ],
        compiler_params=comm_params(1),
        name="torus_reduce",
    )(s_last, x_first, d_first, a_first, g_first)[0]


GATHER_LEN = [BATCH_LEN[0][f] + BATCH_LEN[1][f] for f in FLOWS]
GATHER_START = [sum(GATHER_LEN[:f]) for f in FLOWS]


def gather_kernel(block_ref, all_ref, own_sem, send1, got1, send2, got2, send3, got3, pair_send, pair_got):
    core, pos = my_place()
    partner = device_at(pos, 1 - core)
    entry_barrier([partner] + all_neighbors(pos, core))
    target = [[neighbor(pos, core, dim, flow_sign(f)) for dim in flow_dims(f)] for f in FLOWS]

    def flow_rows(flow):
        return pl.ds(GATHER_START[flow] * CHUNK, GATHER_LEN[flow] * CHUNK)

    def back(flow, phase, steps):
        at = pos[flow_dims(flow)[phase]]
        return lax.rem(at + RING - flow_sign(flow) * steps, RING)

    def place(flow, first, second, third):
        index = [None] * 3
        for dim, at in zip(flow_dims(flow), (first, second, third)):
            index[dim] = at
        return all_ref.at[(core, *index, flow_rows(flow), slice(None))]

    def copy1(flow, step):
        ref = place(flow, back(flow, 0, step), back(flow, 1, 0), back(flow, 2, 0))
        if step == 0:
            return remote(block_ref.at[flow_rows(flow)], ref, send1.at[flow, step], got1.at[flow, step], target[flow][0])
        return remote(ref, ref, send1.at[flow, step], got1.at[flow, step], target[flow][0])

    def wait1(flow, step):
        ref = place(flow, back(flow, 0, step + 1), back(flow, 1, 0), back(flow, 2, 0))
        remote(ref, ref, send1.at[flow, step], got1.at[flow, step], target[flow][0]).wait_recv()

    def copy2(flow, step, u, off=0):
        ref = place(flow, back(flow, 0, u), back(flow, 1, step + off), back(flow, 2, 0))
        if step == 0 and u == 0 and off == 0:
            return remote(block_ref.at[flow_rows(flow)], ref, send2.at[flow, step, u], got2.at[flow, step, u], target[flow][1])
        return remote(ref, ref, send2.at[flow, step, u], got2.at[flow, step, u], target[flow][1])

    def copy3(flow, step, v, off=0):
        ref = place(flow, slice(None), back(flow, 1, v), back(flow, 2, step + off))
        return remote(ref, ref, send3.at[flow, step, v], got3.at[flow, step, v], target[flow][2])

    def pair_copy(flow, w, v):
        ref = place(flow, slice(None), back(flow, 1, v), back(flow, 2, w))
        return remote(ref, ref, pair_send.at[flow, w, v], pair_got.at[flow, w, v], partner)

    def pair_wait(flow, w, v):
        index = [None] * 3
        for dim, at in zip(flow_dims(flow), (slice(None), back(flow, 1, v), back(flow, 2, w))):
            index[dim] = at
        ref = all_ref.at[(1 - core, *index, flow_rows(flow), slice(None))]
        remote(ref, ref, pair_send.at[flow, w, v], pair_got.at[flow, w, v], partner).wait_recv()

    flows = FLOWS
    local = pltpu.make_async_copy(block_ref, all_ref.at[core, pos[0], pos[1], pos[2]], own_sem)
    local.start()
    for f in flows:
        copy1(f, 0).start()
    for f in flows:
        copy2(f, 0, 0).start()
    local.wait()
    for step in range(STEPS):
        for f in flows:
            wait1(f, step)
            if step < STEPS - 1:
                copy1(f, step + 1).start()
            copy2(f, 0, step + 1).start()
    for f in flows:
        copy3(f, 0, 0).start()
        pair_copy(f, 0, 0).start()
    for step in range(STEPS):
        for u in range(RING):
            for f in flows:
                copy2(f, step, u, 1).wait_recv()
                if step < STEPS - 1:
                    copy2(f, step + 1, u).start()
                if u == RING - 1:
                    copy3(f, 0, step + 1).start()
                    pair_copy(f, 0, step + 1).start()
    for step in range(STEPS):
        for v in range(RING):
            for f in flows:
                copy3(f, step, v, 1).wait_recv()
                if step < STEPS - 1:
                    copy3(f, step + 1, v).start()
                pair_copy(f, step + 1, v).start()
    for w in range(RING):
        for v in range(RING):
            for f in flows:
                pair_wait(f, w, v)
    for f in flows:
        for step in range(STEPS):
            copy1(f, step).wait_send()
            for u in range(RING):
                copy2(f, step, u).wait_send()
                copy3(f, step, u).wait_send()
        for w in range(RING):
            for v in range(RING):
                pair_copy(f, w, v).wait_send()


def gather_blocks(block):
    one, four, pair = SEMS((N_FLOWS, STEPS)), SEMS((N_FLOWS, STEPS, RING)), SEMS((N_FLOWS, RING, RING))
    return pl.pallas_call(
        gather_kernel,
        out_shape=jax.ShapeDtypeStruct((2, RING, RING, RING, ROWS, COLS), BF16),
        in_specs=[in_vmem()],
        out_specs=in_hbm(),
        scratch_shapes=[SEMS, one, one, four, four, four, four, pair, pair],
        compiler_params=comm_params(2),
        name="torus_gather",
    )(block)


def grad_kernel(core_ref, left, left_pair, right, right_pair, *refs):
    del core_ref
    out = refs[-1]
    total = rounded_product(left[...], right[...]) + rounded_product(left_pair[...], right_pair[...])
    if total.shape[1] == COLS:
        out[...] = total.reshape(out.shape)
    else:
        for x in range(out.shape[1]):
            out[:, x, 0] = total[:, COLS * x:COLS * (x + 1)].reshape(-1, BLOCK, COLS)


def grad_sum(core, left, left_pair, right, right_pair, sums):
    tokens = left.shape[0]
    zy = RING * RING
    if sums is None:
        grid = (2, 2)
        left_spec = pl.BlockSpec((tokens, COLS), lambda i, x, c: (0, i))
        right_spec = pl.BlockSpec((tokens, 2 * COLS), lambda i, x, c: (0, c[0] * 2 + x))
        out_spec = pl.BlockSpec((zy // 2, 2, 1, BLOCK, COLS), lambda i, x, c: (i, x, 0, 0, 0))
    else:
        grid = (FF // COLS,)
        left_spec = pl.BlockSpec((tokens, COLS), lambda i, c: (0, i))
        right_spec = pl.BlockSpec((tokens, COLS), lambda i, c: (0, c[0]))
        out_spec = pl.BlockSpec((2, RING, 1, BLOCK, COLS), lambda i, c: (i, 0, 1, 0, 0))
    before = [] if sums is None else [sums]
    return pl.pallas_call(
        grad_kernel,
        out_shape=jax.ShapeDtypeStruct((zy, RING, 2, BLOCK, COLS), F32),
        grid_spec=pltpu.PrefetchScalarGridSpec(
            num_scalar_prefetch=1,
            grid=grid,
            in_specs=[left_spec, left_spec, right_spec, right_spec] + [in_hbm()] * len(before),
            out_specs=out_spec,
        ),
        input_output_aliases={5: 0} if before else {},
        compiler_params=plain_params(len(grid)),
        cost_estimate=pl.CostEstimate(flops=2 * tokens * WIDTH * FF, bytes_accessed=17_000_000, transcendentals=0),
        name="grad_up" if sums is None else "grad_down",
    )(core, left, left_pair, right, right_pair, *before)


def gelu_fn(pre_act):
    return jax.nn.gelu(pre_act, approximate=True)


def up_kernel(hidden, weight, out):
    wide = jnp.concatenate([weight[0, :, x, 0].reshape(WIDTH, COLS) for x in range(2)], axis=1)
    pre_act = jnp.dot(hidden[...], wide, preferred_element_type=F32)
    out[...] = gelu_fn(pre_act).astype(BF16)


def down_kernel(act, weight, hidden, out, total):
    step = pl.program_id(0)

    @pl.when(step == 0)
    def _():
        total[...] = hidden[...].astype(F32)

    wide = jnp.concatenate([weight[c].reshape(WIDTH, COLS) for c in range(2)], axis=1)
    total[...] += jnp.dot(act[...], wide, preferred_element_type=F32)

    @pl.when(step == pl.num_programs(0) - 1)
    def _():
        out[...] = total[...].astype(BF16)


def forward_layer(hidden, weights, layer):
    tokens = hidden.shape[0]
    act = pl.pallas_call(
        up_kernel,
        out_shape=jax.ShapeDtypeStruct((tokens, FF), BF16),
        grid=(2, 2),
        in_specs=[
            pl.BlockSpec((tokens, WIDTH), lambda c, x: (0, 0)),
            pl.BlockSpec((1, 16, 2, 1, BLOCK, COLS), lambda c, x: (c, 0, x, 2 * (LAYERS - 1 - layer), 0, 0)),
        ],
        out_specs=pl.BlockSpec((tokens, 2 * COLS), lambda c, x: (0, c * 2 + x)),
        compiler_params=plain_params(2),
        name="forward_up",
    )(hidden, weights)
    return pl.pallas_call(
        down_kernel,
        out_shape=jax.ShapeDtypeStruct((tokens, WIDTH), BF16),
        grid=(4,),
        in_specs=[
            pl.BlockSpec((tokens, WIDTH), lambda i: (0, i)),
            pl.BlockSpec((2, 4, 4, 1, BLOCK, COLS), lambda i: (0, i, 0, 2 * (LAYERS - 1 - layer) + 1, 0, 0)),
            pl.BlockSpec((tokens, WIDTH), lambda i: (0, 0)),
        ],
        out_specs=pl.BlockSpec((tokens, WIDTH), lambda i: (0, 0)),
        scratch_shapes=[pltpu.VMEM((tokens, WIDTH), F32)],
        compiler_params=plain_params(1),
        name="forward_down",
    )(act, weights, hidden)


def adamw_update(master_old, mom_one, mom_two, grad_clip):
    mom_one_new = BETA_ONE * mom_one + (1.0 - BETA_ONE) * grad_clip
    mom_two_new = BETA_TWO * mom_two + (1.0 - BETA_TWO) * grad_clip * grad_clip
    first_hat = mom_one_new / (1.0 - BETA_ONE ** ADAM_STEP)
    second_hat = mom_two_new / (1.0 - BETA_TWO ** ADAM_STEP)
    master_new = master_old - LEARN_RATE * (first_hat / (jnp.sqrt(second_hat) + ADAM_EPS) + WEIGHT_DECAY * master_old)
    return master_new, mom_one_new, mom_two_new


N_PEERS = OCTET - 1 + 2 * (RING - 1)


def update_kernel(
    block, gacc_up, gacc_down, master_up, master_down, mom1_up, mom1_down, mom2_up, mom2_down,
    new_block, master_up_new, master_down_new, mom1_up_new, mom1_down_new, mom2_up_new, mom2_down_new,
    stage_up, recv_up, recv_down, grad_up, grad_down, norm_send, norm_recv, wide, shard_up, shard_recv, shard_down,
    send_up, got_up, send_down, got_down, send_norm, got_norm, send_w, got_w, send_wd, got_wd,
):
    core, pos = my_place()
    mine = pos[2] * 2 + core
    partner = device_at(pos, 1 - core)
    octet = [(lax.rem(mine + k, OCTET), device_at((pos[0], pos[1], 0), lax.rem(mine + k, OCTET))) for k in range(1, OCTET)]
    along = [[neighbor(pos, core, dim, k) for k in range(1, RING)] for dim in (1, 0)]
    entry_barrier([device for _, device in octet] + along[0] + along[1])

    def down_copy(layer):
        rows = aligned(down_base(layer) + DOWN_ROWS * (1 - core), DOWN_ROWS)
        return remote(block.at[rows], recv_down.at[layer], send_down.at[layer], got_down.at[layer], partner)

    for layer in range(LAYERS):
        down_copy(layer).start()
    for q in range(OCTET):
        for j in range(UP_ROWS):
            for layer in range(LAYERS):
                stage_up[q, j, pl.ds(layer, 1), :] = block[pl.ds(up_base(layer) + q * UP_ROWS + j, 1), :]

    def up_copy(k):
        to, device = octet[k - 1]
        return remote(stage_up.at[to], recv_up.at[k], send_up.at[k - 1], got_up.at[k - 1], device)

    for k in range(1, OCTET):
        up_copy(k).start()
    recv_up[0] = stage_up[mine]

    total = jnp.zeros((CHUNK, LANES), F32)
    for layer in range(LAYERS):
        down_copy(layer).wait_recv()
        for from_me in (True, False):
            cols = aligned_lanes((core if from_me else 1 - core) * COLS, COLS)
            if from_me:
                part = block[aligned(down_base(layer) + DOWN_ROWS * core, DOWN_ROWS), :]
            else:
                part = recv_down[layer]
            grad = (gacc_down[layer, :, cols] + part) / MICRO_STEPS
            grad_down[layer, :, cols] = grad
            square = grad * grad
            for i in range(COLS // LANES):
                for n in range(COLS // LANES):
                    total = total + square[CHUNK * i:CHUNK * i + CHUNK, LANES * n:LANES * n + LANES]
    total_up = jnp.zeros((LAYERS, LANES), F32)
    for k in range(OCTET):
        if k > 0:
            up_copy(k).wait_recv()
        source = lax.rem(mine + OCTET - k, OCTET)
        cols = aligned_lanes((lax.rem(source, 2) * RING + lax.div(source, 2)) * COLS, COLS)
        for j in range(UP_ROWS):
            grad = (gacc_up[j, :, cols] + recv_up[k, j]) / MICRO_STEPS
            grad_up[j, :, cols] = grad
            square = grad * grad
            for n in range(COLS // LANES):
                total_up = total_up + square[:, LANES * n:LANES * n + LANES]
    norm_send[0] = total + jnp.concatenate([total_up, jnp.zeros((CHUNK - LAYERS, LANES), F32)], axis=0)

    slot = 0
    rounds = ([device for _, device in octet], along[0], along[1])
    sent = []
    for r, peers in enumerate(rounds):
        copies = [
            remote(norm_send.at[r], norm_recv.at[slot + k], send_norm.at[slot + k], got_norm.at[slot + k], device)
            for k, device in enumerate(peers)
        ]
        for copy in copies:
            copy.start()
        total = norm_send[r]
        for k, copy in enumerate(copies):
            copy.wait_recv()
            total = total + norm_recv[slot + k]
        slot += len(peers)
        sent += copies
        if r < 2:
            norm_send[r + 1] = total
    norm_sq = jnp.sum(total, keepdims=True)
    clip_norm = 0.1 * math.sqrt(2 * LAYERS * WIDTH * FF)
    clip = jnp.minimum(1.0, clip_norm / jnp.sqrt(norm_sq))

    for layer in range(LAYERS):
        new = adamw_update(master_down[layer], mom1_down[layer], mom2_down[layer], grad_down[layer] * clip)
        master_down_new[layer], mom1_down_new[layer], mom2_down_new[layer] = new
        weight = new[0].astype(BF16).astype(F32)
        for half in range(LAYERS):
            shard_down[half, layer] = weight[:, half * COLS:half * COLS + COLS]

    def wd_copy(layer):
        rows = aligned(down_base(layer) + DOWN_ROWS * core, DOWN_ROWS)
        return remote(shard_down.at[1 - core, layer], wide.at[rows], send_wd.at[layer], got_wd.at[layer], partner)

    for q in range(OCTET):
        cols = pl.ds(((q % 2) * RING + q // 2) * COLS, COLS)
        for j in range(UP_ROWS):
            new = adamw_update(master_up[j, :, cols], mom1_up[j, :, cols], mom2_up[j, :, cols], grad_up[j, :, cols] * clip)
            master_up_new[j, :, cols], mom1_up_new[j, :, cols], mom2_up_new[j, :, cols] = new
            shard_up[q, j] = new[0].astype(BF16).astype(F32)

    def w_copy(k):
        to, device = octet[k - 1]
        return remote(shard_up.at[to], shard_recv.at[k], send_w.at[k - 1], got_w.at[k - 1], device)

    for layer in range(LAYERS):
        wd_copy(layer).start()
    for k in range(1, OCTET):
        w_copy(k).start()
    shard_recv[0] = shard_up[mine]
    for layer in range(LAYERS):
        wide[aligned(down_base(layer) + DOWN_ROWS * core, DOWN_ROWS), :] = shard_down[core, layer]
    for k in range(OCTET):
        if k > 0:
            w_copy(k).wait_recv()
    for q in range(OCTET):
        behind = lax.rem(mine + OCTET - q, OCTET)
        for j in range(UP_ROWS):
            for layer in range(LAYERS):
                wide[pl.ds(up_base(layer) + q * UP_ROWS + j, 1), :] = shard_recv[behind, j, pl.ds(layer, 1), :]
    for layer in range(LAYERS):
        rows = aligned(down_base(layer) + DOWN_ROWS * (1 - core), DOWN_ROWS)
        remote(shard_down.at[1 - core, layer], wide.at[rows], send_wd.at[layer], got_wd.at[layer], partner).wait_recv()
    new_block[...] = wide[...].astype(BF16)

    for layer in range(LAYERS):
        down_copy(layer).wait_send()
        wd_copy(layer).wait_send()
    for k in range(1, OCTET):
        up_copy(k).wait_send()
        w_copy(k).wait_send()
    for copy in sent:
        copy.wait_send()


UP_SHAPE = (UP_ROWS, LAYERS, FF)
DOWN_SHAPE = (LAYERS, DOWN_ROWS, WIDTH)


def update_rows(block, *arrays):
    up = jax.ShapeDtypeStruct(UP_SHAPE, F32)
    down = jax.ShapeDtypeStruct(DOWN_SHAPE, F32)
    rows = pltpu.VMEM((OCTET, UP_ROWS, LAYERS, COLS), F32)
    seven, two, norm = SEMS((OCTET - 1,)), SEMS((LAYERS,)), SEMS((N_PEERS,))
    return pl.pallas_call(
        update_kernel,
        out_shape=[jax.ShapeDtypeStruct((ROWS, COLS), BF16), up, down, up, down, up, down],
        in_specs=[in_vmem()] * (1 + len(arrays)),
        out_specs=[in_vmem()] * 7,
        scratch_shapes=[
            rows, rows, pltpu.VMEM((LAYERS, DOWN_ROWS, COLS), F32), pltpu.VMEM(UP_SHAPE, F32), pltpu.VMEM(DOWN_SHAPE, F32),
            pltpu.VMEM((3, CHUNK, LANES), F32), pltpu.VMEM((N_PEERS, CHUNK, LANES), F32), pltpu.VMEM((ROWS, COLS), F32),
            rows, rows, pltpu.VMEM((2, LAYERS, DOWN_ROWS, COLS), F32),
            seven, seven, two, two, norm, norm, seven, seven, two, two,
        ],
        compiler_params=comm_params(3),
        name="update_rows",
    )(block, *arrays)


def keep_kernel(*refs):
    half = len(refs) // 2
    for src, dst in zip(refs[:half], refs[half:]):
        dst[...] = src[...]


def keep(arrays):
    return pl.pallas_call(
        keep_kernel,
        out_shape=[jax.ShapeDtypeStruct(a.shape, a.dtype) for a in arrays],
        in_specs=[in_vmem()] * len(arrays),
        out_specs=[in_vmem()] * len(arrays),
        compiler_params=plain_params(0),
        name="keep",
    )(*arrays)


SWAP = [(i, i ^ 1) for i in range(2 * RING * RING * RING)]


def swap_cores(array):
    return lax.ppermute(array, "fsdp", SWAP)


def rows_first(array):
    return jnp.transpose(array, (1, 0, 2))


def local_step(x_saved, grad_out, x_next, w_up, w_down, gacc_up, gacc_down, master_up, master_down, mom1_up, mom1_down, mom2_up, mom2_down):
    core = jnp.reshape(lax.rem(lax.axis_index("fsdp"), 2), (1,))
    x_tokens = x_saved.reshape(LAYERS, -1, WIDTH)
    grad_cur = grad_out.reshape(-1, WIDTH)
    operands = []
    for layer_idx in range(LAYERS - 1, -1, -1):
        x_in = x_tokens[layer_idx]
        pre_act = jnp.dot(x_in, w_up[layer_idx], preferred_element_type=F32)
        hidden_act, gelu_vjp = jax.vjp(gelu_fn, pre_act)
        d_act = lax.dot_general(grad_cur, w_down[layer_idx], (((1,), (1,)), ((), ())), preferred_element_type=F32)
        d_pre = gelu_vjp(d_act)[0].astype(BF16)
        operands.append((x_in, d_pre, hidden_act.astype(BF16), grad_cur))
        if layer_idx > 0:
            grad_cur = (grad_cur.astype(F32) + lax.dot_general(d_pre, w_up[layer_idx], (((1,), (1,)), ((), ())), preferred_element_type=F32)).astype(BF16)
    x_last, d_last, a_last, g_last = operands[0]
    sums = grad_sum(core, x_last, swap_cores(x_last), d_last, swap_cores(d_last), None)
    sums = grad_sum(core, a_last, swap_cores(a_last), g_last, swap_cores(g_last), sums)
    block = reduce_blocks(sums.reshape(RING, RING, RING, PAIR_ROWS, COLS), *operands[1])

    new_block, *state = update_rows(
        block, rows_first(gacc_up), gacc_down, rows_first(master_up), master_down,
        rows_first(mom1_up), mom1_down, rows_first(mom2_up), mom2_down,
    )
    weights = gather_blocks(new_block).reshape(2, RING * RING, RING, 2 * LAYERS, BLOCK, COLS)
    master_up, master_down, mom1_up, mom1_down, mom2_up, mom2_down = keep(state)

    hidden = x_next.reshape(-1, WIDTH)
    for layer_idx in range(LAYERS):
        hidden = forward_layer(hidden, weights, layer_idx)
    return (hidden.reshape(x_next.shape), rows_first(master_up), master_down, rows_first(mom1_up), mom1_down, rows_first(mom2_up), mom2_down)


def solution(mesh):
    rows_spec = P(None, "fsdp")
    return jax.shard_map(local_step, mesh=mesh, in_specs=(rows_spec, P("fsdp"), P("fsdp"), P(), P(), rows_spec, rows_spec, rows_spec, rows_spec, rows_spec, rows_spec, rows_spec, rows_spec), out_specs=(P("fsdp"), rows_spec, rows_spec, rows_spec, rows_spec, rows_spec, rows_spec), check_vma=False)
```

```python
import functools
import math

import jax
import jax.numpy as jnp
from jax import lax
from jax.experimental import pallas as pl
from jax.experimental.pallas import tpu as pltpu
from jax.sharding import PartitionSpec as P

LEARN_RATE = 0.001
BETA_ONE = 0.9
BETA_TWO = 0.95
ADAM_EPS = 1e-8
WEIGHT_DECAY = 0.1
ADAM_STEP = 3
MICRO_STEPS = 2

MESH = pl.DeviceIdType.MESH
BF16 = jnp.bfloat16
F32 = jnp.float32
VMEM_LIMIT = 67_000_000
LAYERS = 2
RING = 4
WIDTH = 1280
FF = 5120
UP_ROWS = 10
DOWN_ROWS = 40
BLOCK = 80
COLS = 640
PAIR_ROWS = 2 * BLOCK
ROWS = LAYERS * PAIR_ROWS
LANES = 128
OCTET = 8
CHUNK = 8
SEMS = pltpu.SemaphoreType.DMA

BATCH_CHUNKS = PAIR_ROWS // CHUNK
ORDERS = ((0, 1, 2), (1, 2, 0), (2, 0, 1))
N_FLOWS = 6
FLOWS = range(N_FLOWS)
TICKS = RING
STEPS = RING - 1
BATCH_LEN = [[TICKS if f // 2 == b else TICKS - 1 for f in FLOWS] for b in range(LAYERS)]
BATCH_START = [[sum(lens[:f]) for f in FLOWS] for lens in BATCH_LEN]
OWN_SLOTS = 3
UP_TILES = 8
TILES = 16


def up_base(layer):
    return (LAYERS - 1 - layer) * PAIR_ROWS


def down_base(layer):
    return up_base(layer) + BLOCK


def comm_params(collective_id):
    return pltpu.CompilerParams(collective_id=collective_id, has_side_effects=True, vmem_limit_bytes=VMEM_LIMIT)


def plain_params(dims):
    return pltpu.CompilerParams(dimension_semantics=("arbitrary",) * dims, vmem_limit_bytes=VMEM_LIMIT)


def in_vmem():
    return pl.BlockSpec(memory_space=pltpu.VMEM)


def in_hbm():
    return pl.BlockSpec(memory_space=pl.ANY)


def aligned(start, size):
    return pl.ds(pl.multiple_of(start, CHUNK), size)


def aligned_lanes(start, size):
    return pl.ds(pl.multiple_of(start, LANES), size)


def remote(src, dst, send, got, device):
    return pltpu.make_async_remote_copy(
        src_ref=src, dst_ref=dst, send_sem=send, recv_sem=got, device_id=(device,), device_id_type=MESH
    )

def flow_dims(flow):
    return ORDERS[flow // 2]


def flow_sign(flow):
    return 1 - 2 * (flow % 2)


def my_place():
    me = lax.axis_index("fsdp")
    core, chip = lax.rem(me, 2), lax.div(me, 2)
    line = lax.div(chip, RING)
    return core, (lax.div(line, RING), lax.rem(line, RING), lax.rem(chip, RING))


def device_at(pos, core):
    return ((pos[0] * RING + pos[1]) * RING + pos[2]) * 2 + core


def neighbor(pos, core, dim, sign):
    moved = list(pos)
    moved[dim] = lax.rem(pos[dim] + RING + sign, RING)
    return device_at(moved, core)


def all_neighbors(pos, core):
    return [neighbor(pos, core, dim, sign) for dim in range(3) for sign in (1, -1)]


def entry_barrier(peers):
    barrier = pltpu.get_barrier_semaphore()
    for peer in peers:
        pl.semaphore_signal(barrier, inc=1, device_id=(peer,), device_id_type=MESH)
    pl.semaphore_wait(barrier, len(peers))


def rounded_product(left, right):
    return lax.dot_general(left, right, (((0,), (0,)), ((), ())), preferred_element_type=F32).astype(BF16).astype(F32)


def reduce_kernel(
    s_last, x_own, d_own, a_own, g_own, out_ref, s_first, x_pair, d_pair, a_pair, g_pair,
    recv1, recv2, recv3, own, left, left_pair, right, right_pair, tile, own_sem, tile_in, tile_out, pair_send, pair_got, credit,
    send1, got1, send2, got2, send3, got3,
):
    core, pos = my_place()
    partner = device_at(pos, 1 - core)
    entry_barrier([partner] + all_neighbors(pos, core))
    target = [[neighbor(pos, core, dim, flow_sign(f)) for dim in flow_dims(f)] for f in FLOWS]
    source = [neighbor(pos, core, flow_dims(f)[0], -flow_sign(f)) for f in FLOWS]
    sums = (s_last, s_first)

    def seg(flow, phase, step):
        at = pos[flow_dims(flow)[phase]]
        return lax.rem(at + 2 * RING - flow_sign(flow) * (1 + step), RING)

    def s_slice(b, flow, j, chunk):
        index = [slice(None)] * 3
        index[flow_dims(flow)[0]] = j
        return sums[b].at[(*index, aligned(chunk * CHUNK, CHUNK), slice(None))]

    def part2(flow, ref, j):
        second, third = flow_dims(flow)[1:]
        return ref.at[j] if second < third else ref.at[:, j]

    def slot1(b, step):
        return step + b * 2 * ((step + 1) // 2)

    def land1(b, step, chunk):
        return recv1.at[slot1(b, step), chunk]

    def land2(b, step, chunk):
        return recv2.at[b, step, chunk]

    def land3(b, step, chunk):
        return recv3.at[b, step, chunk]

    lands, sends, gots = (land1, land2, land3), (send1, send2, send3), (got1, got2, got3)

    def copy(phase, b, flow, step, chunk, src):
        dst = lands[phase](b, step, chunk)
        return remote(dst if src is None else src, dst, sends[phase].at[b, step, chunk], gots[phase].at[b, step, chunk], target[flow][phase])

    def first_copy(phase, b, flow, chunk):
        j = seg(flow, phase, 0)
        if phase == 0:
            src = s_slice(b, flow, j, chunk)
        elif phase == 1:
            src = part2(flow, land1(b, STEPS - 1, chunk), j)
        else:
            src = recv2.at[b, STEPS - 1, chunk, j]
        return copy(phase, b, flow, 0, chunk, src)

    def next_copy(phase, b, flow, step, chunk):
        return copy(phase, b, flow, step + 1, chunk, lands[phase](b, step, chunk))

    def own_copy(b, flow, n):
        step, k = lax.div(n, TICKS), lax.rem(n, TICKS)
        slot = lax.rem(n, OWN_SLOTS)
        src = s_slice(b, flow, seg(flow, 0, step + 1), BATCH_START[b][flow] + k)
        return pltpu.make_async_copy(src, own.at[flow, slot], own_sem.at[flow, slot])

    def start_batch(b):
        for k in range(TICKS):
            for f in FLOWS:
                if k < BATCH_LEN[b][f]:
                    first_copy(0, b, f, BATCH_START[b][f] + k).start()
        for n in range(OWN_SLOTS - 1):
            for f in FLOWS:
                own_copy(b, f, n).start()

    def tick(phase, b, n):
        step, k = lax.div(n, TICKS), lax.rem(n, TICKS)

        def each(body):
            for f in FLOWS:
                if BATCH_LEN[b][f] == TICKS:
                    body(f, BATCH_START[b][f] + k)
                else:
                    pl.when(k < BATCH_LEN[b][f])(functools.partial(body, f, BATCH_START[b][f] + k))

        def add(f, chunk):
            copy(phase, b, f, step, chunk, None).wait_recv()
            landed = lands[phase](b, step, chunk)
            if phase == 0:
                own_copy(b, f, n).wait()
                landed[...] = landed[...] + own[f, lax.rem(n, OWN_SLOTS)]
            elif phase == 1:
                landed[...] = landed[...] + part2(f, land1(b, STEPS - 1, chunk), seg(f, 1, step + 1))[...]
            else:
                landed[...] = landed[...] + recv2[b, STEPS - 1, chunk, seg(f, 2, step + 1)]

        def pass_on(f, chunk):
            @pl.when(step < STEPS - 1)
            def _():
                next_copy(phase, b, f, step, chunk).start()

            @pl.when(step == STEPS - 1)
            def _():
                if phase < 2:
                    first_copy(phase + 1, b, f, chunk).start()
                else:
                    out_ref[aligned((b * BATCH_CHUNKS + chunk) * CHUNK, CHUNK), :] = recv3[b, STEPS - 1, chunk]

        if phase == 0:
            later = n + OWN_SLOTS - 1
            for f in FLOWS:
                @pl.when((later < STEPS * TICKS) & (lax.rem(later, TICKS) < BATCH_LEN[b][f]))
                def _():
                    own_copy(b, f, later).start()

        each(add)
        each(pass_on)

    def tile_reads(job, up):
        slot = lax.rem(job, 2)
        if up:
            rows = aligned_lanes(lax.div(job, RING) * COLS, COLS)
            cols = lax.rem(job, RING) * COLS
            reads = (x_own.at[:, rows], x_pair.at[:, rows], d_own.at[:, aligned_lanes(core * (FF // 2) + cols, COLS)], d_pair.at[:, aligned_lanes(cols, COLS)])
        else:
            rows = aligned_lanes((job - UP_TILES) * COLS, COLS)
            reads = (a_own.at[:, rows], a_pair.at[:, rows], g_own.at[:, aligned_lanes(core * COLS, COLS)], g_pair)
        return [
            pltpu.make_async_copy(src, dst.at[slot], tile_in.at[i, slot])
            for i, (src, dst) in enumerate(zip(reads, (left, left_pair, right, right_pair)))
        ]

    def start_reads(job):
        for up in (True, False):
            @pl.when((job < UP_TILES) if up else (job >= UP_TILES) & (job < TILES))
            def _():
                for read in tile_reads(job, up):
                    read.start()

    def tile_write(job, up):
        slot = lax.rem(job, 2)
        if up:
            dst = s_first.at[pl.ds(lax.div(job, RING) * 2, 2), :, lax.rem(job, RING), pl.ds(0, BLOCK)]
        else:
            i = job - UP_TILES
            dst = s_first.at[lax.div(i, 2), pl.ds(lax.rem(i, 2) * 2, 2), :, pl.ds(BLOCK, BLOCK)]
        return pltpu.make_async_copy(tile.at[slot], dst, tile_out.at[slot])

    def compute(job):
        slot = lax.rem(job, 2)
        start_reads(job + 1)
        for read in tile_reads(UP_TILES + slot, False):
            read.wait()

        @pl.when(job >= 2)
        def _():
            tile_write(UP_TILES + slot, False).wait()

        total = rounded_product(left[slot], right[slot]) + rounded_product(left_pair[slot], right_pair[slot])
        tile[slot] = total.reshape(tile.shape[1:])
        for up in (True, False):
            @pl.when((job < UP_TILES) if up else (job >= UP_TILES))
            def _():
                tile_write(job, up).start()

    start_batch(0)
    other = 1 - core
    gives = (x_own, d_own.at[:, aligned_lanes(other * (FF // 2), FF // 2)], a_own, g_own.at[:, aligned_lanes(other * COLS, COLS)])
    exchange = [
        remote(src, dst, pair_send.at[i], pair_got.at[i], partner)
        for i, (src, dst) in enumerate(zip(gives, (x_pair, d_pair, a_pair, g_pair)))
    ]
    for give in exchange:
        give.start()
    for give in exchange:
        give.wait_recv()
    start_reads(0)

    @pl.loop(0, 2 * TICKS)
    def _(n):
        tick(0, 0, n)

        @pl.loop(0, 2)
        def _(i):
            compute(2 * n + i)

    for slot in range(2):
        tile_write(UP_TILES + slot, False).wait()
    for f in FLOWS:
        for k in range(BATCH_LEN[0][f]):
            copy(0, 0, f, 1, BATCH_START[0][f] + k, None).wait_send()
        pl.semaphore_signal(credit.at[f], inc=1, device_id=(source[f],), device_id_type=MESH)
    for f in FLOWS:
        pl.semaphore_wait(credit.at[f], 1)
    for k in range(TICKS):
        for f in FLOWS:
            if k < BATCH_LEN[1][f]:
                first_copy(0, 1, f, BATCH_START[1][f] + k).start()

    @pl.loop(2 * TICKS, STEPS * TICKS)
    def _(n):
        tick(0, 0, n)

    for n in range(OWN_SLOTS - 1):
        for f in FLOWS:
            own_copy(1, f, n).start()

    @pl.loop(0, STEPS * TICKS)
    def _(n):
        tick(0, 1, n)
        tick(1, 0, n)

    @pl.loop(0, STEPS * TICKS)
    def _(n):
        tick(1, 1, n)
        tick(2, 0, n)

    @pl.loop(0, STEPS * TICKS)
    def _(n):
        tick(2, 1, n)

    for give in exchange:
        give.wait_send()
    for b in range(LAYERS):
        for f in FLOWS:
            @pl.loop(BATCH_START[b][f], BATCH_START[b][f] + BATCH_LEN[b][f])
            def _(chunk):
                for phase in range(3):
                    for step in range(STEPS):
                        if (phase, b, step) != (0, 0, 1):
                            copy(phase, b, f, step, chunk, None).wait_send()


def reduce_blocks(s_last, x_first, d_first, a_first, g_first):
    tokens = x_first.shape[0]

    def half(width):
        return jax.ShapeDtypeStruct((tokens, width), BF16)

    piece = pltpu.VMEM((2, tokens, COLS), BF16)
    sems = SEMS((LAYERS, STEPS, BATCH_CHUNKS))
    return pl.pallas_call(
        reduce_kernel,
        out_shape=[jax.ShapeDtypeStruct((ROWS, COLS), F32), jax.ShapeDtypeStruct(s_last.shape, F32), half(WIDTH), half(FF // 2), half(FF), half(COLS)],
        in_specs=[in_hbm()] * 5,
        out_specs=[in_vmem()] + [in_hbm()] * 5,
        scratch_shapes=[
            pltpu.VMEM((5, BATCH_CHUNKS, RING, RING, CHUNK, COLS), F32),
            pltpu.VMEM((LAYERS, STEPS, BATCH_CHUNKS, RING, CHUNK, COLS), F32),
            pltpu.VMEM((LAYERS, STEPS, BATCH_CHUNKS, CHUNK, COLS), F32),
            pltpu.VMEM((N_FLOWS, OWN_SLOTS, RING, RING, CHUNK, COLS), F32),
            piece, piece, piece, piece,
            pltpu.VMEM((2, 2, RING, BLOCK, COLS), F32),
            SEMS((N_FLOWS, OWN_SLOTS)), SEMS((4, 2)), SEMS((2,)), SEMS((4,)), SEMS((4,)), pltpu.SemaphoreType.REGULAR((N_FLOWS,)),
            sems, sems, sems, sems, sems, sems,
        ],
        compiler_params=comm_params(1),
        name="torus_reduce",
    )(s_last, x_first, d_first, a_first, g_first)[0]


N_MATRICES = 2 * LAYERS
MATRIX_BASE = [base for layer in range(LAYERS) for base in (up_base(layer), down_base(layer))]
SHORT = (2, 1, 0, 2)
MATRIX_LEN = [[CHUNK if f // 2 == SHORT[q] else 2 * CHUNK for f in FLOWS] for q in range(N_MATRICES)]
MATRIX_START = [[MATRIX_BASE[q] + sum(MATRIX_LEN[q][:f]) for f in FLOWS] for q in range(N_MATRICES)]


def gather_kernel(
    block_ref, x_ref, all_ref, hidden_ref, act_ref,
    total, weight, own_sem, load_sem, send1, got1, send2, got2, send3, got3, pair_send, pair_got,
):
    core, pos = my_place()
    partner = device_at(pos, 1 - core)
    entry_barrier([partner] + all_neighbors(pos, core))
    target = [[neighbor(pos, core, dim, flow_sign(f)) for dim in flow_dims(f)] for f in FLOWS]
    pieces = [(q, f) for q in range(N_MATRICES) for f in FLOWS]

    def rows_of(q, flow):
        return pl.ds(MATRIX_START[q][flow], MATRIX_LEN[q][flow])

    def back(flow, phase, steps):
        at = pos[flow_dims(flow)[phase]]
        return lax.rem(at + RING - flow_sign(flow) * steps, RING)

    def place(which, q, flow, *at):
        index = [slice(None)] * 3
        for phase, steps in enumerate(at):
            if steps is not None:
                index[flow_dims(flow)[phase]] = back(flow, phase, steps)
        return all_ref.at[(which, *index, rows_of(q, flow), slice(None))]

    def copy1(q, flow, step, off=0):
        dst = place(core, q, flow, step + off, 0, 0)
        src = dst if off or step else block_ref.at[rows_of(q, flow)]
        return remote(src, dst, send1.at[q, flow, step], got1.at[q, flow, step], target[flow][0])

    def copy2(q, flow, step, off=0):
        ref = place(core, q, flow, None, step + off, 0)
        return remote(ref, ref, send2.at[q, flow, step], got2.at[q, flow, step], target[flow][1])

    def copy3(q, flow, step, v, off=0):
        ref = place(core, q, flow, None, v, step + off)
        return remote(ref, ref, send3.at[q, flow, step, v], got3.at[q, flow, step, v], target[flow][2])

    def pair_copy(q, flow, w, which=core):
        ref = place(which, q, flow, None, None, w)
        return remote(ref, ref, pair_send.at[q, flow, w], pair_got.at[q, flow, w], partner)

    local = pltpu.make_async_copy(block_ref, all_ref.at[core, pos[0], pos[1], pos[2]], own_sem)
    local.start()
    for q, f in pieces:
        copy1(q, f, 0).start()
    local.wait()
    for step in range(STEPS):
        for q, f in pieces:
            copy1(q, f, step, 1).wait_recv()
            if step < STEPS - 1:
                copy1(q, f, step + 1).start()
            else:
                copy2(q, f, 0).start()
    for q, f in pieces:
        copy3(q, f, 0, 0).start()
    for step in range(STEPS):
        for q, f in pieces:
            copy2(q, f, step, 1).wait_recv()
            if step < STEPS - 1:
                copy2(q, f, step + 1).start()
            copy3(q, f, 0, step + 1).start()
    for q, f in pieces:
        pair_copy(q, f, 0).start()

    @pl.loop(0, STEPS - 1)
    def _(step):
        for q in range(N_MATRICES):
            for v in range(RING):
                for f in FLOWS:
                    copy3(q, f, step, v, 1).wait_recv()
                    copy3(q, f, step + 1, v).start()
            for f in FLOWS:
                pair_copy(q, f, step + 1).start()

    def last_step(q):
        for f in FLOWS:
            for v in range(RING):
                copy3(q, f, STEPS - 1, v, 1).wait_recv()
            pair_copy(q, f, STEPS).start()

    def have_pair(q):
        for f in FLOWS:
            for w in range(RING):
                pair_copy(q, f, w, 1 - core).wait_recv()

    def load(q, i):
        rows = pl.ds(MATRIX_BASE[q], BLOCK)
        if q % 2 == 0:
            src = all_ref.at[lax.div(i, 2), :, :, pl.ds(lax.rem(i, 2) * 2, 2), rows]
        else:
            src = all_ref.at[:, i, :, :, rows]
        slot = lax.rem(i, 2)
        dst = weight.at[slot].reshape(src.shape)
        return pltpu.make_async_copy(src, dst, load_sem.at[slot])

    def product(q, i):
        slot = lax.rem(i, 2)
        cols = aligned_lanes(i * WIDTH, WIDTH)
        if q % 2 == 0:
            tiles = weight[slot].reshape(RING * RING, 2, BLOCK, COLS)
            wide = jnp.concatenate([tiles[:, x].reshape(WIDTH, COLS) for x in range(2)], axis=1)
            hidden = x_ref if q == 0 else hidden_ref
            act_ref[:, cols] = gelu_fn(jnp.dot(hidden[...], wide, preferred_element_type=F32)).astype(BF16)
        else:
            tiles = weight[slot].reshape(2, WIDTH, COLS)
            wide = jnp.concatenate([tiles[c] for c in range(2)], axis=1)
            total[...] += jnp.dot(act_ref[:, cols], wide, preferred_element_type=F32)

    last_step(0)
    have_pair(0)
    load(0, 0).start()
    for q in range(N_MATRICES - 1):
        if q % 2:
            total[...] = x_ref[...].astype(F32)

        @pl.loop(0, RING)
        def _(i):
            load(q, i).wait()

            @pl.when(i < RING - 1)
            def _():
                load(q, i + 1).start()

            @pl.when(i == RING - 1)
            def _():
                have_pair(q + 1)
                if q + 1 < N_MATRICES - 1:
                    load(q + 1, 0).start()

            product(q, i)

            @pl.when(i == 1)
            def _():
                last_step(q + 1)

        if q % 2:
            hidden_ref[...] = total[...].astype(BF16)
    for q, f in pieces:
        for step in range(STEPS):
            copy1(q, f, step).wait_send()
            copy2(q, f, step).wait_send()
            for v in range(RING):
                copy3(q, f, step, v).wait_send()
        for w in range(RING):
            pair_copy(q, f, w).wait_send()


def gather_forward(block, x_next):
    tokens = x_next.shape[0]
    one, four = SEMS((N_MATRICES, N_FLOWS, STEPS)), SEMS((N_MATRICES, N_FLOWS, STEPS, RING))
    pair = SEMS((N_MATRICES, N_FLOWS, RING))
    return pl.pallas_call(
        gather_kernel,
        out_shape=[
            jax.ShapeDtypeStruct((2, RING, RING, RING, ROWS, COLS), BF16),
            jax.ShapeDtypeStruct((tokens, WIDTH), BF16),
            jax.ShapeDtypeStruct((tokens, FF), BF16),
        ],
        in_specs=[in_vmem(), in_vmem()],
        out_specs=[in_hbm(), in_vmem(), in_vmem()],
        scratch_shapes=[
            pltpu.VMEM((tokens, WIDTH), F32), pltpu.VMEM((2, 2, RING, RING, BLOCK, COLS), BF16),
            SEMS, SEMS((2,)), one, one, one, one, four, four, pair, pair,
        ],
        compiler_params=comm_params(2),
        name="torus_gather_forward",
    )(block, x_next)


def grad_kernel(core_ref, left, left_pair, right, right_pair, *refs):
    del core_ref
    out = refs[-1]
    total = rounded_product(left[...], right[...]) + rounded_product(left_pair[...], right_pair[...])
    if total.shape[1] == COLS:
        out[...] = total.reshape(out.shape)
    else:
        for x in range(out.shape[1]):
            out[:, x, 0] = total[:, COLS * x:COLS * (x + 1)].reshape(-1, BLOCK, COLS)


def grad_sum(core, left, left_pair, right, right_pair, sums):
    tokens = left.shape[0]
    zy = RING * RING
    if sums is None:
        grid = (2, 2)
        left_spec = pl.BlockSpec((tokens, COLS), lambda i, x, c: (0, i))
        right_spec = pl.BlockSpec((tokens, 2 * COLS), lambda i, x, c: (0, c[0] * 2 + x))
        out_spec = pl.BlockSpec((zy // 2, 2, 1, BLOCK, COLS), lambda i, x, c: (i, x, 0, 0, 0))
    else:
        grid = (FF // COLS,)
        left_spec = pl.BlockSpec((tokens, COLS), lambda i, c: (0, i))
        right_spec = pl.BlockSpec((tokens, COLS), lambda i, c: (0, c[0]))
        out_spec = pl.BlockSpec((2, RING, 1, BLOCK, COLS), lambda i, c: (i, 0, 1, 0, 0))
    before = [] if sums is None else [sums]
    return pl.pallas_call(
        grad_kernel,
        out_shape=jax.ShapeDtypeStruct((zy, RING, 2, BLOCK, COLS), F32),
        grid_spec=pltpu.PrefetchScalarGridSpec(
            num_scalar_prefetch=1,
            grid=grid,
            in_specs=[left_spec, left_spec, right_spec, right_spec] + [in_hbm()] * len(before),
            out_specs=out_spec,
        ),
        input_output_aliases={5: 0} if before else {},
        compiler_params=plain_params(len(grid)),
        cost_estimate=pl.CostEstimate(flops=2 * tokens * WIDTH * FF, bytes_accessed=17_000_000, transcendentals=0),
        name="grad_up" if sums is None else "grad_down",
    )(core, left, left_pair, right, right_pair, *before)


def gelu_fn(pre_act):
    return jax.nn.gelu(pre_act, approximate=True)


def down_kernel(act, weight, hidden, out, total):
    step = pl.program_id(0)

    @pl.when(step == 0)
    def _():
        total[...] = hidden[...].astype(F32)

    wide = jnp.concatenate([weight[c].reshape(WIDTH, COLS) for c in range(2)], axis=1)
    total[...] += jnp.dot(act[...], wide, preferred_element_type=F32)

    @pl.when(step == pl.num_programs(0) - 1)
    def _():
        out[...] = total[...].astype(BF16)


def last_product(act, weights, hidden):
    tokens = hidden.shape[0]
    return pl.pallas_call(
        down_kernel,
        out_shape=jax.ShapeDtypeStruct((tokens, WIDTH), BF16),
        grid=(RING,),
        in_specs=[
            pl.BlockSpec((tokens, WIDTH), lambda i: (0, i)),
            pl.BlockSpec((2, RING, RING, 1, BLOCK, COLS), lambda i: (0, i, 0, 1, 0, 0)),
            pl.BlockSpec((tokens, WIDTH), lambda i: (0, 0)),
        ],
        out_specs=pl.BlockSpec((tokens, WIDTH), lambda i: (0, 0)),
        scratch_shapes=[pltpu.VMEM((tokens, WIDTH), F32)],
        compiler_params=plain_params(1),
        name="forward_down",
    )(act, weights, hidden)


def adamw_update(master_old, mom_one, mom_two, grad_clip):
    mom_one_new = BETA_ONE * mom_one + (1.0 - BETA_ONE) * grad_clip
    mom_two_new = BETA_TWO * mom_two + (1.0 - BETA_TWO) * grad_clip * grad_clip
    first_hat = mom_one_new / (1.0 - BETA_ONE ** ADAM_STEP)
    second_hat = mom_two_new / (1.0 - BETA_TWO ** ADAM_STEP)
    master_new = master_old - LEARN_RATE * (first_hat / (jnp.sqrt(second_hat) + ADAM_EPS) + WEIGHT_DECAY * master_old)
    return master_new, mom_one_new, mom_two_new


N_PEERS = OCTET - 1 + 2 * (RING - 1)


def update_kernel(
    block, gacc_up, gacc_down, master_up, master_down, mom1_up, mom1_down, mom2_up, mom2_down,
    new_block, master_up_new, master_down_new, mom1_up_new, mom1_down_new, mom2_up_new, mom2_down_new,
    stage_up, recv_up, recv_down, grad_up, grad_down, norm_send, norm_recv, wide, shard_up, shard_recv, shard_down,
    send_up, got_up, send_down, got_down, send_norm, got_norm, send_w, got_w, send_wd, got_wd,
):
    core, pos = my_place()
    mine = pos[2] * 2 + core
    partner = device_at(pos, 1 - core)
    octet = [(lax.rem(mine + k, OCTET), device_at((pos[0], pos[1], 0), lax.rem(mine + k, OCTET))) for k in range(1, OCTET)]
    along = [[neighbor(pos, core, dim, k) for k in range(1, RING)] for dim in (1, 0)]
    entry_barrier([device for _, device in octet] + along[0] + along[1])

    def down_copy(layer):
        rows = aligned(down_base(layer) + DOWN_ROWS * (1 - core), DOWN_ROWS)
        return remote(block.at[rows], recv_down.at[layer], send_down.at[layer], got_down.at[layer], partner)

    for layer in range(LAYERS):
        down_copy(layer).start()
    for q in range(OCTET):
        for j in range(UP_ROWS):
            for layer in range(LAYERS):
                stage_up[q, j, pl.ds(layer, 1), :] = block[pl.ds(up_base(layer) + q * UP_ROWS + j, 1), :]

    def up_copy(k):
        to, device = octet[k - 1]
        return remote(stage_up.at[to], recv_up.at[k], send_up.at[k - 1], got_up.at[k - 1], device)

    for k in range(1, OCTET):
        up_copy(k).start()
    recv_up[0] = stage_up[mine]

    total = jnp.zeros((CHUNK, LANES), F32)
    for layer in range(LAYERS):
        down_copy(layer).wait_recv()
        for from_me in (True, False):
            cols = aligned_lanes((core if from_me else 1 - core) * COLS, COLS)
            if from_me:
                part = block[aligned(down_base(layer) + DOWN_ROWS * core, DOWN_ROWS), :]
            else:
                part = recv_down[layer]
            grad = (gacc_down[layer, :, cols] + part) / MICRO_STEPS
            grad_down[layer, :, cols] = grad
            square = grad * grad
            for i in range(COLS // LANES):
                for n in range(COLS // LANES):
                    total = total + square[CHUNK * i:CHUNK * i + CHUNK, LANES * n:LANES * n + LANES]
    total_up = jnp.zeros((LAYERS, LANES), F32)
    for k in range(OCTET):
        if k > 0:
            up_copy(k).wait_recv()
        source = lax.rem(mine + OCTET - k, OCTET)
        cols = aligned_lanes((lax.rem(source, 2) * RING + lax.div(source, 2)) * COLS, COLS)
        for j in range(UP_ROWS):
            grad = (gacc_up[j, :, cols] + recv_up[k, j]) / MICRO_STEPS
            grad_up[j, :, cols] = grad
            square = grad * grad
            for n in range(COLS // LANES):
                total_up = total_up + square[:, LANES * n:LANES * n + LANES]
    norm_send[0] = total + jnp.concatenate([total_up, jnp.zeros((CHUNK - LAYERS, LANES), F32)], axis=0)

    slot = 0
    rounds = ([device for _, device in octet], along[0], along[1])
    sent = []
    for r, peers in enumerate(rounds):
        copies = [
            remote(norm_send.at[r], norm_recv.at[slot + k], send_norm.at[slot + k], got_norm.at[slot + k], device)
            for k, device in enumerate(peers)
        ]
        for copy in copies:
            copy.start()
        total = norm_send[r]
        for k, copy in enumerate(copies):
            copy.wait_recv()
            total = total + norm_recv[slot + k]
        slot += len(peers)
        sent += copies
        if r < 2:
            norm_send[r + 1] = total
    norm_sq = jnp.sum(total, keepdims=True)
    clip_norm = 0.1 * math.sqrt(2 * LAYERS * WIDTH * FF)
    clip = jnp.minimum(1.0, clip_norm / jnp.sqrt(norm_sq))

    for layer in range(LAYERS):
        new = adamw_update(master_down[layer], mom1_down[layer], mom2_down[layer], grad_down[layer] * clip)
        master_down_new[layer], mom1_down_new[layer], mom2_down_new[layer] = new
        weight = new[0].astype(BF16).astype(F32)
        for half in range(LAYERS):
            shard_down[half, layer] = weight[:, half * COLS:half * COLS + COLS]

    def wd_copy(layer):
        rows = aligned(down_base(layer) + DOWN_ROWS * core, DOWN_ROWS)
        return remote(shard_down.at[1 - core, layer], wide.at[rows], send_wd.at[layer], got_wd.at[layer], partner)

    for q in range(OCTET):
        cols = pl.ds(((q % 2) * RING + q // 2) * COLS, COLS)
        for j in range(UP_ROWS):
            new = adamw_update(master_up[j, :, cols], mom1_up[j, :, cols], mom2_up[j, :, cols], grad_up[j, :, cols] * clip)
            master_up_new[j, :, cols], mom1_up_new[j, :, cols], mom2_up_new[j, :, cols] = new
            shard_up[q, j] = new[0].astype(BF16).astype(F32)

    def w_copy(k):
        to, device = octet[k - 1]
        return remote(shard_up.at[to], shard_recv.at[k], send_w.at[k - 1], got_w.at[k - 1], device)

    for layer in range(LAYERS):
        wd_copy(layer).start()
    for k in range(1, OCTET):
        w_copy(k).start()
    shard_recv[0] = shard_up[mine]
    for layer in range(LAYERS):
        wide[aligned(down_base(layer) + DOWN_ROWS * core, DOWN_ROWS), :] = shard_down[core, layer]
    for k in range(OCTET):
        if k > 0:
            w_copy(k).wait_recv()
    for q in range(OCTET):
        behind = lax.rem(mine + OCTET - q, OCTET)
        for j in range(UP_ROWS):
            for layer in range(LAYERS):
                wide[pl.ds(up_base(layer) + q * UP_ROWS + j, 1), :] = shard_recv[behind, j, pl.ds(layer, 1), :]
    for layer in range(LAYERS):
        rows = aligned(down_base(layer) + DOWN_ROWS * (1 - core), DOWN_ROWS)
        remote(shard_down.at[1 - core, layer], wide.at[rows], send_wd.at[layer], got_wd.at[layer], partner).wait_recv()
    new_block[...] = wide[...].astype(BF16)

    for layer in range(LAYERS):
        down_copy(layer).wait_send()
        wd_copy(layer).wait_send()
    for k in range(1, OCTET):
        up_copy(k).wait_send()
        w_copy(k).wait_send()
    for copy in sent:
        copy.wait_send()


UP_SHAPE = (UP_ROWS, LAYERS, FF)
DOWN_SHAPE = (LAYERS, DOWN_ROWS, WIDTH)


def update_rows(block, *arrays):
    up = jax.ShapeDtypeStruct(UP_SHAPE, F32)
    down = jax.ShapeDtypeStruct(DOWN_SHAPE, F32)
    rows = pltpu.VMEM((OCTET, UP_ROWS, LAYERS, COLS), F32)
    seven, two, norm = SEMS((OCTET - 1,)), SEMS((LAYERS,)), SEMS((N_PEERS,))
    return pl.pallas_call(
        update_kernel,
        out_shape=[jax.ShapeDtypeStruct((ROWS, COLS), BF16), up, down, up, down, up, down],
        in_specs=[in_vmem()] * (1 + len(arrays)),
        out_specs=[in_vmem()] * 7,
        scratch_shapes=[
            rows, rows, pltpu.VMEM((LAYERS, DOWN_ROWS, COLS), F32), pltpu.VMEM(UP_SHAPE, F32), pltpu.VMEM(DOWN_SHAPE, F32),
            pltpu.VMEM((3, CHUNK, LANES), F32), pltpu.VMEM((N_PEERS, CHUNK, LANES), F32), pltpu.VMEM((ROWS, COLS), F32),
            rows, rows, pltpu.VMEM((2, LAYERS, DOWN_ROWS, COLS), F32),
            seven, seven, two, two, norm, norm, seven, seven, two, two,
        ],
        compiler_params=comm_params(3),
        name="update_rows",
    )(block, *arrays)


def keep_kernel(*refs):
    half = len(refs) // 2
    for src, dst in zip(refs[:half], refs[half:]):
        dst[...] = src[...]


def keep(arrays):
    return pl.pallas_call(
        keep_kernel,
        out_shape=[jax.ShapeDtypeStruct(a.shape, a.dtype) for a in arrays],
        in_specs=[in_vmem()] * len(arrays),
        out_specs=[in_vmem()] * len(arrays),
        compiler_params=plain_params(0),
        name="keep",
    )(*arrays)


SWAP = [(i, i ^ 1) for i in range(2 * RING * RING * RING)]


def swap_cores(array):
    return lax.ppermute(array, "fsdp", SWAP)


def rows_first(array):
    return jnp.transpose(array, (1, 0, 2))


def local_step(x_saved, grad_out, x_next, w_up, w_down, gacc_up, gacc_down, master_up, master_down, mom1_up, mom1_down, mom2_up, mom2_down):
    core = jnp.reshape(lax.rem(lax.axis_index("fsdp"), 2), (1,))
    x_tokens = x_saved.reshape(LAYERS, -1, WIDTH)
    grad_cur = grad_out.reshape(-1, WIDTH)
    operands = []
    for layer_idx in range(LAYERS - 1, -1, -1):
        x_in = x_tokens[layer_idx]
        pre_act = jnp.dot(x_in, w_up[layer_idx], preferred_element_type=F32)
        hidden_act, gelu_vjp = jax.vjp(gelu_fn, pre_act)
        d_act = lax.dot_general(grad_cur, w_down[layer_idx], (((1,), (1,)), ((), ())), preferred_element_type=F32)
        d_pre = gelu_vjp(d_act)[0].astype(BF16)
        operands.append((x_in, d_pre, hidden_act.astype(BF16), grad_cur))
        if layer_idx > 0:
            grad_cur = (grad_cur.astype(F32) + lax.dot_general(d_pre, w_up[layer_idx], (((1,), (1,)), ((), ())), preferred_element_type=F32)).astype(BF16)
    x_last, d_last, a_last, g_last = operands[0]
    sums = grad_sum(core, x_last, swap_cores(x_last), d_last, swap_cores(d_last), None)
    sums = grad_sum(core, a_last, swap_cores(a_last), g_last, swap_cores(g_last), sums)
    block = reduce_blocks(sums.reshape(RING, RING, RING, PAIR_ROWS, COLS), *operands[1])

    new_block, *state = update_rows(
        block, rows_first(gacc_up), gacc_down, rows_first(master_up), master_down,
        rows_first(mom1_up), mom1_down, rows_first(mom2_up), mom2_down,
    )
    weights, hidden, act = gather_forward(new_block, x_next.reshape(-1, WIDTH))
    weights = weights.reshape(2, RING * RING, RING, N_MATRICES, BLOCK, COLS)
    hidden = last_product(act, weights, hidden)
    master_up, master_down, mom1_up, mom1_down, mom2_up, mom2_down = keep(state)
    return (hidden.reshape(x_next.shape), rows_first(master_up), master_down, rows_first(mom1_up), mom1_down, rows_first(mom2_up), mom2_down)


def solution(mesh):
    rows_spec = P(None, "fsdp")
    return jax.shard_map(local_step, mesh=mesh, in_specs=(rows_spec, P("fsdp"), P("fsdp"), P(), P(), rows_spec, rows_spec, rows_spec, rows_spec, rows_spec, rows_spec, rows_spec, rows_spec), out_specs=(P("fsdp"), rows_spec, rows_spec, rows_spec, rows_spec, rows_spec, rows_spec), check_vma=False)
```

```python
import functools
import math

import jax
import jax.numpy as jnp
from jax import lax
from jax.experimental import pallas as pl
from jax.experimental.pallas import tpu as pltpu
from jax.sharding import PartitionSpec as P

LEARN_RATE = 0.001
BETA_ONE = 0.9
BETA_TWO = 0.95
ADAM_EPS = 1e-8
WEIGHT_DECAY = 0.1
ADAM_STEP = 3
MICRO_STEPS = 2

MESH = pl.DeviceIdType.MESH
BF16 = jnp.bfloat16
F32 = jnp.float32
VMEM_LIMIT = 67_000_000
LAYERS = 2
RING = 4
WIDTH = 1280
FF = 5120
UP_ROWS = 10
DOWN_ROWS = 40
BLOCK = 80
COLS = 640
PAIR_ROWS = 2 * BLOCK
ROWS = LAYERS * PAIR_ROWS
LANES = 128
OCTET = 8
CHUNK = 8
SEMS = pltpu.SemaphoreType.DMA

BATCH_CHUNKS = PAIR_ROWS // CHUNK
ORDERS = ((0, 1, 2), (1, 2, 0), (2, 0, 1))
N_FLOWS = 6
FLOWS = range(N_FLOWS)
TICKS = RING
STEPS = RING - 1
BATCH_LEN = [[TICKS if f // 2 == b else TICKS - 1 for f in FLOWS] for b in range(LAYERS)]
BATCH_START = [[sum(lens[:f]) for f in FLOWS] for lens in BATCH_LEN]
OWN_SLOTS = 3
UP_TILES = 8
TILES = 16


def up_base(layer):
    return (LAYERS - 1 - layer) * PAIR_ROWS


def down_base(layer):
    return up_base(layer) + BLOCK


def comm_params(collective_id):
    return pltpu.CompilerParams(collective_id=collective_id, has_side_effects=True, vmem_limit_bytes=VMEM_LIMIT)


def plain_params(dims):
    return pltpu.CompilerParams(dimension_semantics=("arbitrary",) * dims, vmem_limit_bytes=VMEM_LIMIT)


def in_vmem():
    return pl.BlockSpec(memory_space=pltpu.VMEM)


def in_hbm():
    return pl.BlockSpec(memory_space=pl.ANY)


def aligned(start, size):
    return pl.ds(pl.multiple_of(start, CHUNK), size)


def aligned_lanes(start, size):
    return pl.ds(pl.multiple_of(start, LANES), size)


def remote(src, dst, send, got, device):
    return pltpu.make_async_remote_copy(
        src_ref=src, dst_ref=dst, send_sem=send, recv_sem=got, device_id=(device,), device_id_type=MESH
    )

def flow_dims(flow):
    return ORDERS[flow // 2]


def flow_sign(flow):
    return 1 - 2 * (flow % 2)


def my_place():
    me = lax.axis_index("fsdp")
    core, chip = lax.rem(me, 2), lax.div(me, 2)
    line = lax.div(chip, RING)
    return core, (lax.div(line, RING), lax.rem(line, RING), lax.rem(chip, RING))


def device_at(pos, core):
    return ((pos[0] * RING + pos[1]) * RING + pos[2]) * 2 + core


def neighbor(pos, core, dim, sign):
    moved = list(pos)
    moved[dim] = lax.rem(pos[dim] + RING + sign, RING)
    return device_at(moved, core)


def all_neighbors(pos, core):
    return [neighbor(pos, core, dim, sign) for dim in range(3) for sign in (1, -1)]


def entry_barrier(peers):
    barrier = pltpu.get_barrier_semaphore()
    for peer in peers:
        pl.semaphore_signal(barrier, inc=1, device_id=(peer,), device_id_type=MESH)
    pl.semaphore_wait(barrier, len(peers))


def rounded_product(left, right):
    return lax.dot_general(left, right, (((0,), (0,)), ((), ())), preferred_element_type=F32).astype(BF16).astype(F32)


def reduce_kernel(
    s_last, x_own, d_own, a_own, g_own, out_ref, s_first, x_pair, d_pair, a_pair, g_pair,
    recv1, recv2, recv3, own, left, left_pair, right, right_pair, tile, own_sem, tile_in, tile_out, pair_send, pair_got, credit,
    send1, got1, send2, got2, send3, got3,
):
    core, pos = my_place()
    partner = device_at(pos, 1 - core)
    entry_barrier([partner] + all_neighbors(pos, core))
    target = [[neighbor(pos, core, dim, flow_sign(f)) for dim in flow_dims(f)] for f in FLOWS]
    source = [neighbor(pos, core, flow_dims(f)[0], -flow_sign(f)) for f in FLOWS]
    sums = (s_last, s_first)

    def seg(flow, phase, step):
        at = pos[flow_dims(flow)[phase]]
        return lax.rem(at + 2 * RING - flow_sign(flow) * (1 + step), RING)

    def s_slice(b, flow, j, chunk):
        index = [slice(None)] * 3
        index[flow_dims(flow)[0]] = j
        return sums[b].at[(*index, aligned(chunk * CHUNK, CHUNK), slice(None))]

    def part2(flow, ref, j):
        second, third = flow_dims(flow)[1:]
        return ref.at[j] if second < third else ref.at[:, j]

    def slot1(b, step):
        return step + b * 2 * ((step + 1) // 2)

    def land1(b, step, chunk):
        return recv1.at[slot1(b, step), chunk]

    def land2(b, step, chunk):
        return recv2.at[b, step, chunk]

    def land3(b, step, chunk):
        return recv3.at[b, step, chunk]

    lands, sends, gots = (land1, land2, land3), (send1, send2, send3), (got1, got2, got3)

    def copy(phase, b, flow, step, chunk, src):
        dst = lands[phase](b, step, chunk)
        return remote(dst if src is None else src, dst, sends[phase].at[b, step, chunk], gots[phase].at[b, step, chunk], target[flow][phase])

    def first_copy(phase, b, flow, chunk):
        j = seg(flow, phase, 0)
        if phase == 0:
            src = s_slice(b, flow, j, chunk)
        elif phase == 1:
            src = part2(flow, land1(b, STEPS - 1, chunk), j)
        else:
            src = recv2.at[b, STEPS - 1, chunk, j]
        return copy(phase, b, flow, 0, chunk, src)

    def next_copy(phase, b, flow, step, chunk):
        return copy(phase, b, flow, step + 1, chunk, lands[phase](b, step, chunk))

    def own_copy(b, flow, n):
        step, k = lax.div(n, TICKS), lax.rem(n, TICKS)
        slot = lax.rem(n, OWN_SLOTS)
        src = s_slice(b, flow, seg(flow, 0, step + 1), BATCH_START[b][flow] + k)
        return pltpu.make_async_copy(src, own.at[flow, slot], own_sem.at[flow, slot])

    def start_batch(b):
        for k in range(TICKS):
            for f in FLOWS:
                if k < BATCH_LEN[b][f]:
                    first_copy(0, b, f, BATCH_START[b][f] + k).start()
        for n in range(OWN_SLOTS - 1):
            for f in FLOWS:
                own_copy(b, f, n).start()

    def tick(phase, b, n):
        step, k = lax.div(n, TICKS), lax.rem(n, TICKS)

        def each(body):
            for f in FLOWS:
                if BATCH_LEN[b][f] == TICKS:
                    body(f, BATCH_START[b][f] + k)
                else:
                    pl.when(k < BATCH_LEN[b][f])(functools.partial(body, f, BATCH_START[b][f] + k))

        def add(f, chunk):
            copy(phase, b, f, step, chunk, None).wait_recv()
            landed = lands[phase](b, step, chunk)
            if phase == 0:
                own_copy(b, f, n).wait()
                landed[...] = landed[...] + own[f, lax.rem(n, OWN_SLOTS)]
            elif phase == 1:
                landed[...] = landed[...] + part2(f, land1(b, STEPS - 1, chunk), seg(f, 1, step + 1))[...]
            else:
                landed[...] = landed[...] + recv2[b, STEPS - 1, chunk, seg(f, 2, step + 1)]

        def pass_on(f, chunk):
            @pl.when(step < STEPS - 1)
            def _():
                next_copy(phase, b, f, step, chunk).start()

            @pl.when(step == STEPS - 1)
            def _():
                if phase < 2:
                    first_copy(phase + 1, b, f, chunk).start()
                else:
                    out_ref[aligned((b * BATCH_CHUNKS + chunk) * CHUNK, CHUNK), :] = recv3[b, STEPS - 1, chunk]

        if phase == 0:
            later = n + OWN_SLOTS - 1
            for f in FLOWS:
                @pl.when((later < STEPS * TICKS) & (lax.rem(later, TICKS) < BATCH_LEN[b][f]))
                def _():
                    own_copy(b, f, later).start()

        each(add)
        each(pass_on)

    def tile_reads(job, up):
        slot = lax.rem(job, 2)
        if up:
            rows = aligned_lanes(lax.div(job, RING) * COLS, COLS)
            cols = lax.rem(job, RING) * COLS
            reads = (x_own.at[:, rows], x_pair.at[:, rows], d_own.at[:, aligned_lanes(core * (FF // 2) + cols, COLS)], d_pair.at[:, aligned_lanes(cols, COLS)])
        else:
            rows = aligned_lanes((job - UP_TILES) * COLS, COLS)
            reads = (a_own.at[:, rows], a_pair.at[:, rows], g_own.at[:, aligned_lanes(core * COLS, COLS)], g_pair)
        return [
            pltpu.make_async_copy(src, dst.at[slot], tile_in.at[i, slot])
            for i, (src, dst) in enumerate(zip(reads, (left, left_pair, right, right_pair)))
        ]

    def start_reads(job):
        for up in (True, False):
            @pl.when((job < UP_TILES) if up else (job >= UP_TILES) & (job < TILES))
            def _():
                for read in tile_reads(job, up):
                    read.start()

    def tile_write(job, up):
        slot = lax.rem(job, 2)
        if up:
            dst = s_first.at[pl.ds(lax.div(job, RING) * 2, 2), :, lax.rem(job, RING), pl.ds(0, BLOCK)]
        else:
            i = job - UP_TILES
            dst = s_first.at[lax.div(i, 2), pl.ds(lax.rem(i, 2) * 2, 2), :, pl.ds(BLOCK, BLOCK)]
        return pltpu.make_async_copy(tile.at[slot], dst, tile_out.at[slot])

    def compute(job):
        slot = lax.rem(job, 2)
        start_reads(job + 1)
        for read in tile_reads(UP_TILES + slot, False):
            read.wait()

        @pl.when(job >= 2)
        def _():
            tile_write(UP_TILES + slot, False).wait()

        total = rounded_product(left[slot], right[slot]) + rounded_product(left_pair[slot], right_pair[slot])
        tile[slot] = total.reshape(tile.shape[1:])
        for up in (True, False):
            @pl.when((job < UP_TILES) if up else (job >= UP_TILES))
            def _():
                tile_write(job, up).start()

    start_batch(0)
    other = 1 - core
    gives = (x_own, d_own.at[:, aligned_lanes(other * (FF // 2), FF // 2)], a_own, g_own.at[:, aligned_lanes(other * COLS, COLS)])
    exchange = [
        remote(src, dst, pair_send.at[i], pair_got.at[i], partner)
        for i, (src, dst) in enumerate(zip(gives, (x_pair, d_pair, a_pair, g_pair)))
    ]
    for give in exchange:
        give.start()
    for give in exchange:
        give.wait_recv()
    start_reads(0)

    @pl.loop(0, 2 * TICKS)
    def _(n):
        tick(0, 0, n)

        @pl.loop(0, 2)
        def _(i):
            compute(2 * n + i)

    for slot in range(2):
        tile_write(UP_TILES + slot, False).wait()
    for f in FLOWS:
        for k in range(BATCH_LEN[0][f]):
            copy(0, 0, f, 1, BATCH_START[0][f] + k, None).wait_send()
        pl.semaphore_signal(credit.at[f], inc=1, device_id=(source[f],), device_id_type=MESH)
    for f in FLOWS:
        pl.semaphore_wait(credit.at[f], 1)
    for k in range(TICKS):
        for f in FLOWS:
            if k < BATCH_LEN[1][f]:
                first_copy(0, 1, f, BATCH_START[1][f] + k).start()

    @pl.loop(2 * TICKS, STEPS * TICKS)
    def _(n):
        tick(0, 0, n)

    for n in range(OWN_SLOTS - 1):
        for f in FLOWS:
            own_copy(1, f, n).start()

    @pl.loop(0, STEPS * TICKS)
    def _(n):
        tick(0, 1, n)
        tick(1, 0, n)

    @pl.loop(0, STEPS * TICKS)
    def _(n):
        tick(1, 1, n)
        tick(2, 0, n)

    @pl.loop(0, STEPS * TICKS)
    def _(n):
        tick(2, 1, n)

    for give in exchange:
        give.wait_send()
    for b in range(LAYERS):
        for f in FLOWS:
            @pl.loop(BATCH_START[b][f], BATCH_START[b][f] + BATCH_LEN[b][f])
            def _(chunk):
                for phase in range(3):
                    for step in range(STEPS):
                        if (phase, b, step) != (0, 0, 1):
                            copy(phase, b, f, step, chunk, None).wait_send()


def reduce_blocks(s_last, x_first, d_first, a_first, g_first):
    tokens = x_first.shape[0]

    def half(width):
        return jax.ShapeDtypeStruct((tokens, width), BF16)

    piece = pltpu.VMEM((2, tokens, COLS), BF16)
    sems = SEMS((LAYERS, STEPS, BATCH_CHUNKS))
    return pl.pallas_call(
        reduce_kernel,
        out_shape=[jax.ShapeDtypeStruct((ROWS, COLS), F32), jax.ShapeDtypeStruct(s_last.shape, F32), half(WIDTH), half(FF // 2), half(FF), half(COLS)],
        in_specs=[in_hbm()] * 5,
        out_specs=[in_vmem()] + [in_hbm()] * 5,
        scratch_shapes=[
            pltpu.VMEM((5, BATCH_CHUNKS, RING, RING, CHUNK, COLS), F32),
            pltpu.VMEM((LAYERS, STEPS, BATCH_CHUNKS, RING, CHUNK, COLS), F32),
            pltpu.VMEM((LAYERS, STEPS, BATCH_CHUNKS, CHUNK, COLS), F32),
            pltpu.VMEM((N_FLOWS, OWN_SLOTS, RING, RING, CHUNK, COLS), F32),
            piece, piece, piece, piece,
            pltpu.VMEM((2, 2, RING, BLOCK, COLS), F32),
            SEMS((N_FLOWS, OWN_SLOTS)), SEMS((4, 2)), SEMS((2,)), SEMS((4,)), SEMS((4,)), pltpu.SemaphoreType.REGULAR((N_FLOWS,)),
            sems, sems, sems, sems, sems, sems,
        ],
        compiler_params=comm_params(1),
        name="torus_reduce",
    )(s_last, x_first, d_first, a_first, g_first)[0]


N_MATRICES = 2 * LAYERS
MATRIX_BASE = [base for layer in range(LAYERS) for base in (up_base(layer), down_base(layer))]
SHORT = (2, 1, 0, 2)
MATRIX_LEN = [[CHUNK if f // 2 == SHORT[q] else 2 * CHUNK for f in FLOWS] for q in range(N_MATRICES)]
MATRIX_START = [[MATRIX_BASE[q] + sum(MATRIX_LEN[q][:f]) for f in FLOWS] for q in range(N_MATRICES)]


LINK_ORDER = ((0, 0), (1, 0), (0, 1), (1, 1), (0, 2), (2, 0), (1, 2), (2, 1), (3, 0), (2, 2), (3, 1), (3, 2))
AHEAD = 2


def before(at):
    q, step = LINK_ORDER[at]
    return LINK_ORDER.index((q, step - 1)) if step else -1


GROUP_EVENTS = ((range(0, 6), (0,)), (range(6, 7), ()), (range(7, 8), (1,)), (range(8, 9), ()), (range(9, 11), (2,)), (range(11, 12), ()))
LAST_EVENTS = ()


def gather_kernel(
    block_ref, x_ref, all_ref, hidden_ref, act_ref,
    total, weight, own_sem, load_sem, send1, got1, send2, got2, send3, got3, pair_send, pair_got,
):
    core, pos = my_place()
    partner = device_at(pos, 1 - core)
    entry_barrier([partner] + all_neighbors(pos, core))
    target = [[neighbor(pos, core, dim, flow_sign(f)) for dim in flow_dims(f)] for f in FLOWS]
    pieces = [(q, f) for q in range(N_MATRICES) for f in FLOWS]

    def rows_of(q, flow):
        return pl.ds(MATRIX_START[q][flow], MATRIX_LEN[q][flow])

    def back(flow, phase, steps):
        at = pos[flow_dims(flow)[phase]]
        return lax.rem(at + RING - flow_sign(flow) * steps, RING)

    def place(which, q, flow, *at):
        index = [slice(None)] * 3
        for phase, steps in enumerate(at):
            if steps is not None:
                index[flow_dims(flow)[phase]] = back(flow, phase, steps)
        return all_ref.at[(which, *index, rows_of(q, flow), slice(None))]

    def copy1(q, flow, step, off=0):
        dst = place(core, q, flow, step + off, 0, 0)
        src = dst if off or step else block_ref.at[rows_of(q, flow)]
        return remote(src, dst, send1.at[q, flow, step], got1.at[q, flow, step], target[flow][0])

    def copy2(q, flow, step, off=0):
        ref = place(core, q, flow, None, step + off, 0)
        return remote(ref, ref, send2.at[q, flow, step], got2.at[q, flow, step], target[flow][1])

    def copy3(q, flow, step, off=0):
        ref = place(core, q, flow, None, None, step + off)
        return remote(ref, ref, send3.at[q, flow, step], got3.at[q, flow, step], target[flow][2])

    def pair_copy(q, flow, w, which=core):
        ref = place(which, q, flow, None, None, w)
        return remote(ref, ref, pair_send.at[q, flow, w], pair_got.at[q, flow, w], partner)

    local = pltpu.make_async_copy(block_ref, all_ref.at[core, pos[0], pos[1], pos[2]], own_sem)
    local.start()
    for q, f in pieces:
        copy1(q, f, 0).start()
    local.wait()
    for step in range(STEPS):
        for q, f in pieces:
            copy1(q, f, step, 1).wait_recv()
            if step < STEPS - 1:
                copy1(q, f, step + 1).start()
            else:
                copy2(q, f, 0).start()
    for step in range(STEPS):
        for q, f in pieces:
            copy2(q, f, step, 1).wait_recv()
            if step < STEPS - 1:
                copy2(q, f, step + 1).start()
            elif (q, 0) in LINK_ORDER[:AHEAD]:
                copy3(q, f, 0).start()
    for q, f in pieces:
        pair_copy(q, f, 0).start()

    def arrive(k):
        q, step = LINK_ORDER[k]
        due = [at for at in (k + AHEAD - 1, k + AHEAD) if at < len(LINK_ORDER) and max(at - AHEAD, before(at)) == k]
        for f in FLOWS:
            copy3(q, f, step, 1).wait_recv()
            for at in due:
                copy3(LINK_ORDER[at][0], f, LINK_ORDER[at][1]).start()
        for f in FLOWS:
            pair_copy(q, f, step + 1).start()

    def have_pair(q):
        for f in FLOWS:
            for w in range(RING):
                pair_copy(q, f, w, 1 - core).wait_recv()

    def load(up, layer, i):
        rows = pl.ds(pl.multiple_of(up_base(layer) + (0 if up else BLOCK), CHUNK), BLOCK)
        if up:
            src = all_ref.at[lax.div(i, 2), :, :, pl.ds(lax.rem(i, 2) * 2, 2), rows]
        else:
            src = all_ref.at[:, i, :, :, rows]
        slot = lax.rem(i, 2)
        return pltpu.make_async_copy(src, weight.at[slot].reshape(src.shape), load_sem.at[slot])

    def product(up, i):
        slot = lax.rem(i, 2)
        cols = aligned_lanes(i * WIDTH, WIDTH)
        if up:
            tiles = weight[slot].reshape(RING * RING, 2, BLOCK, COLS)
            wide = jnp.concatenate([tiles[:, x].reshape(WIDTH, COLS) for x in range(2)], axis=1)
            act_ref[:, cols] = gelu_fn(jnp.dot(hidden_ref[...], wide, preferred_element_type=F32)).astype(BF16)
        else:
            tiles = weight[slot].reshape(2, WIDTH, COLS)
            wide = jnp.concatenate([tiles[c] for c in range(2)], axis=1)
            total[...] += jnp.dot(act_ref[:, cols], wide, preferred_element_type=F32)

    hidden_ref[...] = x_ref[...]
    total[...] = x_ref[...].astype(F32)

    @pl.loop(0, len(GROUP_EVENTS))
    def _(group):
        matrix, half = lax.div(group, 2), lax.rem(group, 2)
        layer = lax.div(matrix, 2)
        for g, (events, ready) in enumerate(GROUP_EVENTS):
            @pl.when(group == g)
            def _():
                for k in events:
                    arrive(k)
                for q in ready:
                    have_pair(q)

        for up in (True, False):
            @pl.when((lax.rem(matrix, 2) == 0) == up)
            def _():
                first = half * 2
                load(up, layer, first).start()
                load(up, layer, first + 1).start()

                @pl.loop(first, first + 2)
                def _(i):
                    load(up, layer, i).wait()
                    product(up, i)

                if not up:
                    @pl.when(half == 1)
                    def _():
                        hidden_ref[...] = total[...].astype(BF16)

    for k in LAST_EVENTS:
        arrive(k)
    have_pair(N_MATRICES - 1)
    for q, f in pieces:
        for step in range(STEPS):
            copy1(q, f, step).wait_send()
            copy2(q, f, step).wait_send()
            copy3(q, f, step).wait_send()
        for w in range(RING):
            pair_copy(q, f, w).wait_send()


def gather_forward(block, x_next):
    tokens = x_next.shape[0]
    one = SEMS((N_MATRICES, N_FLOWS, STEPS))
    pair = SEMS((N_MATRICES, N_FLOWS, RING))
    return pl.pallas_call(
        gather_kernel,
        out_shape=[
            jax.ShapeDtypeStruct((2, RING, RING, RING, ROWS, COLS), BF16),
            jax.ShapeDtypeStruct((tokens, WIDTH), BF16),
            jax.ShapeDtypeStruct((tokens, FF), BF16),
        ],
        in_specs=[in_vmem(), in_vmem()],
        out_specs=[in_hbm(), in_vmem(), in_vmem()],
        scratch_shapes=[
            pltpu.VMEM((tokens, WIDTH), F32), pltpu.VMEM((2, 2, RING, RING, BLOCK, COLS), BF16),
            SEMS, SEMS((2,)), one, one, one, one, one, one, pair, pair,
        ],
        compiler_params=comm_params(2),
        name="torus_gather_forward",
    )(block, x_next)


def grad_kernel(core_ref, left, left_pair, right, right_pair, *refs):
    del core_ref
    out = refs[-1]
    total = rounded_product(left[...], right[...]) + rounded_product(left_pair[...], right_pair[...])
    if total.shape[1] == COLS:
        out[...] = total.reshape(out.shape)
    else:
        for x in range(out.shape[1]):
            out[:, x, 0] = total[:, COLS * x:COLS * (x + 1)].reshape(-1, BLOCK, COLS)


def grad_sum(core, left, left_pair, right, right_pair, sums):
    tokens = left.shape[0]
    zy = RING * RING
    if sums is None:
        grid = (2, 2)
        left_spec = pl.BlockSpec((tokens, COLS), lambda i, x, c: (0, i))
        right_spec = pl.BlockSpec((tokens, 2 * COLS), lambda i, x, c: (0, c[0] * 2 + x))
        out_spec = pl.BlockSpec((zy // 2, 2, 1, BLOCK, COLS), lambda i, x, c: (i, x, 0, 0, 0))
    else:
        grid = (FF // COLS,)
        left_spec = pl.BlockSpec((tokens, COLS), lambda i, c: (0, i))
        right_spec = pl.BlockSpec((tokens, COLS), lambda i, c: (0, c[0]))
        out_spec = pl.BlockSpec((2, RING, 1, BLOCK, COLS), lambda i, c: (i, 0, 1, 0, 0))
    before = [] if sums is None else [sums]
    return pl.pallas_call(
        grad_kernel,
        out_shape=jax.ShapeDtypeStruct((zy, RING, 2, BLOCK, COLS), F32),
        grid_spec=pltpu.PrefetchScalarGridSpec(
            num_scalar_prefetch=1,
            grid=grid,
            in_specs=[left_spec, left_spec, right_spec, right_spec] + [in_hbm()] * len(before),
            out_specs=out_spec,
        ),
        input_output_aliases={5: 0} if before else {},
        compiler_params=plain_params(len(grid)),
        cost_estimate=pl.CostEstimate(flops=2 * tokens * WIDTH * FF, bytes_accessed=17_000_000, transcendentals=0),
        name="grad_up" if sums is None else "grad_down",
    )(core, left, left_pair, right, right_pair, *before)


def gelu_fn(pre_act):
    return jax.nn.gelu(pre_act, approximate=True)


def down_kernel(act, weight, hidden, out, total):
    step = pl.program_id(0)

    @pl.when(step == 0)
    def _():
        total[...] = hidden[...].astype(F32)

    wide = jnp.concatenate([weight[c].reshape(WIDTH, COLS) for c in range(2)], axis=1)
    total[...] += jnp.dot(act[...], wide, preferred_element_type=F32)

    @pl.when(step == pl.num_programs(0) - 1)
    def _():
        out[...] = total[...].astype(BF16)


def last_product(act, weights, hidden):
    tokens = hidden.shape[0]
    return pl.pallas_call(
        down_kernel,
        out_shape=jax.ShapeDtypeStruct((tokens, WIDTH), BF16),
        grid=(RING,),
        in_specs=[
            pl.BlockSpec((tokens, WIDTH), lambda i: (0, i)),
            pl.BlockSpec((2, RING, RING, 1, BLOCK, COLS), lambda i: (0, i, 0, 1, 0, 0)),
            pl.BlockSpec((tokens, WIDTH), lambda i: (0, 0)),
        ],
        out_specs=pl.BlockSpec((tokens, WIDTH), lambda i: (0, 0)),
        scratch_shapes=[pltpu.VMEM((tokens, WIDTH), F32)],
        compiler_params=plain_params(1),
        name="forward_down",
    )(act, weights, hidden)


def adamw_update(master_old, mom_one, mom_two, grad_clip):
    mom_one_new = BETA_ONE * mom_one + (1.0 - BETA_ONE) * grad_clip
    mom_two_new = BETA_TWO * mom_two + (1.0 - BETA_TWO) * grad_clip * grad_clip
    first_hat = mom_one_new / (1.0 - BETA_ONE ** ADAM_STEP)
    second_hat = mom_two_new / (1.0 - BETA_TWO ** ADAM_STEP)
    master_new = master_old - LEARN_RATE * (first_hat / (jnp.sqrt(second_hat) + ADAM_EPS) + WEIGHT_DECAY * master_old)
    return master_new, mom_one_new, mom_two_new


N_PEERS = OCTET - 1 + 2 * (RING - 1)


def update_kernel(
    block, gacc_up, gacc_down, master_up, master_down, mom1_up, mom1_down, mom2_up, mom2_down,
    new_block, master_up_new, master_down_new, mom1_up_new, mom1_down_new, mom2_up_new, mom2_down_new,
    stage_up, recv_up, recv_down, grad_up, grad_down, norm_send, norm_recv, wide, shard_up, shard_recv, shard_down,
    send_up, got_up, send_down, got_down, send_norm, got_norm, send_w, got_w, send_wd, got_wd,
):
    core, pos = my_place()
    mine = pos[2] * 2 + core
    partner = device_at(pos, 1 - core)
    octet = [(lax.rem(mine + k, OCTET), device_at((pos[0], pos[1], 0), lax.rem(mine + k, OCTET))) for k in range(1, OCTET)]
    along = [[neighbor(pos, core, dim, k) for k in range(1, RING)] for dim in (1, 0)]
    entry_barrier([device for _, device in octet] + along[0] + along[1])

    def down_copy(layer):
        rows = aligned(down_base(layer) + DOWN_ROWS * (1 - core), DOWN_ROWS)
        return remote(block.at[rows], recv_down.at[layer], send_down.at[layer], got_down.at[layer], partner)

    for layer in range(LAYERS):
        down_copy(layer).start()
    for q in range(OCTET):
        for j in range(UP_ROWS):
            for layer in range(LAYERS):
                stage_up[q, j, pl.ds(layer, 1), :] = block[pl.ds(up_base(layer) + q * UP_ROWS + j, 1), :]

    def up_copy(k):
        to, device = octet[k - 1]
        return remote(stage_up.at[to], recv_up.at[k], send_up.at[k - 1], got_up.at[k - 1], device)

    for k in range(1, OCTET):
        up_copy(k).start()
    recv_up[0] = stage_up[mine]

    total = jnp.zeros((CHUNK, LANES), F32)
    for layer in range(LAYERS):
        down_copy(layer).wait_recv()
        for from_me in (True, False):
            cols = aligned_lanes((core if from_me else 1 - core) * COLS, COLS)
            if from_me:
                part = block[aligned(down_base(layer) + DOWN_ROWS * core, DOWN_ROWS), :]
            else:
                part = recv_down[layer]
            grad = (gacc_down[layer, :, cols] + part) / MICRO_STEPS
            grad_down[layer, :, cols] = grad
            square = grad * grad
            for i in range(COLS // LANES):
                for n in range(COLS // LANES):
                    total = total + square[CHUNK * i:CHUNK * i + CHUNK, LANES * n:LANES * n + LANES]
    total_up = jnp.zeros((LAYERS, LANES), F32)
    for k in range(OCTET):
        if k > 0:
            up_copy(k).wait_recv()
        source = lax.rem(mine + OCTET - k, OCTET)
        cols = aligned_lanes((lax.rem(source, 2) * RING + lax.div(source, 2)) * COLS, COLS)
        for j in range(UP_ROWS):
            grad = (gacc_up[j, :, cols] + recv_up[k, j]) / MICRO_STEPS
            grad_up[j, :, cols] = grad
            square = grad * grad
            for n in range(COLS // LANES):
                total_up = total_up + square[:, LANES * n:LANES * n + LANES]
    norm_send[0] = total + jnp.concatenate([total_up, jnp.zeros((CHUNK - LAYERS, LANES), F32)], axis=0)

    slot = 0
    rounds = ([device for _, device in octet], along[0], along[1])
    sent = []
    for r, peers in enumerate(rounds):
        copies = [
            remote(norm_send.at[r], norm_recv.at[slot + k], send_norm.at[slot + k], got_norm.at[slot + k], device)
            for k, device in enumerate(peers)
        ]
        for copy in copies:
            copy.start()
        total = norm_send[r]
        for k, copy in enumerate(copies):
            copy.wait_recv()
            total = total + norm_recv[slot + k]
        slot += len(peers)
        sent += copies
        if r < 2:
            norm_send[r + 1] = total
    norm_sq = jnp.sum(total, keepdims=True)
    clip_norm = 0.1 * math.sqrt(2 * LAYERS * WIDTH * FF)
    clip = jnp.minimum(1.0, clip_norm / jnp.sqrt(norm_sq))

    for layer in range(LAYERS):
        new = adamw_update(master_down[layer], mom1_down[layer], mom2_down[layer], grad_down[layer] * clip)
        master_down_new[layer], mom1_down_new[layer], mom2_down_new[layer] = new
        weight = new[0].astype(BF16).astype(F32)
        for half in range(LAYERS):
            shard_down[half, layer] = weight[:, half * COLS:half * COLS + COLS]

    def wd_copy(layer):
        rows = aligned(down_base(layer) + DOWN_ROWS * core, DOWN_ROWS)
        return remote(shard_down.at[1 - core, layer], wide.at[rows], send_wd.at[layer], got_wd.at[layer], partner)

    for q in range(OCTET):
        cols = pl.ds(((q % 2) * RING + q // 2) * COLS, COLS)
        for j in range(UP_ROWS):
            new = adamw_update(master_up[j, :, cols], mom1_up[j, :, cols], mom2_up[j, :, cols], grad_up[j, :, cols] * clip)
            master_up_new[j, :, cols], mom1_up_new[j, :, cols], mom2_up_new[j, :, cols] = new
            shard_up[q, j] = new[0].astype(BF16).astype(F32)

    def w_copy(k):
        to, device = octet[k - 1]
        return remote(shard_up.at[to], shard_recv.at[k], send_w.at[k - 1], got_w.at[k - 1], device)

    for layer in range(LAYERS):
        wd_copy(layer).start()
    for k in range(1, OCTET):
        w_copy(k).start()
    shard_recv[0] = shard_up[mine]
    for layer in range(LAYERS):
        wide[aligned(down_base(layer) + DOWN_ROWS * core, DOWN_ROWS), :] = shard_down[core, layer]
    for k in range(OCTET):
        if k > 0:
            w_copy(k).wait_recv()
    for q in range(OCTET):
        behind = lax.rem(mine + OCTET - q, OCTET)
        for j in range(UP_ROWS):
            for layer in range(LAYERS):
                wide[pl.ds(up_base(layer) + q * UP_ROWS + j, 1), :] = shard_recv[behind, j, pl.ds(layer, 1), :]
    for layer in range(LAYERS):
        rows = aligned(down_base(layer) + DOWN_ROWS * (1 - core), DOWN_ROWS)
        remote(shard_down.at[1 - core, layer], wide.at[rows], send_wd.at[layer], got_wd.at[layer], partner).wait_recv()
    new_block[...] = wide[...].astype(BF16)

    for layer in range(LAYERS):
        down_copy(layer).wait_send()
        wd_copy(layer).wait_send()
    for k in range(1, OCTET):
        up_copy(k).wait_send()
        w_copy(k).wait_send()
    for copy in sent:
        copy.wait_send()


UP_SHAPE = (UP_ROWS, LAYERS, FF)
DOWN_SHAPE = (LAYERS, DOWN_ROWS, WIDTH)


def update_rows(block, *arrays):
    up = jax.ShapeDtypeStruct(UP_SHAPE, F32)
    down = jax.ShapeDtypeStruct(DOWN_SHAPE, F32)
    rows = pltpu.VMEM((OCTET, UP_ROWS, LAYERS, COLS), F32)
    seven, two, norm = SEMS((OCTET - 1,)), SEMS((LAYERS,)), SEMS((N_PEERS,))
    return pl.pallas_call(
        update_kernel,
        out_shape=[jax.ShapeDtypeStruct((ROWS, COLS), BF16), up, down, up, down, up, down],
        in_specs=[in_vmem()] * (1 + len(arrays)),
        out_specs=[in_vmem()] * 7,
        scratch_shapes=[
            rows, rows, pltpu.VMEM((LAYERS, DOWN_ROWS, COLS), F32), pltpu.VMEM(UP_SHAPE, F32), pltpu.VMEM(DOWN_SHAPE, F32),
            pltpu.VMEM((3, CHUNK, LANES), F32), pltpu.VMEM((N_PEERS, CHUNK, LANES), F32), pltpu.VMEM((ROWS, COLS), F32),
            rows, rows, pltpu.VMEM((2, LAYERS, DOWN_ROWS, COLS), F32),
            seven, seven, two, two, norm, norm, seven, seven, two, two,
        ],
        compiler_params=comm_params(3),
        name="update_rows",
    )(block, *arrays)


def keep_kernel(*refs):
    half = len(refs) // 2
    for src, dst in zip(refs[:half], refs[half:]):
        dst[...] = src[...]


def keep(arrays):
    return pl.pallas_call(
        keep_kernel,
        out_shape=[jax.ShapeDtypeStruct(a.shape, a.dtype) for a in arrays],
        in_specs=[in_vmem()] * len(arrays),
        out_specs=[in_vmem()] * len(arrays),
        compiler_params=plain_params(0),
        name="keep",
    )(*arrays)


SWAP = [(i, i ^ 1) for i in range(2 * RING * RING * RING)]


def swap_cores(array):
    return lax.ppermute(array, "fsdp", SWAP)


def rows_first(array):
    return jnp.transpose(array, (1, 0, 2))


def local_step(x_saved, grad_out, x_next, w_up, w_down, gacc_up, gacc_down, master_up, master_down, mom1_up, mom1_down, mom2_up, mom2_down):
    core = jnp.reshape(lax.rem(lax.axis_index("fsdp"), 2), (1,))
    x_tokens = x_saved.reshape(LAYERS, -1, WIDTH)
    grad_cur = grad_out.reshape(-1, WIDTH)
    operands = []
    for layer_idx in range(LAYERS - 1, -1, -1):
        x_in = x_tokens[layer_idx]
        pre_act = jnp.dot(x_in, w_up[layer_idx], preferred_element_type=F32)
        hidden_act, gelu_vjp = jax.vjp(gelu_fn, pre_act)
        d_act = lax.dot_general(grad_cur, w_down[layer_idx], (((1,), (1,)), ((), ())), preferred_element_type=F32)
        d_pre = gelu_vjp(d_act)[0].astype(BF16)
        operands.append((x_in, d_pre, hidden_act.astype(BF16), grad_cur))
        if layer_idx > 0:
            grad_cur = (grad_cur.astype(F32) + lax.dot_general(d_pre, w_up[layer_idx], (((1,), (1,)), ((), ())), preferred_element_type=F32)).astype(BF16)
    x_last, d_last, a_last, g_last = operands[0]
    sums = grad_sum(core, x_last, swap_cores(x_last), d_last, swap_cores(d_last), None)
    sums = grad_sum(core, a_last, swap_cores(a_last), g_last, swap_cores(g_last), sums)
    block = reduce_blocks(sums.reshape(RING, RING, RING, PAIR_ROWS, COLS), *operands[1])

    new_block, *state = update_rows(
        block, rows_first(gacc_up), gacc_down, rows_first(master_up), master_down,
        rows_first(mom1_up), mom1_down, rows_first(mom2_up), mom2_down,
    )
    weights, hidden, act = gather_forward(new_block, x_next.reshape(-1, WIDTH))
    weights = weights.reshape(2, RING * RING, RING, N_MATRICES, BLOCK, COLS)
    hidden = last_product(act, weights, hidden)
    master_up, master_down, mom1_up, mom1_down, mom2_up, mom2_down = keep(state)
    return (hidden.reshape(x_next.shape), rows_first(master_up), master_down, rows_first(mom1_up), mom1_down, rows_first(mom2_up), mom2_down)


def solution(mesh):
    rows_spec = P(None, "fsdp")
    return jax.shard_map(local_step, mesh=mesh, in_specs=(rows_spec, P("fsdp"), P("fsdp"), P(), P(), rows_spec, rows_spec, rows_spec, rows_spec, rows_spec, rows_spec, rows_spec, rows_spec), out_specs=(P("fsdp"), rows_spec, rows_spec, rows_spec, rows_spec, rows_spec, rows_spec), check_vma=False)
```

```python
import functools
import math

import jax
import jax.numpy as jnp
from jax import lax
from jax.experimental import pallas as pl
from jax.experimental.pallas import tpu as pltpu
from jax.sharding import PartitionSpec as P

LEARN_RATE = 0.001
BETA_ONE = 0.9
BETA_TWO = 0.95
ADAM_EPS = 1e-8
WEIGHT_DECAY = 0.1
ADAM_STEP = 3
MICRO_STEPS = 2

MESH = pl.DeviceIdType.MESH
BF16 = jnp.bfloat16
F32 = jnp.float32
VMEM_LIMIT = 67_000_000
LAYERS = 2
RING = 4
WIDTH = 1280
FF = 5120
UP_ROWS = 10
DOWN_ROWS = 40
BLOCK = 80
COLS = 640
PAIR_ROWS = 2 * BLOCK
ROWS = LAYERS * PAIR_ROWS
LANES = 128
OCTET = 8
CHUNK = 8
SEMS = pltpu.SemaphoreType.DMA

BATCH_CHUNKS = PAIR_ROWS // CHUNK
ORDERS = ((0, 1, 2), (1, 2, 0), (2, 0, 1))
N_FLOWS = 6
FLOWS = range(N_FLOWS)
TICKS = RING
STEPS = RING - 1
BATCH_LEN = [[TICKS if f // 2 == b else TICKS - 1 for f in FLOWS] for b in range(LAYERS)]
BATCH_START = [[sum(lens[:f]) for f in FLOWS] for lens in BATCH_LEN]
OWN_SLOTS = 2
UP_TILES = 8
TILES = 16
GELU_TICK, SUM_TICK = 2, 6
CARRY_JOBS, GELU_JOBS, SUM_JOBS = 4, 2, 3


def up_base(layer):
    return (LAYERS - 1 - layer) * PAIR_ROWS


def down_base(layer):
    return up_base(layer) + BLOCK


def comm_params(collective_id):
    return pltpu.CompilerParams(collective_id=collective_id, has_side_effects=True, vmem_limit_bytes=VMEM_LIMIT)


def plain_params(dims):
    return pltpu.CompilerParams(dimension_semantics=("arbitrary",) * dims, vmem_limit_bytes=VMEM_LIMIT)


def in_vmem():
    return pl.BlockSpec(memory_space=pltpu.VMEM)


def in_hbm():
    return pl.BlockSpec(memory_space=pl.ANY)


def aligned(start, size):
    return pl.ds(pl.multiple_of(start, CHUNK), size)


def aligned_lanes(start, size):
    return pl.ds(pl.multiple_of(start, LANES), size)


def remote(src, dst, send, got, device):
    return pltpu.make_async_remote_copy(
        src_ref=src, dst_ref=dst, send_sem=send, recv_sem=got, device_id=(device,), device_id_type=MESH
    )

def flow_dims(flow):
    return ORDERS[flow // 2]


def flow_sign(flow):
    return 1 - 2 * (flow % 2)


def my_place():
    me = lax.axis_index("fsdp")
    core, chip = lax.rem(me, 2), lax.div(me, 2)
    line = lax.div(chip, RING)
    return core, (lax.div(line, RING), lax.rem(line, RING), lax.rem(chip, RING))


def device_at(pos, core):
    return ((pos[0] * RING + pos[1]) * RING + pos[2]) * 2 + core


def neighbor(pos, core, dim, sign):
    moved = list(pos)
    moved[dim] = lax.rem(pos[dim] + RING + sign, RING)
    return device_at(moved, core)


def all_neighbors(pos, core):
    return [neighbor(pos, core, dim, sign) for dim in range(3) for sign in (1, -1)]


def entry_barrier(peers):
    barrier = pltpu.get_barrier_semaphore()
    for peer in peers:
        pl.semaphore_signal(barrier, inc=1, device_id=(peer,), device_id_type=MESH)
    pl.semaphore_wait(barrier, len(peers))


def rounded_product(left, right):
    return lax.dot_general(left, right, (((0,), (0,)), ((), ())), preferred_element_type=F32).astype(BF16).astype(F32)


def reduce_kernel(
    s_last, x_own, g_last, d_last, w_up, w_down, out_ref, s_first, x_pair, d_own, d_pair, a_own, a_pair, g_pair,
    recv1, recv2, recv3, own, left, left_pair, right, right_pair, tile, w_tile, w_tile_down, g_own,
    own_sem, tile_in, tile_out, side_send, side_got, act_send, act_got, d_send, d_got, act_out, d_out, credit,
    send1, got1, send2, got2, send3, got3,
):
    core, pos = my_place()
    partner = device_at(pos, 1 - core)
    entry_barrier([partner] + all_neighbors(pos, core))
    target = [[neighbor(pos, core, dim, flow_sign(f)) for dim in flow_dims(f)] for f in FLOWS]
    source = [neighbor(pos, core, flow_dims(f)[0], -flow_sign(f)) for f in FLOWS]
    sums = (s_last, s_first)

    def seg(flow, phase, step):
        at = pos[flow_dims(flow)[phase]]
        return lax.rem(at + 2 * RING - flow_sign(flow) * (1 + step), RING)

    def s_slice(b, flow, j, chunk):
        index = [slice(None)] * 3
        index[flow_dims(flow)[0]] = j
        return sums[b].at[(*index, aligned(chunk * CHUNK, CHUNK), slice(None))]

    def part2(flow, ref, j):
        second, third = flow_dims(flow)[1:]
        return ref.at[j] if second < third else ref.at[:, j]

    def slot1(b, step):
        return step + b * (step // 2)

    def land1(b, step, chunk):
        return recv1.at[slot1(b, step), chunk]

    def land2(b, step, chunk):
        return recv2.at[b, step, chunk]

    def land3(b, step, chunk):
        return recv3.at[b, step, chunk]

    lands, sends, gots = (land1, land2, land3), (send1, send2, send3), (got1, got2, got3)

    def copy(phase, b, flow, step, chunk, src):
        dst = lands[phase](b, step, chunk)
        return remote(dst if src is None else src, dst, sends[phase].at[b, step, chunk], gots[phase].at[b, step, chunk], target[flow][phase])

    def first_copy(phase, b, flow, chunk):
        j = seg(flow, phase, 0)
        if phase == 0:
            src = s_slice(b, flow, j, chunk)
        elif phase == 1:
            src = part2(flow, land1(b, STEPS - 1, chunk), j)
        else:
            src = recv2.at[b, STEPS - 1, chunk, j]
        return copy(phase, b, flow, 0, chunk, src)

    def next_copy(phase, b, flow, step, chunk):
        return copy(phase, b, flow, step + 1, chunk, lands[phase](b, step, chunk))

    def own_copy(b, flow, n):
        step, k = lax.div(n, TICKS), lax.rem(n, TICKS)
        slot = lax.rem(n, OWN_SLOTS)
        src = s_slice(b, flow, seg(flow, 0, step + 1), BATCH_START[b][flow] + k)
        return pltpu.make_async_copy(src, own.at[flow, slot], own_sem.at[flow, slot])

    def start_batch(b):
        for k in range(TICKS):
            for f in FLOWS:
                if k < BATCH_LEN[b][f]:
                    first_copy(0, b, f, BATCH_START[b][f] + k).start()
        for n in range(OWN_SLOTS - 1):
            for f in FLOWS:
                own_copy(b, f, n).start()

    def tick(phase, b, n):
        step, k = lax.div(n, TICKS), lax.rem(n, TICKS)

        def each(body):
            for f in FLOWS:
                if BATCH_LEN[b][f] == TICKS:
                    body(f, BATCH_START[b][f] + k)
                else:
                    pl.when(k < BATCH_LEN[b][f])(functools.partial(body, f, BATCH_START[b][f] + k))

        def add(f, chunk):
            copy(phase, b, f, step, chunk, None).wait_recv()
            landed = lands[phase](b, step, chunk)
            if phase == 0:
                own_copy(b, f, n).wait()
                landed[...] = landed[...] + own[f, lax.rem(n, OWN_SLOTS)]
            elif phase == 1:
                landed[...] = landed[...] + part2(f, land1(b, STEPS - 1, chunk), seg(f, 1, step + 1))[...]
            else:
                landed[...] = landed[...] + recv2[b, STEPS - 1, chunk, seg(f, 2, step + 1)]

        def pass_on(f, chunk):
            @pl.when(step < STEPS - 1)
            def _():
                next_copy(phase, b, f, step, chunk).start()

            @pl.when(step == STEPS - 1)
            def _():
                if phase < 2:
                    first_copy(phase + 1, b, f, chunk).start()
                else:
                    out_ref[aligned((b * BATCH_CHUNKS + chunk) * CHUNK, CHUNK), :] = recv3[b, STEPS - 1, chunk]

        if phase == 0:
            later = n + OWN_SLOTS - 1
            for f in FLOWS:
                @pl.when((later < STEPS * TICKS) & (lax.rem(later, TICKS) < BATCH_LEN[b][f]))
                def _():
                    own_copy(b, f, later).start()

        each(add)
        each(pass_on)

    tokens = x_own.shape[0]
    other = 1 - core

    def back_reads(job, early):
        slot = lax.rem(job, 2)
        if early:
            cols = aligned_lanes(job * COLS, COLS)
            reads = ((w_up.at[LAYERS - 1, :, cols], w_tile), (d_last.at[:, cols], left))
        else:
            cols = aligned_lanes((job - UP_TILES) * COLS, COLS)
            reads = ((w_up.at[0, :, cols], w_tile), (w_down.at[0, cols], w_tile_down))
        return [pltpu.make_async_copy(src, dst.at[slot], tile_in.at[i, slot]) for i, (src, dst) in enumerate(reads)]

    def start_back_reads(job):
        for early in (True, False):
            @pl.when((job < UP_TILES) if early else (job >= UP_TILES) & (job < TILES))
            def _():
                for read in back_reads(job, early):
                    read.start()

    def transposed(lhs, rhs):
        return lax.dot_general(lhs, rhs, (((1,), (1,)), ((), ())), preferred_element_type=F32)

    def carry_gradient(job):
        slot = lax.rem(job, 2)
        start_back_reads(job + 1)
        for read in back_reads(slot, True):
            read.wait()
        for half in range(2):
            at = pl.ds(half * COLS, COLS)
            tile[half, pl.ds(0, tokens)] += transposed(left[slot], w_tile[slot, at])

    def act_copies(i):
        slot, cols = lax.rem(i, 2), aligned_lanes(i * COLS, COLS)
        src = right.at[slot]
        return pltpu.make_async_copy(src, a_own.at[:, cols], act_out.at[slot]), remote(src, a_pair.at[:, cols], act_send.at[slot], act_got.at[i], partner)

    def d_local(i):
        slot = lax.rem(i, 2)
        return pltpu.make_async_copy(right_pair.at[slot], d_own.at[:, aligned_lanes(lax.rem(i, RING) * COLS, COLS)], d_out.at[slot])

    def d_remote(i):
        slot, at = lax.rem(i, 2), lax.rem(i, RING)
        return remote(right_pair.at[slot], d_pair.at[:, aligned_lanes(at * COLS, COLS)], d_send.at[slot], d_got.at[at], partner)

    def wait_back_writes(i):
        own_act, pair_act = act_copies(i)
        own_act.wait()
        pair_act.wait_send()
        mine = lax.div(i, RING) == core

        @pl.when(mine)
        def _():
            d_local(i).wait()

        @pl.when(jnp.logical_not(mine))
        def _():
            d_remote(i).wait_send()

    def through_gelu(i):
        slot = lax.rem(i, 2)
        start_back_reads(i + UP_TILES + 1)
        for read in back_reads(UP_TILES + slot, False):
            read.wait()
        pre_act = jnp.dot(x_own[...], w_tile[slot], preferred_element_type=F32)
        act, gelu_vjp = jax.vjp(gelu_fn, pre_act)
        d_pre = gelu_vjp(transposed(g_own[...], w_tile_down[slot]))[0]

        @pl.when(i >= 2)
        def _():
            wait_back_writes(i - 2)

        right[slot] = act.astype(BF16)
        right_pair[slot] = d_pre.astype(BF16)
        for write in act_copies(i):
            write.start()
        mine = lax.div(i, RING) == core

        @pl.when(mine)
        def _():
            d_local(i).start()

        @pl.when(jnp.logical_not(mine))
        def _():
            d_remote(i).start()

    def tile_reads(job, up):
        slot = lax.rem(job, 2)
        if up:
            rows = aligned_lanes(lax.div(job, RING) * COLS, COLS)
            cols = aligned_lanes(lax.rem(job, RING) * COLS, COLS)
            reads = (x_own.at[:, rows], x_pair.at[:, rows], d_own.at[:, cols], d_pair.at[:, cols])
        else:
            rows = aligned_lanes((job - UP_TILES) * COLS, COLS)
            reads = (a_own.at[:, rows], a_pair.at[:, rows], g_own.at[:, aligned_lanes(core * COLS, COLS)], g_pair)
        return [
            pltpu.make_async_copy(src, dst.at[slot], tile_in.at[i, slot])
            for i, (src, dst) in enumerate(zip(reads, (left, left_pair, right, right_pair)))
        ]

    def start_reads(job):
        for up in (True, False):
            @pl.when((job < UP_TILES) if up else (job >= UP_TILES) & (job < TILES))
            def _():
                for read in tile_reads(job, up):
                    read.start()

    def tile_write(job, up):
        slot = lax.rem(job, 2)
        if up:
            dst = s_first.at[pl.ds(lax.div(job, RING) * 2, 2), :, lax.rem(job, RING), pl.ds(0, BLOCK)]
        else:
            i = job - UP_TILES
            dst = s_first.at[lax.div(i, 2), pl.ds(lax.rem(i, 2) * 2, 2), :, pl.ds(BLOCK, BLOCK)]
        return pltpu.make_async_copy(tile.at[slot].reshape(dst.shape), dst, tile_out.at[slot])

    def compute(job):
        slot = lax.rem(job, 2)
        start_reads(job + 1)
        for read in tile_reads(UP_TILES + slot, False):
            read.wait()

        @pl.when(job >= 2)
        def _():
            tile_write(UP_TILES + slot, False).wait()

        tile[slot] = rounded_product(left[slot], right[slot]) + rounded_product(left_pair[slot], right_pair[slot])
        for up in (True, False):
            @pl.when((job < UP_TILES) if up else (job >= UP_TILES))
            def _():
                tile_write(job, up).start()

    def side_copy(i):
        src, dst = ((x_own, x_pair), (g_own.at[:, aligned_lanes(other * COLS, COLS)], g_pair))[i]
        return remote(src, dst, side_send.at[i], side_got.at[i], partner)

    start_batch(0)
    side_copy(0).start()
    start_back_reads(0)
    for half in range(2):
        tile[half, pl.ds(0, tokens)] = g_last[:, pl.ds(half * COLS, COLS)].astype(F32)

    @pl.loop(0, STEPS * TICKS)
    def _(n):
        tick(0, 0, n)

        @pl.when(n < GELU_TICK)
        def _():
            @pl.loop(0, CARRY_JOBS)
            def _(i):
                carry_gradient(n * CARRY_JOBS + i)

        @pl.when(n == GELU_TICK - 1)
        def _():
            for half in range(2):
                g_own[:, pl.ds(half * COLS, COLS)] = tile[half, pl.ds(0, tokens)].astype(BF16)

        @pl.when((n >= GELU_TICK) & (n < SUM_TICK))
        def _():
            @pl.loop(0, GELU_JOBS)
            def _(i):
                through_gelu((n - GELU_TICK) * GELU_JOBS + i)

        @pl.when(n == GELU_TICK)
        def _():
            side_copy(1).start()

        @pl.when(n == SUM_TICK)
        def _():
            for i in range(2):
                wait_back_writes(UP_TILES - 2 + i)
                side_copy(i).wait_recv()
            for i in range(UP_TILES):
                act_copies(i)[1].wait_recv()
            for i in range(RING):
                d_remote(i).wait_recv()
            start_reads(0)

        @pl.when(n >= SUM_TICK)
        def _():
            @pl.loop(0, SUM_JOBS)
            def _(i):
                job = (n - SUM_TICK) * SUM_JOBS + i
                pl.when(job < TILES)(functools.partial(compute, job))

    for slot in range(2):
        tile_write(UP_TILES + slot, False).wait()
    for f in FLOWS:
        for k in range(BATCH_LEN[0][f]):
            for step in range(1, STEPS):
                copy(0, 0, f, step, BATCH_START[0][f] + k, None).wait_send()
        pl.semaphore_signal(credit.at[f], inc=1, device_id=(source[f],), device_id_type=MESH)
    for f in FLOWS:
        pl.semaphore_wait(credit.at[f], 1)
    start_batch(1)

    @pl.loop(0, STEPS * TICKS)
    def _(n):
        tick(0, 1, n)
        tick(1, 0, n)

    @pl.loop(0, STEPS * TICKS)
    def _(n):
        tick(1, 1, n)
        tick(2, 0, n)

    @pl.loop(0, STEPS * TICKS)
    def _(n):
        tick(2, 1, n)

    for i in range(2):
        side_copy(i).wait_send()
    for b in range(LAYERS):
        for f in FLOWS:
            @pl.loop(BATCH_START[b][f], BATCH_START[b][f] + BATCH_LEN[b][f])
            def _(chunk):
                for phase in range(3):
                    for step in range(STEPS):
                        if step == 0 or phase + b:
                            copy(phase, b, f, step, chunk, None).wait_send()


def reduce_blocks(s_last, x_first, g_last, d_last, w_up, w_down):
    tokens = x_first.shape[0]

    def half(width):
        return jax.ShapeDtypeStruct((tokens, width), BF16)

    piece = pltpu.VMEM((2, tokens, COLS), BF16)
    sems = SEMS((LAYERS, STEPS, BATCH_CHUNKS))
    two, tiles = SEMS((2,)), SEMS((UP_TILES,))
    spaces = [half(WIDTH), half(FF // 2), half(FF // 2), half(FF), half(FF), half(COLS)]
    return pl.pallas_call(
        reduce_kernel,
        out_shape=[jax.ShapeDtypeStruct((ROWS, COLS), F32), jax.ShapeDtypeStruct(s_last.shape, F32)] + spaces,
        in_specs=[in_hbm(), in_vmem(), in_vmem(), in_hbm(), in_hbm(), in_hbm()],
        out_specs=[in_vmem(), in_hbm()] + [in_hbm()] * len(spaces),
        scratch_shapes=[
            pltpu.VMEM((RING, BATCH_CHUNKS, RING, RING, CHUNK, COLS), F32),
            pltpu.VMEM((LAYERS, STEPS, BATCH_CHUNKS, RING, CHUNK, COLS), F32),
            pltpu.VMEM((LAYERS, STEPS, BATCH_CHUNKS, CHUNK, COLS), F32),
            pltpu.VMEM((N_FLOWS, OWN_SLOTS, RING, RING, CHUNK, COLS), F32),
            piece, piece, piece, piece,
            pltpu.VMEM((2, COLS, COLS), F32), pltpu.VMEM((2, WIDTH, COLS), BF16), pltpu.VMEM((2, COLS, WIDTH), BF16),
            pltpu.VMEM((tokens, WIDTH), BF16),
            SEMS((N_FLOWS, OWN_SLOTS)), SEMS((RING, 2)), two, two, two, two, tiles, two, SEMS((RING,)), two, two,
            pltpu.SemaphoreType.REGULAR((N_FLOWS,)),
            sems, sems, sems, sems, sems, sems,
        ],
        compiler_params=comm_params(1),
        name="torus_reduce",
    )(s_last, x_first, g_last, d_last, w_up, w_down)[0]


N_MATRICES = 2 * LAYERS
MATRIX_BASE = [base for layer in range(LAYERS) for base in (up_base(layer), down_base(layer))]
SHORT = (2, 1, 0, 2)
MATRIX_LEN = [[CHUNK if f // 2 == SHORT[q] else 2 * CHUNK for f in FLOWS] for q in range(N_MATRICES)]
MATRIX_START = [[MATRIX_BASE[q] + sum(MATRIX_LEN[q][:f]) for f in FLOWS] for q in range(N_MATRICES)]


LINK_ORDER = ((0, 0), (1, 0), (0, 1), (1, 1), (0, 2), (2, 0), (1, 2), (2, 1), (3, 0), (2, 2), (3, 1), (3, 2))
AHEAD = 2


def before(at):
    q, step = LINK_ORDER[at]
    return LINK_ORDER.index((q, step - 1)) if step else -1


GROUP_EVENTS = ((range(0, 6), (0,)), (range(6, 7), ()), (range(7, 8), (1,)), (range(8, 9), ()), (range(9, 11), (2,)), (range(11, 12), ()))
LAST_EVENTS = ()


def gather_kernel(
    block_ref, x_ref, all_ref, hidden_ref, act_ref,
    total, weight, own_sem, load_sem, send1, got1, send2, got2, send3, got3, pair_send, pair_got,
):
    core, pos = my_place()
    partner = device_at(pos, 1 - core)
    entry_barrier([partner] + all_neighbors(pos, core))
    target = [[neighbor(pos, core, dim, flow_sign(f)) for dim in flow_dims(f)] for f in FLOWS]
    pieces = [(q, f) for q in range(N_MATRICES) for f in FLOWS]

    def rows_of(q, flow):
        return pl.ds(MATRIX_START[q][flow], MATRIX_LEN[q][flow])

    def back(flow, phase, steps):
        at = pos[flow_dims(flow)[phase]]
        return lax.rem(at + RING - flow_sign(flow) * steps, RING)

    def place(which, q, flow, *at):
        index = [slice(None)] * 3
        for phase, steps in enumerate(at):
            if steps is not None:
                index[flow_dims(flow)[phase]] = back(flow, phase, steps)
        return all_ref.at[(which, *index, rows_of(q, flow), slice(None))]

    def copy1(q, flow, step, off=0):
        dst = place(core, q, flow, step + off, 0, 0)
        src = dst if off or step else block_ref.at[rows_of(q, flow)]
        return remote(src, dst, send1.at[q, flow, step], got1.at[q, flow, step], target[flow][0])

    def copy2(q, flow, step, off=0):
        ref = place(core, q, flow, None, step + off, 0)
        return remote(ref, ref, send2.at[q, flow, step], got2.at[q, flow, step], target[flow][1])

    def copy3(q, flow, step, off=0):
        ref = place(core, q, flow, None, None, step + off)
        return remote(ref, ref, send3.at[q, flow, step], got3.at[q, flow, step], target[flow][2])

    def pair_copy(q, flow, w, which=core):
        ref = place(which, q, flow, None, None, w)
        return remote(ref, ref, pair_send.at[q, flow, w], pair_got.at[q, flow, w], partner)

    local = pltpu.make_async_copy(block_ref, all_ref.at[core, pos[0], pos[1], pos[2]], own_sem)
    local.start()
    for q, f in pieces:
        copy1(q, f, 0).start()
    local.wait()
    for step in range(STEPS):
        for q, f in pieces:
            copy1(q, f, step, 1).wait_recv()
            if step < STEPS - 1:
                copy1(q, f, step + 1).start()
            else:
                copy2(q, f, 0).start()
    for step in range(STEPS):
        for q, f in pieces:
            copy2(q, f, step, 1).wait_recv()
            if step < STEPS - 1:
                copy2(q, f, step + 1).start()
            elif (q, 0) in LINK_ORDER[:AHEAD]:
                copy3(q, f, 0).start()
    for q, f in pieces:
        pair_copy(q, f, 0).start()

    def arrive(k):
        q, step = LINK_ORDER[k]
        due = [at for at in (k + AHEAD - 1, k + AHEAD) if at < len(LINK_ORDER) and max(at - AHEAD, before(at)) == k]
        for f in FLOWS:
            copy3(q, f, step, 1).wait_recv()
            for at in due:
                copy3(LINK_ORDER[at][0], f, LINK_ORDER[at][1]).start()
        for f in FLOWS:
            pair_copy(q, f, step + 1).start()

    def have_pair(q):
        for f in FLOWS:
            for w in range(RING):
                pair_copy(q, f, w, 1 - core).wait_recv()

    def load(up, layer, i):
        rows = pl.ds(pl.multiple_of(up_base(layer) + (0 if up else BLOCK), CHUNK), BLOCK)
        if up:
            src = all_ref.at[lax.div(i, 2), :, :, pl.ds(lax.rem(i, 2) * 2, 2), rows]
        else:
            src = all_ref.at[:, i, :, :, rows]
        slot = lax.rem(i, 2)
        return pltpu.make_async_copy(src, weight.at[slot].reshape(src.shape), load_sem.at[slot])

    def product(up, i):
        slot = lax.rem(i, 2)
        cols = aligned_lanes(i * WIDTH, WIDTH)
        if up:
            tiles = weight[slot].reshape(RING * RING, 2, BLOCK, COLS)
            wide = jnp.concatenate([tiles[:, x].reshape(WIDTH, COLS) for x in range(2)], axis=1)
            act_ref[:, cols] = gelu_fn(jnp.dot(hidden_ref[...], wide, preferred_element_type=F32)).astype(BF16)
        else:
            tiles = weight[slot].reshape(2, WIDTH, COLS)
            wide = jnp.concatenate([tiles[c] for c in range(2)], axis=1)
            total[...] += jnp.dot(act_ref[:, cols], wide, preferred_element_type=F32)

    hidden_ref[...] = x_ref[...]
    total[...] = x_ref[...].astype(F32)

    @pl.loop(0, len(GROUP_EVENTS))
    def _(group):
        matrix, half = lax.div(group, 2), lax.rem(group, 2)
        layer = lax.div(matrix, 2)
        for g, (events, ready) in enumerate(GROUP_EVENTS):
            @pl.when(group == g)
            def _():
                for k in events:
                    arrive(k)
                for q in ready:
                    have_pair(q)

        for up in (True, False):
            @pl.when((lax.rem(matrix, 2) == 0) == up)
            def _():
                first = half * 2
                load(up, layer, first).start()
                load(up, layer, first + 1).start()

                @pl.loop(first, first + 2)
                def _(i):
                    load(up, layer, i).wait()
                    product(up, i)

                if not up:
                    @pl.when(half == 1)
                    def _():
                        hidden_ref[...] = total[...].astype(BF16)

    for k in LAST_EVENTS:
        arrive(k)
    have_pair(N_MATRICES - 1)
    for q, f in pieces:
        for step in range(STEPS):
            copy1(q, f, step).wait_send()
            copy2(q, f, step).wait_send()
            copy3(q, f, step).wait_send()
        for w in range(RING):
            pair_copy(q, f, w).wait_send()


def gather_forward(block, x_next):
    tokens = x_next.shape[0]
    one = SEMS((N_MATRICES, N_FLOWS, STEPS))
    pair = SEMS((N_MATRICES, N_FLOWS, RING))
    return pl.pallas_call(
        gather_kernel,
        out_shape=[
            jax.ShapeDtypeStruct((2, RING, RING, RING, ROWS, COLS), BF16),
            jax.ShapeDtypeStruct((tokens, WIDTH), BF16),
            jax.ShapeDtypeStruct((tokens, FF), BF16),
        ],
        in_specs=[in_vmem(), in_vmem()],
        out_specs=[in_hbm(), in_vmem(), in_vmem()],
        scratch_shapes=[
            pltpu.VMEM((tokens, WIDTH), F32), pltpu.VMEM((2, 2, RING, RING, BLOCK, COLS), BF16),
            SEMS, SEMS((2,)), one, one, one, one, one, one, pair, pair,
        ],
        compiler_params=comm_params(2),
        name="torus_gather_forward",
    )(block, x_next)


def grad_kernel(core_ref, left, left_pair, right, right_pair, *refs):
    del core_ref
    out = refs[-1]
    total = rounded_product(left[...], right[...]) + rounded_product(left_pair[...], right_pair[...])
    if total.shape[1] == COLS:
        out[...] = total.reshape(out.shape)
    else:
        for x in range(out.shape[1]):
            out[:, x, 0] = total[:, COLS * x:COLS * (x + 1)].reshape(-1, BLOCK, COLS)


def grad_sum(core, left, left_pair, right, right_pair, sums, up):
    tokens = left.shape[0]
    zy = RING * RING
    if up:
        grid = (2, 2)
        left_spec = pl.BlockSpec((tokens, COLS), lambda i, x, c: (0, i))
        right_spec = pl.BlockSpec((tokens, 2 * COLS), lambda i, x, c: (0, c[0] * 2 + x))
        out_spec = pl.BlockSpec((zy // 2, 2, 1, BLOCK, COLS), lambda i, x, c: (i, x, 0, 0, 0))
    else:
        grid = (FF // COLS,)
        left_spec = pl.BlockSpec((tokens, COLS), lambda i, c: (0, i))
        right_spec = pl.BlockSpec((tokens, COLS), lambda i, c: (0, c[0]))
        out_spec = pl.BlockSpec((2, RING, 1, BLOCK, COLS), lambda i, c: (i, 0, 1, 0, 0))
    before = [] if sums is None else [sums]
    return pl.pallas_call(
        grad_kernel,
        out_shape=jax.ShapeDtypeStruct((zy, RING, 2, BLOCK, COLS), F32),
        grid_spec=pltpu.PrefetchScalarGridSpec(
            num_scalar_prefetch=1,
            grid=grid,
            in_specs=[left_spec, left_spec, right_spec, right_spec] + [in_hbm()] * len(before),
            out_specs=out_spec,
        ),
        input_output_aliases={5: 0} if before else {},
        compiler_params=plain_params(len(grid)),
        cost_estimate=pl.CostEstimate(flops=2 * tokens * WIDTH * FF, bytes_accessed=17_000_000, transcendentals=0),
        name="grad_up" if up else "grad_down",
    )(core, left, left_pair, right, right_pair, *before)


def gelu_fn(pre_act):
    return jax.nn.gelu(pre_act, approximate=True)


def down_kernel(act, weight, hidden, out, total):
    step = pl.program_id(0)

    @pl.when(step == 0)
    def _():
        total[...] = hidden[...].astype(F32)

    wide = jnp.concatenate([weight[c].reshape(WIDTH, COLS) for c in range(2)], axis=1)
    total[...] += jnp.dot(act[...], wide, preferred_element_type=F32)

    @pl.when(step == pl.num_programs(0) - 1)
    def _():
        out[...] = total[...].astype(BF16)


def last_product(act, weights, hidden):
    tokens = hidden.shape[0]
    return pl.pallas_call(
        down_kernel,
        out_shape=jax.ShapeDtypeStruct((tokens, WIDTH), BF16),
        grid=(RING,),
        in_specs=[
            pl.BlockSpec((tokens, WIDTH), lambda i: (0, i)),
            pl.BlockSpec((2, RING, RING, 1, BLOCK, COLS), lambda i: (0, i, 0, 1, 0, 0)),
            pl.BlockSpec((tokens, WIDTH), lambda i: (0, 0)),
        ],
        out_specs=pl.BlockSpec((tokens, WIDTH), lambda i: (0, 0)),
        scratch_shapes=[pltpu.VMEM((tokens, WIDTH), F32)],
        compiler_params=plain_params(1),
        name="forward_down",
    )(act, weights, hidden)


def adamw_update(master_old, mom_one, mom_two, grad_clip):
    mom_one_new = BETA_ONE * mom_one + (1.0 - BETA_ONE) * grad_clip
    mom_two_new = BETA_TWO * mom_two + (1.0 - BETA_TWO) * grad_clip * grad_clip
    first_hat = mom_one_new / (1.0 - BETA_ONE ** ADAM_STEP)
    second_hat = mom_two_new / (1.0 - BETA_TWO ** ADAM_STEP)
    master_new = master_old - LEARN_RATE * (first_hat / (jnp.sqrt(second_hat) + ADAM_EPS) + WEIGHT_DECAY * master_old)
    return master_new, mom_one_new, mom_two_new


N_PEERS = OCTET - 1 + 2 * (RING - 1)


def update_kernel(
    block, gacc_up, gacc_down, master_up, master_down, mom1_up, mom1_down, mom2_up, mom2_down,
    new_block, master_up_new, master_down_new, mom1_up_new, mom1_down_new, mom2_up_new, mom2_down_new,
    stage_up, recv_up, recv_down, grad_up, grad_down, norm_send, norm_recv, wide, shard_up, shard_recv, shard_down,
    send_up, got_up, send_down, got_down, send_norm, got_norm, send_w, got_w, send_wd, got_wd,
):
    core, pos = my_place()
    mine = pos[2] * 2 + core
    partner = device_at(pos, 1 - core)
    octet = [(lax.rem(mine + k, OCTET), device_at((pos[0], pos[1], 0), lax.rem(mine + k, OCTET))) for k in range(1, OCTET)]
    along = [[neighbor(pos, core, dim, k) for k in range(1, RING)] for dim in (1, 0)]
    entry_barrier([device for _, device in octet] + along[0] + along[1])

    def down_copy(layer):
        rows = aligned(down_base(layer) + DOWN_ROWS * (1 - core), DOWN_ROWS)
        return remote(block.at[rows], recv_down.at[layer], send_down.at[layer], got_down.at[layer], partner)

    for layer in range(LAYERS):
        down_copy(layer).start()
    for q in range(OCTET):
        for j in range(UP_ROWS):
            for layer in range(LAYERS):
                stage_up[q, j, pl.ds(layer, 1), :] = block[pl.ds(up_base(layer) + q * UP_ROWS + j, 1), :]

    def up_copy(k):
        to, device = octet[k - 1]
        return remote(stage_up.at[to], recv_up.at[k], send_up.at[k - 1], got_up.at[k - 1], device)

    for k in range(1, OCTET):
        up_copy(k).start()
    recv_up[0] = stage_up[mine]

    total = jnp.zeros((CHUNK, LANES), F32)
    for layer in range(LAYERS):
        down_copy(layer).wait_recv()
        for from_me in (True, False):
            cols = aligned_lanes((core if from_me else 1 - core) * COLS, COLS)
            if from_me:
                part = block[aligned(down_base(layer) + DOWN_ROWS * core, DOWN_ROWS), :]
            else:
                part = recv_down[layer]
            grad = (gacc_down[layer, :, cols] + part) / MICRO_STEPS
            grad_down[layer, :, cols] = grad
            square = grad * grad
            for i in range(COLS // LANES):
                for n in range(COLS // LANES):
                    total = total + square[CHUNK * i:CHUNK * i + CHUNK, LANES * n:LANES * n + LANES]
    total_up = jnp.zeros((LAYERS, LANES), F32)
    for k in range(OCTET):
        if k > 0:
            up_copy(k).wait_recv()
        source = lax.rem(mine + OCTET - k, OCTET)
        cols = aligned_lanes((lax.rem(source, 2) * RING + lax.div(source, 2)) * COLS, COLS)
        for j in range(UP_ROWS):
            grad = (gacc_up[j, :, cols] + recv_up[k, j]) / MICRO_STEPS
            grad_up[j, :, cols] = grad
            square = grad * grad
            for n in range(COLS // LANES):
                total_up = total_up + square[:, LANES * n:LANES * n + LANES]
    norm_send[0] = total + jnp.concatenate([total_up, jnp.zeros((CHUNK - LAYERS, LANES), F32)], axis=0)

    slot = 0
    rounds = ([device for _, device in octet], along[0], along[1])
    sent = []
    for r, peers in enumerate(rounds):
        copies = [
            remote(norm_send.at[r], norm_recv.at[slot + k], send_norm.at[slot + k], got_norm.at[slot + k], device)
            for k, device in enumerate(peers)
        ]
        for copy in copies:
            copy.start()
        total = norm_send[r]
        for k, copy in enumerate(copies):
            copy.wait_recv()
            total = total + norm_recv[slot + k]
        slot += len(peers)
        sent += copies
        if r < 2:
            norm_send[r + 1] = total
    norm_sq = jnp.sum(total, keepdims=True)
    clip_norm = 0.1 * math.sqrt(2 * LAYERS * WIDTH * FF)
    clip = jnp.minimum(1.0, clip_norm / jnp.sqrt(norm_sq))

    for layer in range(LAYERS):
        new = adamw_update(master_down[layer], mom1_down[layer], mom2_down[layer], grad_down[layer] * clip)
        master_down_new[layer], mom1_down_new[layer], mom2_down_new[layer] = new
        weight = new[0].astype(BF16).astype(F32)
        for half in range(LAYERS):
            shard_down[half, layer] = weight[:, half * COLS:half * COLS + COLS]

    def wd_copy(layer):
        rows = aligned(down_base(layer) + DOWN_ROWS * core, DOWN_ROWS)
        return remote(shard_down.at[1 - core, layer], wide.at[rows], send_wd.at[layer], got_wd.at[layer], partner)

    for q in range(OCTET):
        cols = pl.ds(((q % 2) * RING + q // 2) * COLS, COLS)
        for j in range(UP_ROWS):
            new = adamw_update(master_up[j, :, cols], mom1_up[j, :, cols], mom2_up[j, :, cols], grad_up[j, :, cols] * clip)
            master_up_new[j, :, cols], mom1_up_new[j, :, cols], mom2_up_new[j, :, cols] = new
            shard_up[q, j] = new[0].astype(BF16).astype(F32)

    def w_copy(k):
        to, device = octet[k - 1]
        return remote(shard_up.at[to], shard_recv.at[k], send_w.at[k - 1], got_w.at[k - 1], device)

    for layer in range(LAYERS):
        wd_copy(layer).start()
    for k in range(1, OCTET):
        w_copy(k).start()
    shard_recv[0] = shard_up[mine]
    for layer in range(LAYERS):
        wide[aligned(down_base(layer) + DOWN_ROWS * core, DOWN_ROWS), :] = shard_down[core, layer]
    for k in range(OCTET):
        if k > 0:
            w_copy(k).wait_recv()
    for q in range(OCTET):
        behind = lax.rem(mine + OCTET - q, OCTET)
        for j in range(UP_ROWS):
            for layer in range(LAYERS):
                wide[pl.ds(up_base(layer) + q * UP_ROWS + j, 1), :] = shard_recv[behind, j, pl.ds(layer, 1), :]
    for layer in range(LAYERS):
        rows = aligned(down_base(layer) + DOWN_ROWS * (1 - core), DOWN_ROWS)
        remote(shard_down.at[1 - core, layer], wide.at[rows], send_wd.at[layer], got_wd.at[layer], partner).wait_recv()
    new_block[...] = wide[...].astype(BF16)

    for layer in range(LAYERS):
        down_copy(layer).wait_send()
        wd_copy(layer).wait_send()
    for k in range(1, OCTET):
        up_copy(k).wait_send()
        w_copy(k).wait_send()
    for copy in sent:
        copy.wait_send()


UP_SHAPE = (UP_ROWS, LAYERS, FF)
DOWN_SHAPE = (LAYERS, DOWN_ROWS, WIDTH)


def update_rows(block, *arrays):
    up = jax.ShapeDtypeStruct(UP_SHAPE, F32)
    down = jax.ShapeDtypeStruct(DOWN_SHAPE, F32)
    rows = pltpu.VMEM((OCTET, UP_ROWS, LAYERS, COLS), F32)
    seven, two, norm = SEMS((OCTET - 1,)), SEMS((LAYERS,)), SEMS((N_PEERS,))
    return pl.pallas_call(
        update_kernel,
        out_shape=[jax.ShapeDtypeStruct((ROWS, COLS), BF16), up, down, up, down, up, down],
        in_specs=[in_vmem()] * (1 + len(arrays)),
        out_specs=[in_vmem()] * 7,
        scratch_shapes=[
            rows, rows, pltpu.VMEM((LAYERS, DOWN_ROWS, COLS), F32), pltpu.VMEM(UP_SHAPE, F32), pltpu.VMEM(DOWN_SHAPE, F32),
            pltpu.VMEM((3, CHUNK, LANES), F32), pltpu.VMEM((N_PEERS, CHUNK, LANES), F32), pltpu.VMEM((ROWS, COLS), F32),
            rows, rows, pltpu.VMEM((2, LAYERS, DOWN_ROWS, COLS), F32),
            seven, seven, two, two, norm, norm, seven, seven, two, two,
        ],
        compiler_params=comm_params(3),
        name="update_rows",
    )(block, *arrays)


def keep_kernel(*refs):
    half = len(refs) // 2
    for src, dst in zip(refs[:half], refs[half:]):
        dst[...] = src[...]


def keep(arrays):
    return pl.pallas_call(
        keep_kernel,
        out_shape=[jax.ShapeDtypeStruct(a.shape, a.dtype) for a in arrays],
        in_specs=[in_vmem()] * len(arrays),
        out_specs=[in_vmem()] * len(arrays),
        compiler_params=plain_params(0),
        name="keep",
    )(*arrays)


SWAP = [(i, i ^ 1) for i in range(2 * RING * RING * RING)]


def swap_cores(array):
    return lax.ppermute(array, "fsdp", SWAP)


def rows_first(array):
    return jnp.transpose(array, (1, 0, 2))


def local_step(x_saved, grad_out, x_next, w_up, w_down, gacc_up, gacc_down, master_up, master_down, mom1_up, mom1_down, mom2_up, mom2_down):
    core = jnp.reshape(lax.rem(lax.axis_index("fsdp"), 2), (1,))
    x_tokens = x_saved.reshape(LAYERS, -1, WIDTH)
    grad_last = grad_out.reshape(-1, WIDTH)
    x_last = x_tokens[LAYERS - 1]
    pre_act = jnp.dot(x_last, w_up[LAYERS - 1], preferred_element_type=F32)
    hidden_act, gelu_vjp = jax.vjp(gelu_fn, pre_act)
    act_last = hidden_act.astype(BF16)
    d_act = lax.dot_general(grad_last, w_down[LAYERS - 1], (((1,), (1,)), ((), ())), preferred_element_type=F32)
    d_last = gelu_vjp(d_act)[0].astype(BF16)
    sums = grad_sum(core, act_last, swap_cores(act_last), grad_last, swap_cores(grad_last), None, False)
    sums = grad_sum(core, x_last, swap_cores(x_last), d_last, swap_cores(d_last), sums, True)
    block = reduce_blocks(sums.reshape(RING, RING, RING, PAIR_ROWS, COLS), x_tokens[0], grad_last, d_last, w_up, w_down)

    new_block, *state = update_rows(
        block, rows_first(gacc_up), gacc_down, rows_first(master_up), master_down,
        rows_first(mom1_up), mom1_down, rows_first(mom2_up), mom2_down,
    )
    weights, hidden, act = gather_forward(new_block, x_next.reshape(-1, WIDTH))
    weights = weights.reshape(2, RING * RING, RING, N_MATRICES, BLOCK, COLS)
    hidden = last_product(act, weights, hidden)
    master_up, master_down, mom1_up, mom1_down, mom2_up, mom2_down = keep(state)
    return (hidden.reshape(x_next.shape), rows_first(master_up), master_down, rows_first(mom1_up), mom1_down, rows_first(mom2_up), mom2_down)


def solution(mesh):
    rows_spec = P(None, "fsdp")
    return jax.shard_map(local_step, mesh=mesh, in_specs=(rows_spec, P("fsdp"), P("fsdp"), P(), P(), rows_spec, rows_spec, rows_spec, rows_spec, rows_spec, rows_spec, rows_spec, rows_spec), out_specs=(P("fsdp"), rows_spec, rows_spec, rows_spec, rows_spec, rows_spec, rows_spec), check_vma=False)
```

```python
import functools
import math

import jax
import jax.numpy as jnp
from jax import lax
from jax.experimental import pallas as pl
from jax.experimental.pallas import tpu as pltpu
from jax.sharding import PartitionSpec as P

LEARN_RATE = 0.001
BETA_ONE = 0.9
BETA_TWO = 0.95
ADAM_EPS = 1e-8
WEIGHT_DECAY = 0.1
ADAM_STEP = 3
MICRO_STEPS = 2

MESH = pl.DeviceIdType.MESH
BF16 = jnp.bfloat16
F32 = jnp.float32
VMEM_LIMIT = 67_000_000
LAYERS = 2
RING = 4
WIDTH = 1280
FF = 5120
UP_ROWS = 10
DOWN_ROWS = 40
BLOCK = 80
COLS = 640
PAIR_ROWS = 2 * BLOCK
ROWS = LAYERS * PAIR_ROWS
LANES = 128
OCTET = 8
CHUNK = 8
SEMS = pltpu.SemaphoreType.DMA

BATCH_CHUNKS = PAIR_ROWS // CHUNK
ORDERS = ((0, 1, 2), (1, 2, 0), (2, 0, 1))
N_FLOWS = 6
FLOWS = range(N_FLOWS)
TICKS = RING
STEPS = RING - 1
BATCH_LEN = [[TICKS if f // 2 == b else TICKS - 1 for f in FLOWS] for b in range(LAYERS)]
BATCH_START = [[sum(lens[:f]) for f in FLOWS] for lens in BATCH_LEN]
OWN_SLOTS = 2
UP_TILES = 8
TILES = 16
GELU_TICK, SUM_TICK = 2, 6
CARRY_JOBS, GELU_JOBS = 4, 2


def up_base(layer):
    return (LAYERS - 1 - layer) * PAIR_ROWS


def down_base(layer):
    return up_base(layer) + BLOCK


def comm_params(collective_id):
    return pltpu.CompilerParams(collective_id=collective_id, has_side_effects=True, vmem_limit_bytes=VMEM_LIMIT)


def plain_params(dims):
    return pltpu.CompilerParams(dimension_semantics=("arbitrary",) * dims, vmem_limit_bytes=VMEM_LIMIT)


def in_vmem():
    return pl.BlockSpec(memory_space=pltpu.VMEM)


def in_hbm():
    return pl.BlockSpec(memory_space=pl.ANY)


def aligned(start, size):
    return pl.ds(pl.multiple_of(start, CHUNK), size)


def aligned_lanes(start, size):
    return pl.ds(pl.multiple_of(start, LANES), size)


def remote(src, dst, send, got, device):
    return pltpu.make_async_remote_copy(
        src_ref=src, dst_ref=dst, send_sem=send, recv_sem=got, device_id=(device,), device_id_type=MESH
    )

def flow_dims(flow):
    return ORDERS[flow // 2]


def flow_sign(flow):
    return 1 - 2 * (flow % 2)


def my_place():
    me = lax.axis_index("fsdp")
    core, chip = lax.rem(me, 2), lax.div(me, 2)
    line = lax.div(chip, RING)
    return core, (lax.div(line, RING), lax.rem(line, RING), lax.rem(chip, RING))


def device_at(pos, core):
    return ((pos[0] * RING + pos[1]) * RING + pos[2]) * 2 + core


def neighbor(pos, core, dim, sign):
    moved = list(pos)
    moved[dim] = lax.rem(pos[dim] + RING + sign, RING)
    return device_at(moved, core)


def all_neighbors(pos, core):
    return [neighbor(pos, core, dim, sign) for dim in range(3) for sign in (1, -1)]


def entry_barrier(peers):
    barrier = pltpu.get_barrier_semaphore()
    for peer in peers:
        pl.semaphore_signal(barrier, inc=1, device_id=(peer,), device_id_type=MESH)
    pl.semaphore_wait(barrier, len(peers))


def rounded_product(left, right):
    return lax.dot_general(left, right, (((0,), (0,)), ((), ())), preferred_element_type=F32).astype(BF16).astype(F32)


def reduce_kernel(
    s_last, x_own, g_last, d_last, w_up, w_down, out_ref, s_first, x_pair, d_own, d_pair, a_own, a_pair, g_pair,
    recv1, recv2, recv3, own, left, left_pair, right, right_pair, tile, w_tile, w_tile_down, g_own,
    own_sem, tile_in, tile_out, side_send, side_got, act_send, act_got, d_send, d_got, act_out, d_out, credit,
    send1, got1, send2, got2, send3, got3,
):
    core, pos = my_place()
    partner = device_at(pos, 1 - core)
    entry_barrier([partner] + all_neighbors(pos, core))
    target = [[neighbor(pos, core, dim, flow_sign(f)) for dim in flow_dims(f)] for f in FLOWS]
    source = [neighbor(pos, core, flow_dims(f)[0], -flow_sign(f)) for f in FLOWS]
    sums = (s_last, s_first)

    def seg(flow, phase, step):
        at = pos[flow_dims(flow)[phase]]
        return lax.rem(at + 2 * RING - flow_sign(flow) * (1 + step), RING)

    def s_slice(b, flow, j, chunk):
        index = [slice(None)] * 3
        index[flow_dims(flow)[0]] = j
        return sums[b].at[(*index, aligned(chunk * CHUNK, CHUNK), slice(None))]

    def part2(flow, ref, j):
        second, third = flow_dims(flow)[1:]
        return ref.at[j] if second < third else ref.at[:, j]

    def slot1(b, step):
        return step + b * (step // 2)

    def land1(b, step, chunk):
        return recv1.at[slot1(b, step), chunk]

    def land2(b, step, chunk):
        return recv2.at[b, step, chunk]

    def land3(b, step, chunk):
        return recv3.at[b, step, chunk]

    lands, sends, gots = (land1, land2, land3), (send1, send2, send3), (got1, got2, got3)

    def copy(phase, b, flow, step, chunk, src):
        dst = lands[phase](b, step, chunk)
        return remote(dst if src is None else src, dst, sends[phase].at[b, step, chunk], gots[phase].at[b, step, chunk], target[flow][phase])

    def first_copy(phase, b, flow, chunk):
        j = seg(flow, phase, 0)
        if phase == 0:
            src = s_slice(b, flow, j, chunk)
        elif phase == 1:
            src = part2(flow, land1(b, STEPS - 1, chunk), j)
        else:
            src = recv2.at[b, STEPS - 1, chunk, j]
        return copy(phase, b, flow, 0, chunk, src)

    def next_copy(phase, b, flow, step, chunk):
        return copy(phase, b, flow, step + 1, chunk, lands[phase](b, step, chunk))

    def own_copy(b, flow, n):
        step, k = lax.div(n, TICKS), lax.rem(n, TICKS)
        slot = lax.rem(n, OWN_SLOTS)
        src = s_slice(b, flow, seg(flow, 0, step + 1), BATCH_START[b][flow] + k)
        return pltpu.make_async_copy(src, own.at[flow, slot], own_sem.at[flow, slot])

    def start_batch(b):
        for k in range(TICKS):
            for f in FLOWS:
                if k < BATCH_LEN[b][f]:
                    first_copy(0, b, f, BATCH_START[b][f] + k).start()
        for n in range(OWN_SLOTS - 1):
            for f in FLOWS:
                own_copy(b, f, n).start()

    def tick(phase, b, n):
        step, k = lax.div(n, TICKS), lax.rem(n, TICKS)

        def each(body):
            for f in FLOWS:
                if BATCH_LEN[b][f] == TICKS:
                    body(f, BATCH_START[b][f] + k)
                else:
                    pl.when(k < BATCH_LEN[b][f])(functools.partial(body, f, BATCH_START[b][f] + k))

        def add(f, chunk):
            copy(phase, b, f, step, chunk, None).wait_recv()
            landed = lands[phase](b, step, chunk)
            if phase == 0:
                own_copy(b, f, n).wait()
                landed[...] = landed[...] + own[f, lax.rem(n, OWN_SLOTS)]
            elif phase == 1:
                landed[...] = landed[...] + part2(f, land1(b, STEPS - 1, chunk), seg(f, 1, step + 1))[...]
            else:
                landed[...] = landed[...] + recv2[b, STEPS - 1, chunk, seg(f, 2, step + 1)]

        def pass_on(f, chunk):
            @pl.when(step < STEPS - 1)
            def _():
                next_copy(phase, b, f, step, chunk).start()

            @pl.when(step == STEPS - 1)
            def _():
                if phase < 2:
                    first_copy(phase + 1, b, f, chunk).start()
                else:
                    out_ref[aligned((b * BATCH_CHUNKS + chunk) * CHUNK, CHUNK), :] = recv3[b, STEPS - 1, chunk]

        if phase == 0:
            later = n + OWN_SLOTS - 1
            for f in FLOWS:
                @pl.when((later < STEPS * TICKS) & (lax.rem(later, TICKS) < BATCH_LEN[b][f]))
                def _():
                    own_copy(b, f, later).start()

        each(add)
        each(pass_on)

    tokens = x_own.shape[0]
    other = 1 - core

    def back_reads(job, early):
        slot = lax.rem(job, 2)
        if early:
            cols = aligned_lanes(job * COLS, COLS)
            reads = ((w_up.at[LAYERS - 1, :, cols], w_tile), (d_last.at[:, cols], left))
        else:
            cols = aligned_lanes((job - UP_TILES) * COLS, COLS)
            reads = ((w_up.at[0, :, cols], w_tile), (w_down.at[0, cols], w_tile_down))
        return [pltpu.make_async_copy(src, dst.at[slot], tile_in.at[i, slot]) for i, (src, dst) in enumerate(reads)]

    def start_back_reads(job):
        for early in (True, False):
            @pl.when((job < UP_TILES) if early else (job >= UP_TILES) & (job < TILES))
            def _():
                for read in back_reads(job, early):
                    read.start()

    def transposed(lhs, rhs):
        return lax.dot_general(lhs, rhs, (((1,), (1,)), ((), ())), preferred_element_type=F32)

    def carry_gradient(job):
        slot = lax.rem(job, 2)
        start_back_reads(job + 1)
        for read in back_reads(slot, True):
            read.wait()
        for half in range(2):
            at = pl.ds(half * COLS, COLS)
            tile[half, pl.ds(0, tokens)] += transposed(left[slot], w_tile[slot, at])

    def act_copies(i):
        slot, cols = lax.rem(i, 2), aligned_lanes(i * COLS, COLS)
        src = right.at[slot]
        return pltpu.make_async_copy(src, a_own.at[:, cols], act_out.at[slot]), remote(src, a_pair.at[:, cols], act_send.at[slot], act_got.at[i], partner)

    def d_local(i):
        slot = lax.rem(i, 2)
        return pltpu.make_async_copy(right_pair.at[slot], d_own.at[:, aligned_lanes(lax.rem(i, RING) * COLS, COLS)], d_out.at[slot])

    def d_remote(i):
        slot, at = lax.rem(i, 2), lax.rem(i, RING)
        return remote(right_pair.at[slot], d_pair.at[:, aligned_lanes(at * COLS, COLS)], d_send.at[slot], d_got.at[at], partner)

    def wait_back_writes(i):
        own_act, pair_act = act_copies(i)
        own_act.wait()
        pair_act.wait_send()
        mine = lax.div(i, RING) == core

        @pl.when(mine)
        def _():
            d_local(i).wait()

        @pl.when(jnp.logical_not(mine))
        def _():
            d_remote(i).wait_send()

    def through_gelu(i):
        slot = lax.rem(i, 2)
        start_back_reads(i + UP_TILES + 1)
        for read in back_reads(UP_TILES + slot, False):
            read.wait()
        pre_act = jnp.dot(x_own[...], w_tile[slot], preferred_element_type=F32)
        act, gelu_vjp = jax.vjp(gelu_fn, pre_act)
        d_pre = gelu_vjp(transposed(g_own[...], w_tile_down[slot]))[0]

        @pl.when(i >= 2)
        def _():
            wait_back_writes(i - 2)

        right[slot] = act.astype(BF16)
        right_pair[slot] = d_pre.astype(BF16)
        for write in act_copies(i):
            write.start()
        mine = lax.div(i, RING) == core

        @pl.when(mine)
        def _():
            d_local(i).start()

        @pl.when(jnp.logical_not(mine))
        def _():
            d_remote(i).start()

    def tile_reads(job, up):
        slot = lax.rem(job, 2)
        if up:
            rows = aligned_lanes(lax.div(job, RING) * COLS, COLS)
            cols = aligned_lanes(lax.rem(job, RING) * COLS, COLS)
            reads = (x_own.at[:, rows], x_pair.at[:, rows], d_own.at[:, cols], d_pair.at[:, cols])
        else:
            rows = aligned_lanes((job - UP_TILES) * COLS, COLS)
            reads = (a_own.at[:, rows], a_pair.at[:, rows], g_own.at[:, aligned_lanes(core * COLS, COLS)], g_pair)
        return [
            pltpu.make_async_copy(src, dst.at[slot], tile_in.at[i, slot])
            for i, (src, dst) in enumerate(zip(reads, (left, left_pair, right, right_pair)))
        ]

    def start_reads(job):
        for up in (True, False):
            @pl.when((job < UP_TILES) if up else (job >= UP_TILES) & (job < TILES))
            def _():
                for read in tile_reads(job, up):
                    read.start()

    def tile_write(job, up):
        slot = lax.rem(job, 2)
        if up:
            dst = s_first.at[pl.ds(lax.div(job, RING) * 2, 2), :, lax.rem(job, RING), pl.ds(0, BLOCK)]
        else:
            i = job - UP_TILES
            dst = s_first.at[lax.div(i, 2), pl.ds(lax.rem(i, 2) * 2, 2), :, pl.ds(BLOCK, BLOCK)]
        return pltpu.make_async_copy(tile.at[slot].reshape(dst.shape), dst, tile_out.at[slot])

    def compute(job):
        slot = lax.rem(job, 2)
        start_reads(job + 1)
        for read in tile_reads(UP_TILES + slot, False):
            read.wait()

        @pl.when(job >= 2)
        def _():
            tile_write(UP_TILES + slot, False).wait()

        tile[slot] = rounded_product(left[slot], right[slot]) + rounded_product(left_pair[slot], right_pair[slot])
        for up in (True, False):
            @pl.when((job < UP_TILES) if up else (job >= UP_TILES))
            def _():
                tile_write(job, up).start()

    def side_copy(i):
        src, dst = ((x_own, x_pair), (g_own.at[:, aligned_lanes(other * COLS, COLS)], g_pair))[i]
        return remote(src, dst, side_send.at[i], side_got.at[i], partner)

    start_batch(0)
    side_copy(0).start()
    start_back_reads(0)
    for half in range(2):
        tile[half, pl.ds(0, tokens)] = g_last[:, pl.ds(half * COLS, COLS)].astype(F32)

    @pl.loop(0, STEPS * TICKS)
    def _(n):
        tick(0, 0, n)

        @pl.when(n < GELU_TICK)
        def _():
            @pl.loop(0, CARRY_JOBS)
            def _(i):
                carry_gradient(n * CARRY_JOBS + i)

        @pl.when(n == GELU_TICK - 1)
        def _():
            for half in range(2):
                g_own[:, pl.ds(half * COLS, COLS)] = tile[half, pl.ds(0, tokens)].astype(BF16)

        @pl.when((n >= GELU_TICK) & (n < SUM_TICK))
        def _():
            @pl.loop(0, GELU_JOBS)
            def _(i):
                through_gelu((n - GELU_TICK) * GELU_JOBS + i)

        @pl.when(n == GELU_TICK)
        def _():
            side_copy(1).start()

        @pl.when(n == SUM_TICK)
        def _():
            for i in range(2):
                wait_back_writes(UP_TILES - 2 + i)
                side_copy(i).wait_recv()
            for i in range(UP_TILES):
                act_copies(i)[1].wait_recv()
            for i in range(RING):
                d_remote(i).wait_recv()
            start_reads(0)

        @pl.when(n >= SUM_TICK)
        def _():
            compute(n - SUM_TICK)

    for f in FLOWS:
        for k in range(BATCH_LEN[0][f]):
            for step in range(1, STEPS):
                copy(0, 0, f, step, BATCH_START[0][f] + k, None).wait_send()
        pl.semaphore_signal(credit.at[f], inc=1, device_id=(source[f],), device_id_type=MESH)

    @pl.loop(0, STEPS * TICKS)
    def _(n):
        tick(1, 0, n)
        job = n + STEPS * TICKS - SUM_TICK
        pl.when(job < TILES)(functools.partial(compute, job))

    for slot in range(2):
        tile_write(UP_TILES + slot, False).wait()
    for f in FLOWS:
        pl.semaphore_wait(credit.at[f], 1)
    start_batch(1)

    @pl.loop(0, STEPS * TICKS)
    def _(n):
        tick(0, 1, n)
        tick(2, 0, n)

    @pl.loop(0, STEPS * TICKS)
    def _(n):
        tick(1, 1, n)

    @pl.loop(0, STEPS * TICKS)
    def _(n):
        tick(2, 1, n)

    for i in range(2):
        side_copy(i).wait_send()
    for b in range(LAYERS):
        for f in FLOWS:
            @pl.loop(BATCH_START[b][f], BATCH_START[b][f] + BATCH_LEN[b][f])
            def _(chunk):
                for phase in range(3):
                    for step in range(STEPS):
                        if step == 0 or phase + b:
                            copy(phase, b, f, step, chunk, None).wait_send()


def reduce_blocks(s_last, x_first, g_last, d_last, w_up, w_down):
    tokens = x_first.shape[0]

    def half(width):
        return jax.ShapeDtypeStruct((tokens, width), BF16)

    piece = pltpu.VMEM((2, tokens, COLS), BF16)
    sems = SEMS((LAYERS, STEPS, BATCH_CHUNKS))
    two, tiles = SEMS((2,)), SEMS((UP_TILES,))
    spaces = [half(WIDTH), half(FF // 2), half(FF // 2), half(FF), half(FF), half(COLS)]
    return pl.pallas_call(
        reduce_kernel,
        out_shape=[jax.ShapeDtypeStruct((ROWS, COLS), F32), jax.ShapeDtypeStruct(s_last.shape, F32)] + spaces,
        in_specs=[in_hbm(), in_vmem(), in_vmem(), in_hbm(), in_hbm(), in_hbm()],
        out_specs=[in_vmem(), in_hbm()] + [in_hbm()] * len(spaces),
        scratch_shapes=[
            pltpu.VMEM((RING, BATCH_CHUNKS, RING, RING, CHUNK, COLS), F32),
            pltpu.VMEM((LAYERS, STEPS, BATCH_CHUNKS, RING, CHUNK, COLS), F32),
            pltpu.VMEM((LAYERS, STEPS, BATCH_CHUNKS, CHUNK, COLS), F32),
            pltpu.VMEM((N_FLOWS, OWN_SLOTS, RING, RING, CHUNK, COLS), F32),
            piece, piece, piece, piece,
            pltpu.VMEM((2, COLS, COLS), F32), pltpu.VMEM((2, WIDTH, COLS), BF16), pltpu.VMEM((2, COLS, WIDTH), BF16),
            pltpu.VMEM((tokens, WIDTH), BF16),
            SEMS((N_FLOWS, OWN_SLOTS)), SEMS((RING, 2)), two, two, two, two, tiles, two, SEMS((RING,)), two, two,
            pltpu.SemaphoreType.REGULAR((N_FLOWS,)),
            sems, sems, sems, sems, sems, sems,
        ],
        compiler_params=comm_params(1),
        name="torus_reduce",
    )(s_last, x_first, g_last, d_last, w_up, w_down)[0]


N_MATRICES = 2 * LAYERS
MATRIX_BASE = [base for layer in range(LAYERS) for base in (up_base(layer), down_base(layer))]
SHORT = (2, 1, 0, 2)
MATRIX_LEN = [[CHUNK if f // 2 == SHORT[q] else 2 * CHUNK for f in FLOWS] for q in range(N_MATRICES)]
MATRIX_START = [[MATRIX_BASE[q] + sum(MATRIX_LEN[q][:f]) for f in FLOWS] for q in range(N_MATRICES)]


LINK_ORDER = ((0, 0), (1, 0), (0, 1), (1, 1), (0, 2), (2, 0), (1, 2), (2, 1), (3, 0), (2, 2), (3, 1), (3, 2))
AHEAD = 2


def before(at):
    q, step = LINK_ORDER[at]
    return LINK_ORDER.index((q, step - 1)) if step else -1


GROUP_EVENTS = ((range(0, 6), (0,)), (range(6, 7), ()), (range(7, 8), (1,)), (range(8, 9), ()), (range(9, 11), (2,)), (range(11, 12), ()))
LAST_EVENTS = ()


def gather_kernel(
    block_ref, x_ref, all_ref, hidden_ref, act_ref,
    total, weight, own_sem, load_sem, send1, got1, send2, got2, send3, got3, pair_send, pair_got,
):
    core, pos = my_place()
    partner = device_at(pos, 1 - core)
    entry_barrier([partner] + all_neighbors(pos, core))
    target = [[neighbor(pos, core, dim, flow_sign(f)) for dim in flow_dims(f)] for f in FLOWS]
    pieces = [(q, f) for q in range(N_MATRICES) for f in FLOWS]

    def rows_of(q, flow):
        return pl.ds(MATRIX_START[q][flow], MATRIX_LEN[q][flow])

    def back(flow, phase, steps):
        at = pos[flow_dims(flow)[phase]]
        return lax.rem(at + RING - flow_sign(flow) * steps, RING)

    def place(which, q, flow, *at):
        index = [slice(None)] * 3
        for phase, steps in enumerate(at):
            if steps is not None:
                index[flow_dims(flow)[phase]] = back(flow, phase, steps)
        return all_ref.at[(which, *index, rows_of(q, flow), slice(None))]

    def copy1(q, flow, step, off=0):
        dst = place(core, q, flow, step + off, 0, 0)
        src = dst if off or step else block_ref.at[rows_of(q, flow)]
        return remote(src, dst, send1.at[q, flow, step], got1.at[q, flow, step], target[flow][0])

    def copy2(q, flow, step, off=0):
        ref = place(core, q, flow, None, step + off, 0)
        return remote(ref, ref, send2.at[q, flow, step], got2.at[q, flow, step], target[flow][1])

    def copy3(q, flow, step, off=0):
        ref = place(core, q, flow, None, None, step + off)
        return remote(ref, ref, send3.at[q, flow, step], got3.at[q, flow, step], target[flow][2])

    def pair_copy(q, flow, w, which=core):
        ref = place(which, q, flow, None, None, w)
        return remote(ref, ref, pair_send.at[q, flow, w], pair_got.at[q, flow, w], partner)

    local = pltpu.make_async_copy(block_ref, all_ref.at[core, pos[0], pos[1], pos[2]], own_sem)
    local.start()
    for q, f in pieces:
        copy1(q, f, 0).start()
    local.wait()
    for step in range(STEPS):
        for q, f in pieces:
            copy1(q, f, step, 1).wait_recv()
            if step < STEPS - 1:
                copy1(q, f, step + 1).start()
            else:
                copy2(q, f, 0).start()
    for step in range(STEPS):
        for q, f in pieces:
            copy2(q, f, step, 1).wait_recv()
            if step < STEPS - 1:
                copy2(q, f, step + 1).start()
            elif (q, 0) in LINK_ORDER[:AHEAD]:
                copy3(q, f, 0).start()
    for q, f in pieces:
        pair_copy(q, f, 0).start()

    def arrive(k):
        q, step = LINK_ORDER[k]
        due = [at for at in (k + AHEAD - 1, k + AHEAD) if at < len(LINK_ORDER) and max(at - AHEAD, before(at)) == k]
        for f in FLOWS:
            copy3(q, f, step, 1).wait_recv()
            for at in due:
                copy3(LINK_ORDER[at][0], f, LINK_ORDER[at][1]).start()
        for f in FLOWS:
            pair_copy(q, f, step + 1).start()

    def have_pair(q):
        for f in FLOWS:
            for w in range(RING):
                pair_copy(q, f, w, 1 - core).wait_recv()

    def load(up, layer, i):
        rows = pl.ds(pl.multiple_of(up_base(layer) + (0 if up else BLOCK), CHUNK), BLOCK)
        if up:
            src = all_ref.at[lax.div(i, 2), :, :, pl.ds(lax.rem(i, 2) * 2, 2), rows]
        else:
            src = all_ref.at[:, i, :, :, rows]
        slot = lax.rem(i, 2)
        return pltpu.make_async_copy(src, weight.at[slot].reshape(src.shape), load_sem.at[slot])

    def product(up, i):
        slot = lax.rem(i, 2)
        cols = aligned_lanes(i * WIDTH, WIDTH)
        if up:
            tiles = weight[slot].reshape(RING * RING, 2, BLOCK, COLS)
            wide = jnp.concatenate([tiles[:, x].reshape(WIDTH, COLS) for x in range(2)], axis=1)
            act_ref[:, cols] = gelu_fn(jnp.dot(hidden_ref[...], wide, preferred_element_type=F32)).astype(BF16)
        else:
            tiles = weight[slot].reshape(2, WIDTH, COLS)
            wide = jnp.concatenate([tiles[c] for c in range(2)], axis=1)
            total[...] += jnp.dot(act_ref[:, cols], wide, preferred_element_type=F32)

    hidden_ref[...] = x_ref[...]
    total[...] = x_ref[...].astype(F32)

    @pl.loop(0, len(GROUP_EVENTS))
    def _(group):
        matrix, half = lax.div(group, 2), lax.rem(group, 2)
        layer = lax.div(matrix, 2)
        for g, (events, ready) in enumerate(GROUP_EVENTS):
            @pl.when(group == g)
            def _():
                for k in events:
                    arrive(k)
                for q in ready:
                    have_pair(q)

        for up in (True, False):
            @pl.when((lax.rem(matrix, 2) == 0) == up)
            def _():
                first = half * 2
                load(up, layer, first).start()
                load(up, layer, first + 1).start()

                @pl.loop(first, first + 2)
                def _(i):
                    load(up, layer, i).wait()
                    product(up, i)

                if not up:
                    @pl.when(half == 1)
                    def _():
                        hidden_ref[...] = total[...].astype(BF16)

    for k in LAST_EVENTS:
        arrive(k)
    have_pair(N_MATRICES - 1)
    for q, f in pieces:
        for step in range(STEPS):
            copy1(q, f, step).wait_send()
            copy2(q, f, step).wait_send()
            copy3(q, f, step).wait_send()
        for w in range(RING):
            pair_copy(q, f, w).wait_send()


def gather_forward(block, x_next):
    tokens = x_next.shape[0]
    one = SEMS((N_MATRICES, N_FLOWS, STEPS))
    pair = SEMS((N_MATRICES, N_FLOWS, RING))
    return pl.pallas_call(
        gather_kernel,
        out_shape=[
            jax.ShapeDtypeStruct((2, RING, RING, RING, ROWS, COLS), BF16),
            jax.ShapeDtypeStruct((tokens, WIDTH), BF16),
            jax.ShapeDtypeStruct((tokens, FF), BF16),
        ],
        in_specs=[in_vmem(), in_vmem()],
        out_specs=[in_hbm(), in_vmem(), in_vmem()],
        scratch_shapes=[
            pltpu.VMEM((tokens, WIDTH), F32), pltpu.VMEM((2, 2, RING, RING, BLOCK, COLS), BF16),
            SEMS, SEMS((2,)), one, one, one, one, one, one, pair, pair,
        ],
        compiler_params=comm_params(2),
        name="torus_gather_forward",
    )(block, x_next)


def grad_kernel(core_ref, left, left_pair, right, right_pair, *refs):
    del core_ref
    out = refs[-1]
    total = rounded_product(left[...], right[...]) + rounded_product(left_pair[...], right_pair[...])
    if total.shape[1] == COLS:
        out[...] = total.reshape(out.shape)
    else:
        for x in range(out.shape[1]):
            out[:, x, 0] = total[:, COLS * x:COLS * (x + 1)].reshape(-1, BLOCK, COLS)


def grad_sum(core, left, left_pair, right, right_pair, sums, up):
    tokens = left.shape[0]
    zy = RING * RING
    if up:
        grid = (2, 2)
        left_spec = pl.BlockSpec((tokens, COLS), lambda i, x, c: (0, i))
        right_spec = pl.BlockSpec((tokens, 2 * COLS), lambda i, x, c: (0, c[0] * 2 + x))
        out_spec = pl.BlockSpec((zy // 2, 2, 1, BLOCK, COLS), lambda i, x, c: (i, x, 0, 0, 0))
    else:
        grid = (FF // COLS,)
        left_spec = pl.BlockSpec((tokens, COLS), lambda i, c: (0, i))
        right_spec = pl.BlockSpec((tokens, COLS), lambda i, c: (0, c[0]))
        out_spec = pl.BlockSpec((2, RING, 1, BLOCK, COLS), lambda i, c: (i, 0, 1, 0, 0))
    before = [] if sums is None else [sums]
    return pl.pallas_call(
        grad_kernel,
        out_shape=jax.ShapeDtypeStruct((zy, RING, 2, BLOCK, COLS), F32),
        grid_spec=pltpu.PrefetchScalarGridSpec(
            num_scalar_prefetch=1,
            grid=grid,
            in_specs=[left_spec, left_spec, right_spec, right_spec] + [in_hbm()] * len(before),
            out_specs=out_spec,
        ),
        input_output_aliases={5: 0} if before else {},
        compiler_params=plain_params(len(grid)),
        cost_estimate=pl.CostEstimate(flops=2 * tokens * WIDTH * FF, bytes_accessed=17_000_000, transcendentals=0),
        name="grad_up" if up else "grad_down",
    )(core, left, left_pair, right, right_pair, *before)


def gelu_fn(pre_act):
    return jax.nn.gelu(pre_act, approximate=True)


def down_kernel(act, weight, hidden, out, total):
    step = pl.program_id(0)

    @pl.when(step == 0)
    def _():
        total[...] = hidden[...].astype(F32)

    wide = jnp.concatenate([weight[c].reshape(WIDTH, COLS) for c in range(2)], axis=1)
    total[...] += jnp.dot(act[...], wide, preferred_element_type=F32)

    @pl.when(step == pl.num_programs(0) - 1)
    def _():
        out[...] = total[...].astype(BF16)


def last_product(act, weights, hidden):
    tokens = hidden.shape[0]
    return pl.pallas_call(
        down_kernel,
        out_shape=jax.ShapeDtypeStruct((tokens, WIDTH), BF16),
        grid=(RING,),
        in_specs=[
            pl.BlockSpec((tokens, WIDTH), lambda i: (0, i)),
            pl.BlockSpec((2, RING, RING, 1, BLOCK, COLS), lambda i: (0, i, 0, 1, 0, 0)),
            pl.BlockSpec((tokens, WIDTH), lambda i: (0, 0)),
        ],
        out_specs=pl.BlockSpec((tokens, WIDTH), lambda i: (0, 0)),
        scratch_shapes=[pltpu.VMEM((tokens, WIDTH), F32)],
        compiler_params=plain_params(1),
        name="forward_down",
    )(act, weights, hidden)


def adamw_update(master_old, mom_one, mom_two, grad_clip):
    mom_one_new = BETA_ONE * mom_one + (1.0 - BETA_ONE) * grad_clip
    mom_two_new = BETA_TWO * mom_two + (1.0 - BETA_TWO) * grad_clip * grad_clip
    first_hat = mom_one_new / (1.0 - BETA_ONE ** ADAM_STEP)
    second_hat = mom_two_new / (1.0 - BETA_TWO ** ADAM_STEP)
    master_new = master_old - LEARN_RATE * (first_hat / (jnp.sqrt(second_hat) + ADAM_EPS) + WEIGHT_DECAY * master_old)
    return master_new, mom_one_new, mom_two_new


N_PEERS = OCTET - 1 + 2 * (RING - 1)


def update_kernel(
    block, gacc_up, gacc_down, master_up, master_down, mom1_up, mom1_down, mom2_up, mom2_down,
    new_block, master_up_new, master_down_new, mom1_up_new, mom1_down_new, mom2_up_new, mom2_down_new,
    stage_up, recv_up, recv_down, grad_up, grad_down, norm_send, norm_recv, wide, shard_up, shard_recv, shard_down,
    send_up, got_up, send_down, got_down, send_norm, got_norm, send_w, got_w, send_wd, got_wd,
):
    core, pos = my_place()
    mine = pos[2] * 2 + core
    partner = device_at(pos, 1 - core)
    octet = [(lax.rem(mine + k, OCTET), device_at((pos[0], pos[1], 0), lax.rem(mine + k, OCTET))) for k in range(1, OCTET)]
    along = [[neighbor(pos, core, dim, k) for k in range(1, RING)] for dim in (1, 0)]
    entry_barrier([device for _, device in octet] + along[0] + along[1])

    def down_copy(layer):
        rows = aligned(down_base(layer) + DOWN_ROWS * (1 - core), DOWN_ROWS)
        return remote(block.at[rows], recv_down.at[layer], send_down.at[layer], got_down.at[layer], partner)

    for layer in range(LAYERS):
        down_copy(layer).start()
    for q in range(OCTET):
        for j in range(UP_ROWS):
            for layer in range(LAYERS):
                stage_up[q, j, pl.ds(layer, 1), :] = block[pl.ds(up_base(layer) + q * UP_ROWS + j, 1), :]

    def up_copy(k):
        to, device = octet[k - 1]
        return remote(stage_up.at[to], recv_up.at[k], send_up.at[k - 1], got_up.at[k - 1], device)

    for k in range(1, OCTET):
        up_copy(k).start()
    recv_up[0] = stage_up[mine]

    total = jnp.zeros((CHUNK, LANES), F32)
    for layer in range(LAYERS):
        down_copy(layer).wait_recv()
        for from_me in (True, False):
            cols = aligned_lanes((core if from_me else 1 - core) * COLS, COLS)
            if from_me:
                part = block[aligned(down_base(layer) + DOWN_ROWS * core, DOWN_ROWS), :]
            else:
                part = recv_down[layer]
            grad = (gacc_down[layer, :, cols] + part) / MICRO_STEPS
            grad_down[layer, :, cols] = grad
            square = grad * grad
            for i in range(COLS // LANES):
                for n in range(COLS // LANES):
                    total = total + square[CHUNK * i:CHUNK * i + CHUNK, LANES * n:LANES * n + LANES]
    total_up = jnp.zeros((LAYERS, LANES), F32)
    for k in range(OCTET):
        if k > 0:
            up_copy(k).wait_recv()
        source = lax.rem(mine + OCTET - k, OCTET)
        cols = aligned_lanes((lax.rem(source, 2) * RING + lax.div(source, 2)) * COLS, COLS)
        for j in range(UP_ROWS):
            grad = (gacc_up[j, :, cols] + recv_up[k, j]) / MICRO_STEPS
            grad_up[j, :, cols] = grad
            square = grad * grad
            for n in range(COLS // LANES):
                total_up = total_up + square[:, LANES * n:LANES * n + LANES]
    norm_send[0] = total + jnp.concatenate([total_up, jnp.zeros((CHUNK - LAYERS, LANES), F32)], axis=0)

    slot = 0
    rounds = ([device for _, device in octet], along[0], along[1])
    sent = []
    for r, peers in enumerate(rounds):
        copies = [
            remote(norm_send.at[r], norm_recv.at[slot + k], send_norm.at[slot + k], got_norm.at[slot + k], device)
            for k, device in enumerate(peers)
        ]
        for copy in copies:
            copy.start()
        total = norm_send[r]
        for k, copy in enumerate(copies):
            copy.wait_recv()
            total = total + norm_recv[slot + k]
        slot += len(peers)
        sent += copies
        if r < 2:
            norm_send[r + 1] = total
    norm_sq = jnp.sum(total, keepdims=True)
    clip_norm = 0.1 * math.sqrt(2 * LAYERS * WIDTH * FF)
    clip = jnp.minimum(1.0, clip_norm / jnp.sqrt(norm_sq))

    for layer in range(LAYERS):
        new = adamw_update(master_down[layer], mom1_down[layer], mom2_down[layer], grad_down[layer] * clip)
        master_down_new[layer], mom1_down_new[layer], mom2_down_new[layer] = new
        weight = new[0].astype(BF16).astype(F32)
        for half in range(LAYERS):
            shard_down[half, layer] = weight[:, half * COLS:half * COLS + COLS]

    def wd_copy(layer):
        rows = aligned(down_base(layer) + DOWN_ROWS * core, DOWN_ROWS)
        return remote(shard_down.at[1 - core, layer], wide.at[rows], send_wd.at[layer], got_wd.at[layer], partner)

    for q in range(OCTET):
        cols = pl.ds(((q % 2) * RING + q // 2) * COLS, COLS)
        for j in range(UP_ROWS):
            new = adamw_update(master_up[j, :, cols], mom1_up[j, :, cols], mom2_up[j, :, cols], grad_up[j, :, cols] * clip)
            master_up_new[j, :, cols], mom1_up_new[j, :, cols], mom2_up_new[j, :, cols] = new
            shard_up[q, j] = new[0].astype(BF16).astype(F32)

    def w_copy(k):
        to, device = octet[k - 1]
        return remote(shard_up.at[to], shard_recv.at[k], send_w.at[k - 1], got_w.at[k - 1], device)

    for layer in range(LAYERS):
        wd_copy(layer).start()
    for k in range(1, OCTET):
        w_copy(k).start()
    shard_recv[0] = shard_up[mine]
    for layer in range(LAYERS):
        wide[aligned(down_base(layer) + DOWN_ROWS * core, DOWN_ROWS), :] = shard_down[core, layer]
    for k in range(OCTET):
        if k > 0:
            w_copy(k).wait_recv()
    for q in range(OCTET):
        behind = lax.rem(mine + OCTET - q, OCTET)
        for j in range(UP_ROWS):
            for layer in range(LAYERS):
                wide[pl.ds(up_base(layer) + q * UP_ROWS + j, 1), :] = shard_recv[behind, j, pl.ds(layer, 1), :]
    for layer in range(LAYERS):
        rows = aligned(down_base(layer) + DOWN_ROWS * (1 - core), DOWN_ROWS)
        remote(shard_down.at[1 - core, layer], wide.at[rows], send_wd.at[layer], got_wd.at[layer], partner).wait_recv()
    new_block[...] = wide[...].astype(BF16)

    for layer in range(LAYERS):
        down_copy(layer).wait_send()
        wd_copy(layer).wait_send()
    for k in range(1, OCTET):
        up_copy(k).wait_send()
        w_copy(k).wait_send()
    for copy in sent:
        copy.wait_send()


UP_SHAPE = (UP_ROWS, LAYERS, FF)
DOWN_SHAPE = (LAYERS, DOWN_ROWS, WIDTH)


def update_rows(block, *arrays):
    up = jax.ShapeDtypeStruct(UP_SHAPE, F32)
    down = jax.ShapeDtypeStruct(DOWN_SHAPE, F32)
    rows = pltpu.VMEM((OCTET, UP_ROWS, LAYERS, COLS), F32)
    seven, two, norm = SEMS((OCTET - 1,)), SEMS((LAYERS,)), SEMS((N_PEERS,))
    return pl.pallas_call(
        update_kernel,
        out_shape=[jax.ShapeDtypeStruct((ROWS, COLS), BF16), up, down, up, down, up, down],
        in_specs=[in_vmem()] * (1 + len(arrays)),
        out_specs=[in_vmem()] * 7,
        scratch_shapes=[
            rows, rows, pltpu.VMEM((LAYERS, DOWN_ROWS, COLS), F32), pltpu.VMEM(UP_SHAPE, F32), pltpu.VMEM(DOWN_SHAPE, F32),
            pltpu.VMEM((3, CHUNK, LANES), F32), pltpu.VMEM((N_PEERS, CHUNK, LANES), F32), pltpu.VMEM((ROWS, COLS), F32),
            rows, rows, pltpu.VMEM((2, LAYERS, DOWN_ROWS, COLS), F32),
            seven, seven, two, two, norm, norm, seven, seven, two, two,
        ],
        compiler_params=comm_params(3),
        name="update_rows",
    )(block, *arrays)


def keep_kernel(*refs):
    half = len(refs) // 2
    for src, dst in zip(refs[:half], refs[half:]):
        dst[...] = src[...]


def keep(arrays):
    return pl.pallas_call(
        keep_kernel,
        out_shape=[jax.ShapeDtypeStruct(a.shape, a.dtype) for a in arrays],
        in_specs=[in_vmem()] * len(arrays),
        out_specs=[in_vmem()] * len(arrays),
        compiler_params=plain_params(0),
        name="keep",
    )(*arrays)


SWAP = [(i, i ^ 1) for i in range(2 * RING * RING * RING)]


def swap_cores(array):
    return lax.ppermute(array, "fsdp", SWAP)


def rows_first(array):
    return jnp.transpose(array, (1, 0, 2))


def local_step(x_saved, grad_out, x_next, w_up, w_down, gacc_up, gacc_down, master_up, master_down, mom1_up, mom1_down, mom2_up, mom2_down):
    core = jnp.reshape(lax.rem(lax.axis_index("fsdp"), 2), (1,))
    x_tokens = x_saved.reshape(LAYERS, -1, WIDTH)
    grad_last = grad_out.reshape(-1, WIDTH)
    x_last = x_tokens[LAYERS - 1]
    pre_act = jnp.dot(x_last, w_up[LAYERS - 1], preferred_element_type=F32)
    hidden_act, gelu_vjp = jax.vjp(gelu_fn, pre_act)
    act_last = hidden_act.astype(BF16)
    d_act = lax.dot_general(grad_last, w_down[LAYERS - 1], (((1,), (1,)), ((), ())), preferred_element_type=F32)
    d_last = gelu_vjp(d_act)[0].astype(BF16)
    d_sent, x_pair, g_pair = lax.optimization_barrier((d_last, swap_cores(x_last), swap_cores(grad_last)))
    sums = grad_sum(core, act_last, swap_cores(act_last), grad_last, g_pair, None, False)
    sums = grad_sum(core, x_last, x_pair, d_last, swap_cores(d_sent), sums, True)
    block = reduce_blocks(sums.reshape(RING, RING, RING, PAIR_ROWS, COLS), x_tokens[0], grad_last, d_last, w_up, w_down)

    new_block, *state = update_rows(
        block, rows_first(gacc_up), gacc_down, rows_first(master_up), master_down,
        rows_first(mom1_up), mom1_down, rows_first(mom2_up), mom2_down,
    )
    weights, hidden, act = gather_forward(new_block, x_next.reshape(-1, WIDTH))
    weights = weights.reshape(2, RING * RING, RING, N_MATRICES, BLOCK, COLS)
    hidden = last_product(act, weights, hidden)
    master_up, master_down, mom1_up, mom1_down, mom2_up, mom2_down = keep(state)
    return (hidden.reshape(x_next.shape), rows_first(master_up), master_down, rows_first(mom1_up), mom1_down, rows_first(mom2_up), mom2_down)


def solution(mesh):
    rows_spec = P(None, "fsdp")
    return jax.shard_map(local_step, mesh=mesh, in_specs=(rows_spec, P("fsdp"), P("fsdp"), P(), P(), rows_spec, rows_spec, rows_spec, rows_spec, rows_spec, rows_spec, rows_spec, rows_spec), out_specs=(P("fsdp"), rows_spec, rows_spec, rows_spec, rows_spec, rows_spec, rows_spec), check_vma=False)
```

```python
import functools
import math

import jax
import jax.numpy as jnp
from jax import lax
from jax.experimental import pallas as pl
from jax.experimental.pallas import tpu as pltpu
from jax.sharding import PartitionSpec as P

LEARN_RATE = 0.001
BETA_ONE = 0.9
BETA_TWO = 0.95
ADAM_EPS = 1e-8
WEIGHT_DECAY = 0.1
ADAM_STEP = 3
MICRO_STEPS = 2

MESH = pl.DeviceIdType.MESH
BF16 = jnp.bfloat16
F32 = jnp.float32
VMEM_LIMIT = 67_000_000
LAYERS = 2
RING = 4
WIDTH = 1280
FF = 5120
UP_ROWS = 10
DOWN_ROWS = 40
BLOCK = 80
COLS = 640
PAIR_ROWS = 2 * BLOCK
ROWS = LAYERS * PAIR_ROWS
LANES = 128
OCTET = 8
CHUNK = 8
SEMS = pltpu.SemaphoreType.DMA

BATCH_CHUNKS = PAIR_ROWS // CHUNK
ORDERS = ((0, 1, 2), (1, 2, 0), (2, 0, 1))
N_FLOWS = 6
FLOWS = range(N_FLOWS)
TICKS = RING
STEPS = RING - 1
BATCH_LEN = [[TICKS if f // 2 == b else TICKS - 1 for f in FLOWS] for b in range(LAYERS)]
BATCH_START = [[sum(lens[:f]) for f in FLOWS] for lens in BATCH_LEN]
OWN_SLOTS = 2
UP_TILES = 8
TILES = 16
GELU_TICK, SUM_TICK = 2, 6
CARRY_JOBS, GELU_JOBS = 4, 2


def up_base(layer):
    return (LAYERS - 1 - layer) * PAIR_ROWS


def down_base(layer):
    return up_base(layer) + BLOCK


def comm_params(collective_id):
    return pltpu.CompilerParams(collective_id=collective_id, has_side_effects=True, vmem_limit_bytes=VMEM_LIMIT)


def plain_params(dims):
    return pltpu.CompilerParams(dimension_semantics=("arbitrary",) * dims, vmem_limit_bytes=VMEM_LIMIT)


def in_vmem():
    return pl.BlockSpec(memory_space=pltpu.VMEM)


def in_hbm():
    return pl.BlockSpec(memory_space=pl.ANY)


def aligned(start, size):
    return pl.ds(pl.multiple_of(start, CHUNK), size)


def aligned_lanes(start, size):
    return pl.ds(pl.multiple_of(start, LANES), size)


def remote(src, dst, send, got, device):
    return pltpu.make_async_remote_copy(
        src_ref=src, dst_ref=dst, send_sem=send, recv_sem=got, device_id=(device,), device_id_type=MESH
    )

def flow_dims(flow):
    return ORDERS[flow // 2]


def flow_sign(flow):
    return 1 - 2 * (flow % 2)


def my_place():
    me = lax.axis_index("fsdp")
    core, chip = lax.rem(me, 2), lax.div(me, 2)
    line = lax.div(chip, RING)
    return core, (lax.div(line, RING), lax.rem(line, RING), lax.rem(chip, RING))


def device_at(pos, core):
    return ((pos[0] * RING + pos[1]) * RING + pos[2]) * 2 + core


def neighbor(pos, core, dim, sign):
    moved = list(pos)
    moved[dim] = lax.rem(pos[dim] + RING + sign, RING)
    return device_at(moved, core)


def all_neighbors(pos, core):
    return [neighbor(pos, core, dim, sign) for dim in range(3) for sign in (1, -1)]


def entry_barrier(peers):
    barrier = pltpu.get_barrier_semaphore()
    for peer in peers:
        pl.semaphore_signal(barrier, inc=1, device_id=(peer,), device_id_type=MESH)
    pl.semaphore_wait(barrier, len(peers))


def rounded_product(left, right):
    return lax.dot_general(left, right, (((0,), (0,)), ((), ())), preferred_element_type=F32).astype(BF16).astype(F32)


def reduce_kernel(
    s_last, x_own, g_last, d_last, w_up, w_down, out_ref, s_first, x_pair, d_own, d_pair, a_own, a_pair, g_pair,
    recv1, recv2, recv3, own, left, left_pair, right, right_pair, tile, w_tile, w_tile_down, g_own,
    own_sem, tile_in, tile_out, side_send, side_got, act_send, act_got, d_send, d_got, act_out, d_out, credit,
    send1, got1, send2, got2, send3, got3,
):
    core, pos = my_place()
    partner = device_at(pos, 1 - core)
    entry_barrier([partner] + all_neighbors(pos, core))
    target = [[neighbor(pos, core, dim, flow_sign(f)) for dim in flow_dims(f)] for f in FLOWS]
    source = [neighbor(pos, core, flow_dims(f)[0], -flow_sign(f)) for f in FLOWS]
    sums = (s_last, s_first)

    def seg(flow, phase, step):
        at = pos[flow_dims(flow)[phase]]
        return lax.rem(at + 2 * RING - flow_sign(flow) * (1 + step), RING)

    def s_slice(b, flow, j, chunk):
        index = [slice(None)] * 3
        index[flow_dims(flow)[0]] = j
        return sums[b].at[(*index, aligned(chunk * CHUNK, CHUNK), slice(None))]

    def part2(flow, ref, j):
        second, third = flow_dims(flow)[1:]
        return ref.at[j] if second < third else ref.at[:, j]

    def slot1(b, step):
        return step + b * (step // 2)

    def land1(b, step, chunk):
        return recv1.at[slot1(b, step), chunk]

    def land2(b, step, chunk):
        return recv2.at[b, step, chunk]

    def land3(b, step, chunk):
        return recv3.at[b, step, chunk]

    lands, sends, gots = (land1, land2, land3), (send1, send2, send3), (got1, got2, got3)

    def copy(phase, b, flow, step, chunk, src):
        dst = lands[phase](b, step, chunk)
        return remote(dst if src is None else src, dst, sends[phase].at[b, step, chunk], gots[phase].at[b, step, chunk], target[flow][phase])

    def first_copy(phase, b, flow, chunk):
        j = seg(flow, phase, 0)
        if phase == 0:
            src = s_slice(b, flow, j, chunk)
        elif phase == 1:
            src = part2(flow, land1(b, STEPS - 1, chunk), j)
        else:
            src = recv2.at[b, STEPS - 1, chunk, j]
        return copy(phase, b, flow, 0, chunk, src)

    def next_copy(phase, b, flow, step, chunk):
        return copy(phase, b, flow, step + 1, chunk, lands[phase](b, step, chunk))

    def own_copy(b, flow, n):
        step, k = lax.div(n, TICKS), lax.rem(n, TICKS)
        slot = lax.rem(n, OWN_SLOTS)
        src = s_slice(b, flow, seg(flow, 0, step + 1), BATCH_START[b][flow] + k)
        return pltpu.make_async_copy(src, own.at[flow, slot], own_sem.at[flow, slot])

    def start_batch(b):
        for k in range(TICKS):
            for f in FLOWS:
                if k < BATCH_LEN[b][f]:
                    first_copy(0, b, f, BATCH_START[b][f] + k).start()
        for n in range(OWN_SLOTS - 1):
            for f in FLOWS:
                own_copy(b, f, n).start()

    def tick(phase, b, n):
        step, k = lax.div(n, TICKS), lax.rem(n, TICKS)

        def each(body):
            for f in FLOWS:
                if BATCH_LEN[b][f] == TICKS:
                    body(f, BATCH_START[b][f] + k)
                else:
                    pl.when(k < BATCH_LEN[b][f])(functools.partial(body, f, BATCH_START[b][f] + k))

        def add(f, chunk):
            copy(phase, b, f, step, chunk, None).wait_recv()
            landed = lands[phase](b, step, chunk)
            if phase == 0:
                own_copy(b, f, n).wait()
                landed[...] = landed[...] + own[f, lax.rem(n, OWN_SLOTS)]
            elif phase == 1:
                landed[...] = landed[...] + part2(f, land1(b, STEPS - 1, chunk), seg(f, 1, step + 1))[...]
            else:
                landed[...] = landed[...] + recv2[b, STEPS - 1, chunk, seg(f, 2, step + 1)]

        def pass_on(f, chunk):
            @pl.when(step < STEPS - 1)
            def _():
                next_copy(phase, b, f, step, chunk).start()

            @pl.when(step == STEPS - 1)
            def _():
                if phase < 2:
                    first_copy(phase + 1, b, f, chunk).start()
                else:
                    out_ref[aligned((b * BATCH_CHUNKS + chunk) * CHUNK, CHUNK), :] = recv3[b, STEPS - 1, chunk]

        if phase == 0:
            later = n + OWN_SLOTS - 1
            for f in FLOWS:
                @pl.when((later < STEPS * TICKS) & (lax.rem(later, TICKS) < BATCH_LEN[b][f]))
                def _():
                    own_copy(b, f, later).start()

        each(add)
        each(pass_on)

    tokens = x_own.shape[0]
    other = 1 - core

    def back_reads(job, early):
        slot = lax.rem(job, 2)
        if early:
            cols = aligned_lanes(job * COLS, COLS)
            reads = ((w_up.at[LAYERS - 1, :, cols], w_tile), (d_last.at[:, cols], left))
        else:
            cols = aligned_lanes((job - UP_TILES) * COLS, COLS)
            reads = ((w_up.at[0, :, cols], w_tile), (w_down.at[0, cols], w_tile_down))
        return [pltpu.make_async_copy(src, dst.at[slot], tile_in.at[i, slot]) for i, (src, dst) in enumerate(reads)]

    def start_back_reads(job):
        for early in (True, False):
            @pl.when((job < UP_TILES) if early else (job >= UP_TILES) & (job < TILES))
            def _():
                for read in back_reads(job, early):
                    read.start()

    def transposed(lhs, rhs):
        return lax.dot_general(lhs, rhs, (((1,), (1,)), ((), ())), preferred_element_type=F32)

    def carry_gradient(job):
        slot = lax.rem(job, 2)
        start_back_reads(job + 1)
        for read in back_reads(slot, True):
            read.wait()
        for half in range(2):
            at = pl.ds(half * COLS, COLS)
            tile[half, pl.ds(0, tokens)] += transposed(left[slot], w_tile[slot, at])

    def act_copies(i):
        slot, cols = lax.rem(i, 2), aligned_lanes(i * COLS, COLS)
        src = right.at[slot]
        return pltpu.make_async_copy(src, a_own.at[:, cols], act_out.at[slot]), remote(src, a_pair.at[:, cols], act_send.at[slot], act_got.at[i], partner)

    def d_local(i):
        slot = lax.rem(i, 2)
        return pltpu.make_async_copy(right_pair.at[slot], d_own.at[:, aligned_lanes(lax.rem(i, RING) * COLS, COLS)], d_out.at[slot])

    def d_remote(i):
        slot, at = lax.rem(i, 2), lax.rem(i, RING)
        return remote(right_pair.at[slot], d_pair.at[:, aligned_lanes(at * COLS, COLS)], d_send.at[slot], d_got.at[at], partner)

    def wait_back_writes(i):
        own_act, pair_act = act_copies(i)
        own_act.wait()
        pair_act.wait_send()
        mine = lax.div(i, RING) == core

        @pl.when(mine)
        def _():
            d_local(i).wait()

        @pl.when(jnp.logical_not(mine))
        def _():
            d_remote(i).wait_send()

    def through_gelu(i):
        slot = lax.rem(i, 2)
        start_back_reads(i + UP_TILES + 1)
        for read in back_reads(UP_TILES + slot, False):
            read.wait()
        pre_act = jnp.dot(x_own[...], w_tile[slot], preferred_element_type=F32)
        act, gelu_vjp = jax.vjp(gelu_fn, pre_act)
        d_pre = gelu_vjp(transposed(g_own[...], w_tile_down[slot]))[0]

        @pl.when(i >= 2)
        def _():
            wait_back_writes(i - 2)

        right[slot] = act.astype(BF16)
        right_pair[slot] = d_pre.astype(BF16)
        for write in act_copies(i):
            write.start()
        mine = lax.div(i, RING) == core

        @pl.when(mine)
        def _():
            d_local(i).start()

        @pl.when(jnp.logical_not(mine))
        def _():
            d_remote(i).start()

    def tile_reads(job, up):
        slot = lax.rem(job, 2)
        if up:
            rows = aligned_lanes(lax.div(job, RING) * COLS, COLS)
            cols = aligned_lanes(lax.rem(job, RING) * COLS, COLS)
            reads = (x_own.at[:, rows], x_pair.at[:, rows], d_own.at[:, cols], d_pair.at[:, cols])
        else:
            rows = aligned_lanes((job - UP_TILES) * COLS, COLS)
            reads = (a_own.at[:, rows], a_pair.at[:, rows], g_own.at[:, aligned_lanes(core * COLS, COLS)], g_pair)
        return [
            pltpu.make_async_copy(src, dst.at[slot], tile_in.at[i, slot])
            for i, (src, dst) in enumerate(zip(reads, (left, left_pair, right, right_pair)))
        ]

    def start_reads(job):
        for up in (True, False):
            @pl.when((job < UP_TILES) if up else (job >= UP_TILES) & (job < TILES))
            def _():
                for read in tile_reads(job, up):
                    read.start()

    def tile_write(job, up):
        slot = lax.rem(job, 2)
        if up:
            dst = s_first.at[pl.ds(lax.div(job, RING) * 2, 2), :, lax.rem(job, RING), pl.ds(0, BLOCK)]
        else:
            i = job - UP_TILES
            dst = s_first.at[lax.div(i, 2), pl.ds(lax.rem(i, 2) * 2, 2), :, pl.ds(BLOCK, BLOCK)]
        return pltpu.make_async_copy(tile.at[slot].reshape(dst.shape), dst, tile_out.at[slot])

    def compute(job):
        slot = lax.rem(job, 2)
        start_reads(job + 1)
        for read in tile_reads(UP_TILES + slot, False):
            read.wait()

        @pl.when(job >= 2)
        def _():
            tile_write(UP_TILES + slot, False).wait()

        tile[slot] = rounded_product(left[slot], right[slot]) + rounded_product(left_pair[slot], right_pair[slot])
        for up in (True, False):
            @pl.when((job < UP_TILES) if up else (job >= UP_TILES))
            def _():
                tile_write(job, up).start()

    def side_copy(i):
        src, dst = ((x_own, x_pair), (g_own.at[:, aligned_lanes(other * COLS, COLS)], g_pair))[i]
        return remote(src, dst, side_send.at[i], side_got.at[i], partner)

    start_batch(0)
    side_copy(0).start()
    start_back_reads(0)
    for half in range(2):
        tile[half, pl.ds(0, tokens)] = g_last[:, pl.ds(half * COLS, COLS)].astype(F32)

    @pl.loop(0, STEPS * TICKS)
    def _(n):
        tick(0, 0, n)

        @pl.when(n < GELU_TICK)
        def _():
            @pl.loop(0, CARRY_JOBS)
            def _(i):
                carry_gradient(n * CARRY_JOBS + i)

        @pl.when(n == GELU_TICK - 1)
        def _():
            for half in range(2):
                g_own[:, pl.ds(half * COLS, COLS)] = tile[half, pl.ds(0, tokens)].astype(BF16)

        @pl.when((n >= GELU_TICK) & (n < SUM_TICK))
        def _():
            @pl.loop(0, GELU_JOBS)
            def _(i):
                through_gelu((n - GELU_TICK) * GELU_JOBS + i)

        @pl.when(n == GELU_TICK)
        def _():
            side_copy(1).start()

        @pl.when(n == SUM_TICK)
        def _():
            for i in range(2):
                wait_back_writes(UP_TILES - 2 + i)
                side_copy(i).wait_recv()
            for i in range(UP_TILES):
                act_copies(i)[1].wait_recv()
            for i in range(RING):
                d_remote(i).wait_recv()
            start_reads(0)

        @pl.when(n >= SUM_TICK)
        def _():
            compute(n - SUM_TICK)

    for f in FLOWS:
        for k in range(BATCH_LEN[0][f]):
            for step in range(1, STEPS):
                copy(0, 0, f, step, BATCH_START[0][f] + k, None).wait_send()
        pl.semaphore_signal(credit.at[f], inc=1, device_id=(source[f],), device_id_type=MESH)

    done = STEPS * TICKS - SUM_TICK
    ticks_left = (TILES - done) // 2

    @pl.loop(0, ticks_left)
    def _(n):
        tick(1, 0, n)

        @pl.loop(0, 2)
        def _(i):
            compute(done + 2 * n + i)

    for slot in range(2):
        tile_write(UP_TILES + slot, False).wait()
    for f in FLOWS:
        pl.semaphore_wait(credit.at[f], 1)
    start_batch(1)

    @pl.loop(ticks_left, STEPS * TICKS)
    def _(n):
        tick(1, 0, n)

    @pl.loop(0, STEPS * TICKS)
    def _(n):
        tick(0, 1, n)
        tick(2, 0, n)

    @pl.loop(0, STEPS * TICKS)
    def _(n):
        tick(1, 1, n)

    @pl.loop(0, STEPS * TICKS)
    def _(n):
        tick(2, 1, n)

    for i in range(2):
        side_copy(i).wait_send()
    for b in range(LAYERS):
        for f in FLOWS:
            @pl.loop(BATCH_START[b][f], BATCH_START[b][f] + BATCH_LEN[b][f])
            def _(chunk):
                for phase in range(3):
                    for step in range(STEPS):
                        if step == 0 or phase + b:
                            copy(phase, b, f, step, chunk, None).wait_send()


def reduce_blocks(s_last, x_first, g_last, d_last, w_up, w_down):
    tokens = x_first.shape[0]

    def half(width):
        return jax.ShapeDtypeStruct((tokens, width), BF16)

    piece = pltpu.VMEM((2, tokens, COLS), BF16)
    sems = SEMS((LAYERS, STEPS, BATCH_CHUNKS))
    two, tiles = SEMS((2,)), SEMS((UP_TILES,))
    spaces = [half(WIDTH), half(FF // 2), half(FF // 2), half(FF), half(FF), half(COLS)]
    return pl.pallas_call(
        reduce_kernel,
        out_shape=[jax.ShapeDtypeStruct((ROWS, COLS), F32), jax.ShapeDtypeStruct(s_last.shape, F32)] + spaces,
        in_specs=[in_hbm(), in_vmem(), in_vmem(), in_hbm(), in_hbm(), in_hbm()],
        out_specs=[in_vmem(), in_hbm()] + [in_hbm()] * len(spaces),
        scratch_shapes=[
            pltpu.VMEM((RING, BATCH_CHUNKS, RING, RING, CHUNK, COLS), F32),
            pltpu.VMEM((LAYERS, STEPS, BATCH_CHUNKS, RING, CHUNK, COLS), F32),
            pltpu.VMEM((LAYERS, STEPS, BATCH_CHUNKS, CHUNK, COLS), F32),
            pltpu.VMEM((N_FLOWS, OWN_SLOTS, RING, RING, CHUNK, COLS), F32),
            piece, piece, piece, piece,
            pltpu.VMEM((2, COLS, COLS), F32), pltpu.VMEM((2, WIDTH, COLS), BF16), pltpu.VMEM((2, COLS, WIDTH), BF16),
            pltpu.VMEM((tokens, WIDTH), BF16),
            SEMS((N_FLOWS, OWN_SLOTS)), SEMS((RING, 2)), two, two, two, two, tiles, two, SEMS((RING,)), two, two,
            pltpu.SemaphoreType.REGULAR((N_FLOWS,)),
            sems, sems, sems, sems, sems, sems,
        ],
        compiler_params=comm_params(1),
        name="torus_reduce",
    )(s_last, x_first, g_last, d_last, w_up, w_down)[0]


N_MATRICES = 2 * LAYERS
MATRIX_BASE = [base for layer in range(LAYERS) for base in (up_base(layer), down_base(layer))]
SHORT = (2, 1, 0, 2)
MATRIX_LEN = [[CHUNK if f // 2 == SHORT[q] else 2 * CHUNK for f in FLOWS] for q in range(N_MATRICES)]
MATRIX_START = [[MATRIX_BASE[q] + sum(MATRIX_LEN[q][:f]) for f in FLOWS] for q in range(N_MATRICES)]


LINK_ORDER = ((0, 0), (1, 0), (0, 1), (1, 1), (0, 2), (2, 0), (1, 2), (2, 1), (3, 0), (2, 2), (3, 1), (3, 2))
AHEAD = 2


def before(at):
    q, step = LINK_ORDER[at]
    return LINK_ORDER.index((q, step - 1)) if step else -1


GROUP_EVENTS = ((range(0, 6), (0,)), (range(6, 7), ()), (range(7, 8), (1,)), (range(8, 9), ()), (range(9, 11), (2,)), (range(11, 12), ()))
LAST_EVENTS = ()


def gather_kernel(
    block_ref, x_ref, all_ref, hidden_ref, act_ref,
    total, weight, own_sem, load_sem, send1, got1, send2, got2, send3, got3, pair_send, pair_got,
):
    core, pos = my_place()
    partner = device_at(pos, 1 - core)
    entry_barrier([partner] + all_neighbors(pos, core))
    target = [[neighbor(pos, core, dim, flow_sign(f)) for dim in flow_dims(f)] for f in FLOWS]
    pieces = [(q, f) for q in range(N_MATRICES) for f in FLOWS]

    def rows_of(q, flow):
        return pl.ds(MATRIX_START[q][flow], MATRIX_LEN[q][flow])

    def back(flow, phase, steps):
        at = pos[flow_dims(flow)[phase]]
        return lax.rem(at + RING - flow_sign(flow) * steps, RING)

    def place(which, q, flow, *at):
        index = [slice(None)] * 3
        for phase, steps in enumerate(at):
            if steps is not None:
                index[flow_dims(flow)[phase]] = back(flow, phase, steps)
        return all_ref.at[(which, *index, rows_of(q, flow), slice(None))]

    def copy1(q, flow, step, off=0):
        dst = place(core, q, flow, step + off, 0, 0)
        src = dst if off or step else block_ref.at[rows_of(q, flow)]
        return remote(src, dst, send1.at[q, flow, step], got1.at[q, flow, step], target[flow][0])

    def copy2(q, flow, step, off=0):
        ref = place(core, q, flow, None, step + off, 0)
        return remote(ref, ref, send2.at[q, flow, step], got2.at[q, flow, step], target[flow][1])

    def copy3(q, flow, step, off=0):
        ref = place(core, q, flow, None, None, step + off)
        return remote(ref, ref, send3.at[q, flow, step], got3.at[q, flow, step], target[flow][2])

    def pair_copy(q, flow, w, which=core):
        ref = place(which, q, flow, None, None, w)
        return remote(ref, ref, pair_send.at[q, flow, w], pair_got.at[q, flow, w], partner)

    local = pltpu.make_async_copy(block_ref, all_ref.at[core, pos[0], pos[1], pos[2]], own_sem)
    local.start()
    for q, f in pieces:
        copy1(q, f, 0).start()
    local.wait()
    for step in range(STEPS):
        for q, f in pieces:
            copy1(q, f, step, 1).wait_recv()
            if step < STEPS - 1:
                copy1(q, f, step + 1).start()
            else:
                copy2(q, f, 0).start()
    for step in range(STEPS):
        for q, f in pieces:
            copy2(q, f, step, 1).wait_recv()
            if step < STEPS - 1:
                copy2(q, f, step + 1).start()
            elif (q, 0) in LINK_ORDER[:AHEAD]:
                copy3(q, f, 0).start()
    for q, f in pieces:
        pair_copy(q, f, 0).start()

    def arrive(k):
        q, step = LINK_ORDER[k]
        due = [at for at in (k + AHEAD - 1, k + AHEAD) if at < len(LINK_ORDER) and max(at - AHEAD, before(at)) == k]
        for f in FLOWS:
            copy3(q, f, step, 1).wait_recv()
            for at in due:
                copy3(LINK_ORDER[at][0], f, LINK_ORDER[at][1]).start()
        for f in FLOWS:
            pair_copy(q, f, step + 1).start()

    def have_pair(q):
        for f in FLOWS:
            for w in range(RING):
                pair_copy(q, f, w, 1 - core).wait_recv()

    def load(up, layer, i):
        rows = pl.ds(pl.multiple_of(up_base(layer) + (0 if up else BLOCK), CHUNK), BLOCK)
        if up:
            src = all_ref.at[lax.div(i, 2), :, :, pl.ds(lax.rem(i, 2) * 2, 2), rows]
        else:
            src = all_ref.at[:, i, :, :, rows]
        slot = lax.rem(i, 2)
        return pltpu.make_async_copy(src, weight.at[slot].reshape(src.shape), load_sem.at[slot])

    def product(up, i):
        slot = lax.rem(i, 2)
        cols = aligned_lanes(i * WIDTH, WIDTH)
        if up:
            tiles = weight[slot].reshape(RING * RING, 2, BLOCK, COLS)
            wide = jnp.concatenate([tiles[:, x].reshape(WIDTH, COLS) for x in range(2)], axis=1)
            act_ref[:, cols] = gelu_fn(jnp.dot(hidden_ref[...], wide, preferred_element_type=F32)).astype(BF16)
        else:
            tiles = weight[slot].reshape(2, WIDTH, COLS)
            wide = jnp.concatenate([tiles[c] for c in range(2)], axis=1)
            total[...] += jnp.dot(act_ref[:, cols], wide, preferred_element_type=F32)

    hidden_ref[...] = x_ref[...]
    total[...] = x_ref[...].astype(F32)

    @pl.loop(0, len(GROUP_EVENTS))
    def _(group):
        matrix, half = lax.div(group, 2), lax.rem(group, 2)
        layer = lax.div(matrix, 2)
        for g, (events, ready) in enumerate(GROUP_EVENTS):
            @pl.when(group == g)
            def _():
                for k in events:
                    arrive(k)
                for q in ready:
                    have_pair(q)

        for up in (True, False):
            @pl.when((lax.rem(matrix, 2) == 0) == up)
            def _():
                first = half * 2
                load(up, layer, first).start()
                load(up, layer, first + 1).start()

                @pl.loop(first, first + 2)
                def _(i):
                    load(up, layer, i).wait()
                    product(up, i)

                if not up:
                    @pl.when(half == 1)
                    def _():
                        hidden_ref[...] = total[...].astype(BF16)

    for k in LAST_EVENTS:
        arrive(k)
    have_pair(N_MATRICES - 1)
    for q, f in pieces:
        for step in range(STEPS):
            copy1(q, f, step).wait_send()
            copy2(q, f, step).wait_send()
            copy3(q, f, step).wait_send()
        for w in range(RING):
            pair_copy(q, f, w).wait_send()


def gather_forward(block, x_next):
    tokens = x_next.shape[0]
    one = SEMS((N_MATRICES, N_FLOWS, STEPS))
    pair = SEMS((N_MATRICES, N_FLOWS, RING))
    return pl.pallas_call(
        gather_kernel,
        out_shape=[
            jax.ShapeDtypeStruct((2, RING, RING, RING, ROWS, COLS), BF16),
            jax.ShapeDtypeStruct((tokens, WIDTH), BF16),
            jax.ShapeDtypeStruct((tokens, FF), BF16),
        ],
        in_specs=[in_vmem(), in_vmem()],
        out_specs=[in_hbm(), in_vmem(), in_vmem()],
        scratch_shapes=[
            pltpu.VMEM((tokens, WIDTH), F32), pltpu.VMEM((2, 2, RING, RING, BLOCK, COLS), BF16),
            SEMS, SEMS((2,)), one, one, one, one, one, one, pair, pair,
        ],
        compiler_params=comm_params(2),
        name="torus_gather_forward",
    )(block, x_next)


def grad_kernel(core_ref, left, left_pair, right, right_pair, *refs):
    del core_ref
    out = refs[-1]
    total = rounded_product(left[...], right[...]) + rounded_product(left_pair[...], right_pair[...])
    if total.shape[1] == COLS:
        out[...] = total.reshape(out.shape)
    else:
        for x in range(out.shape[1]):
            out[:, x, 0] = total[:, COLS * x:COLS * (x + 1)].reshape(-1, BLOCK, COLS)


def grad_sum(core, left, left_pair, right, right_pair, sums, up):
    tokens = left.shape[0]
    zy = RING * RING
    if up:
        grid = (2, 2)
        left_spec = pl.BlockSpec((tokens, COLS), lambda i, x, c: (0, i))
        right_spec = pl.BlockSpec((tokens, 2 * COLS), lambda i, x, c: (0, c[0] * 2 + x))
        out_spec = pl.BlockSpec((zy // 2, 2, 1, BLOCK, COLS), lambda i, x, c: (i, x, 0, 0, 0))
    else:
        grid = (FF // COLS,)
        left_spec = pl.BlockSpec((tokens, COLS), lambda i, c: (0, i))
        right_spec = pl.BlockSpec((tokens, COLS), lambda i, c: (0, c[0]))
        out_spec = pl.BlockSpec((2, RING, 1, BLOCK, COLS), lambda i, c: (i, 0, 1, 0, 0))
    before = [] if sums is None else [sums]
    return pl.pallas_call(
        grad_kernel,
        out_shape=jax.ShapeDtypeStruct((zy, RING, 2, BLOCK, COLS), F32),
        grid_spec=pltpu.PrefetchScalarGridSpec(
            num_scalar_prefetch=1,
            grid=grid,
            in_specs=[left_spec, left_spec, right_spec, right_spec] + [in_hbm()] * len(before),
            out_specs=out_spec,
        ),
        input_output_aliases={5: 0} if before else {},
        compiler_params=plain_params(len(grid)),
        cost_estimate=pl.CostEstimate(flops=2 * tokens * WIDTH * FF, bytes_accessed=17_000_000, transcendentals=0),
        name="grad_up" if up else "grad_down",
    )(core, left, left_pair, right, right_pair, *before)


def gelu_fn(pre_act):
    return jax.nn.gelu(pre_act, approximate=True)


def down_kernel(act, weight, hidden, out, total):
    step = pl.program_id(0)

    @pl.when(step == 0)
    def _():
        total[...] = hidden[...].astype(F32)

    wide = jnp.concatenate([weight[c].reshape(WIDTH, COLS) for c in range(2)], axis=1)
    total[...] += jnp.dot(act[...], wide, preferred_element_type=F32)

    @pl.when(step == pl.num_programs(0) - 1)
    def _():
        out[...] = total[...].astype(BF16)


def last_product(act, weights, hidden):
    tokens = hidden.shape[0]
    return pl.pallas_call(
        down_kernel,
        out_shape=jax.ShapeDtypeStruct((tokens, WIDTH), BF16),
        grid=(RING,),
        in_specs=[
            pl.BlockSpec((tokens, WIDTH), lambda i: (0, i)),
            pl.BlockSpec((2, RING, RING, 1, BLOCK, COLS), lambda i: (0, i, 0, 1, 0, 0)),
            pl.BlockSpec((tokens, WIDTH), lambda i: (0, 0)),
        ],
        out_specs=pl.BlockSpec((tokens, WIDTH), lambda i: (0, 0)),
        scratch_shapes=[pltpu.VMEM((tokens, WIDTH), F32)],
        compiler_params=plain_params(1),
        name="forward_down",
    )(act, weights, hidden)


def adamw_update(master_old, mom_one, mom_two, grad_clip):
    mom_one_new = BETA_ONE * mom_one + (1.0 - BETA_ONE) * grad_clip
    mom_two_new = BETA_TWO * mom_two + (1.0 - BETA_TWO) * grad_clip * grad_clip
    first_hat = mom_one_new / (1.0 - BETA_ONE ** ADAM_STEP)
    second_hat = mom_two_new / (1.0 - BETA_TWO ** ADAM_STEP)
    master_new = master_old - LEARN_RATE * (first_hat / (jnp.sqrt(second_hat) + ADAM_EPS) + WEIGHT_DECAY * master_old)
    return master_new, mom_one_new, mom_two_new


N_PEERS = OCTET - 1 + 2 * (RING - 1)


def update_kernel(
    block, gacc_up, gacc_down, master_up, master_down, mom1_up, mom1_down, mom2_up, mom2_down,
    new_block, master_up_new, master_down_new, mom1_up_new, mom1_down_new, mom2_up_new, mom2_down_new,
    stage_up, recv_up, recv_down, grad_up, grad_down, norm_send, norm_recv, wide, shard_up, shard_recv, shard_down,
    send_up, got_up, send_down, got_down, send_norm, got_norm, send_w, got_w, send_wd, got_wd,
):
    core, pos = my_place()
    mine = pos[2] * 2 + core
    partner = device_at(pos, 1 - core)
    octet = [(lax.rem(mine + k, OCTET), device_at((pos[0], pos[1], 0), lax.rem(mine + k, OCTET))) for k in range(1, OCTET)]
    along = [[neighbor(pos, core, dim, k) for k in range(1, RING)] for dim in (1, 0)]
    entry_barrier([device for _, device in octet] + along[0] + along[1])

    def down_copy(layer):
        rows = aligned(down_base(layer) + DOWN_ROWS * (1 - core), DOWN_ROWS)
        return remote(block.at[rows], recv_down.at[layer], send_down.at[layer], got_down.at[layer], partner)

    for layer in range(LAYERS):
        down_copy(layer).start()
    for q in range(OCTET):
        for j in range(UP_ROWS):
            for layer in range(LAYERS):
                stage_up[q, j, pl.ds(layer, 1), :] = block[pl.ds(up_base(layer) + q * UP_ROWS + j, 1), :]

    def up_copy(k):
        to, device = octet[k - 1]
        return remote(stage_up.at[to], recv_up.at[k], send_up.at[k - 1], got_up.at[k - 1], device)

    for k in range(1, OCTET):
        up_copy(k).start()
    recv_up[0] = stage_up[mine]

    total = jnp.zeros((CHUNK, LANES), F32)
    for layer in range(LAYERS):
        down_copy(layer).wait_recv()
        for from_me in (True, False):
            cols = aligned_lanes((core if from_me else 1 - core) * COLS, COLS)
            if from_me:
                part = block[aligned(down_base(layer) + DOWN_ROWS * core, DOWN_ROWS), :]
            else:
                part = recv_down[layer]
            grad = (gacc_down[layer, :, cols] + part) / MICRO_STEPS
            grad_down[layer, :, cols] = grad
            square = grad * grad
            for i in range(COLS // LANES):
                for n in range(COLS // LANES):
                    total = total + square[CHUNK * i:CHUNK * i + CHUNK, LANES * n:LANES * n + LANES]
    total_up = jnp.zeros((LAYERS, LANES), F32)
    for k in range(OCTET):
        if k > 0:
            up_copy(k).wait_recv()
        source = lax.rem(mine + OCTET - k, OCTET)
        cols = aligned_lanes((lax.rem(source, 2) * RING + lax.div(source, 2)) * COLS, COLS)
        for j in range(UP_ROWS):
            grad = (gacc_up[j, :, cols] + recv_up[k, j]) / MICRO_STEPS
            grad_up[j, :, cols] = grad
            square = grad * grad
            for n in range(COLS // LANES):
                total_up = total_up + square[:, LANES * n:LANES * n + LANES]
    norm_send[0] = total + jnp.concatenate([total_up, jnp.zeros((CHUNK - LAYERS, LANES), F32)], axis=0)

    slot = 0
    rounds = ([device for _, device in octet], along[0], along[1])
    sent = []
    for r, peers in enumerate(rounds):
        copies = [
            remote(norm_send.at[r], norm_recv.at[slot + k], send_norm.at[slot + k], got_norm.at[slot + k], device)
            for k, device in enumerate(peers)
        ]
        for copy in copies:
            copy.start()
        total = norm_send[r]
        for k, copy in enumerate(copies):
            copy.wait_recv()
            total = total + norm_recv[slot + k]
        slot += len(peers)
        sent += copies
        if r < 2:
            norm_send[r + 1] = total
    norm_sq = jnp.sum(total, keepdims=True)
    clip_norm = 0.1 * math.sqrt(2 * LAYERS * WIDTH * FF)
    clip = jnp.minimum(1.0, clip_norm / jnp.sqrt(norm_sq))

    for layer in range(LAYERS):
        new = adamw_update(master_down[layer], mom1_down[layer], mom2_down[layer], grad_down[layer] * clip)
        master_down_new[layer], mom1_down_new[layer], mom2_down_new[layer] = new
        weight = new[0].astype(BF16).astype(F32)
        for half in range(LAYERS):
            shard_down[half, layer] = weight[:, half * COLS:half * COLS + COLS]

    def wd_copy(layer):
        rows = aligned(down_base(layer) + DOWN_ROWS * core, DOWN_ROWS)
        return remote(shard_down.at[1 - core, layer], wide.at[rows], send_wd.at[layer], got_wd.at[layer], partner)

    for q in range(OCTET):
        cols = pl.ds(((q % 2) * RING + q // 2) * COLS, COLS)
        for j in range(UP_ROWS):
            new = adamw_update(master_up[j, :, cols], mom1_up[j, :, cols], mom2_up[j, :, cols], grad_up[j, :, cols] * clip)
            master_up_new[j, :, cols], mom1_up_new[j, :, cols], mom2_up_new[j, :, cols] = new
            shard_up[q, j] = new[0].astype(BF16).astype(F32)

    def w_copy(k):
        to, device = octet[k - 1]
        return remote(shard_up.at[to], shard_recv.at[k], send_w.at[k - 1], got_w.at[k - 1], device)

    for layer in range(LAYERS):
        wd_copy(layer).start()
    for k in range(1, OCTET):
        w_copy(k).start()
    shard_recv[0] = shard_up[mine]
    for layer in range(LAYERS):
        wide[aligned(down_base(layer) + DOWN_ROWS * core, DOWN_ROWS), :] = shard_down[core, layer]
    for k in range(OCTET):
        if k > 0:
            w_copy(k).wait_recv()
    for q in range(OCTET):
        behind = lax.rem(mine + OCTET - q, OCTET)
        for j in range(UP_ROWS):
            for layer in range(LAYERS):
                wide[pl.ds(up_base(layer) + q * UP_ROWS + j, 1), :] = shard_recv[behind, j, pl.ds(layer, 1), :]
    for layer in range(LAYERS):
        rows = aligned(down_base(layer) + DOWN_ROWS * (1 - core), DOWN_ROWS)
        remote(shard_down.at[1 - core, layer], wide.at[rows], send_wd.at[layer], got_wd.at[layer], partner).wait_recv()
    new_block[...] = wide[...].astype(BF16)

    for layer in range(LAYERS):
        down_copy(layer).wait_send()
        wd_copy(layer).wait_send()
    for k in range(1, OCTET):
        up_copy(k).wait_send()
        w_copy(k).wait_send()
    for copy in sent:
        copy.wait_send()


UP_SHAPE = (UP_ROWS, LAYERS, FF)
DOWN_SHAPE = (LAYERS, DOWN_ROWS, WIDTH)


def update_rows(block, *arrays):
    up = jax.ShapeDtypeStruct(UP_SHAPE, F32)
    down = jax.ShapeDtypeStruct(DOWN_SHAPE, F32)
    rows = pltpu.VMEM((OCTET, UP_ROWS, LAYERS, COLS), F32)
    seven, two, norm = SEMS((OCTET - 1,)), SEMS((LAYERS,)), SEMS((N_PEERS,))
    return pl.pallas_call(
        update_kernel,
        out_shape=[jax.ShapeDtypeStruct((ROWS, COLS), BF16), up, down, up, down, up, down],
        in_specs=[in_vmem()] * (1 + len(arrays)),
        out_specs=[in_vmem()] * 7,
        scratch_shapes=[
            rows, rows, pltpu.VMEM((LAYERS, DOWN_ROWS, COLS), F32), pltpu.VMEM(UP_SHAPE, F32), pltpu.VMEM(DOWN_SHAPE, F32),
            pltpu.VMEM((3, CHUNK, LANES), F32), pltpu.VMEM((N_PEERS, CHUNK, LANES), F32), pltpu.VMEM((ROWS, COLS), F32),
            rows, rows, pltpu.VMEM((2, LAYERS, DOWN_ROWS, COLS), F32),
            seven, seven, two, two, norm, norm, seven, seven, two, two,
        ],
        compiler_params=comm_params(3),
        name="update_rows",
    )(block, *arrays)


def keep_kernel(*refs):
    half = len(refs) // 2
    for src, dst in zip(refs[:half], refs[half:]):
        dst[...] = src[...]


def keep(arrays):
    return pl.pallas_call(
        keep_kernel,
        out_shape=[jax.ShapeDtypeStruct(a.shape, a.dtype) for a in arrays],
        in_specs=[in_vmem()] * len(arrays),
        out_specs=[in_vmem()] * len(arrays),
        compiler_params=plain_params(0),
        name="keep",
    )(*arrays)


SWAP = [(i, i ^ 1) for i in range(2 * RING * RING * RING)]


def swap_cores(array):
    return lax.ppermute(array, "fsdp", SWAP)


def rows_first(array):
    return jnp.transpose(array, (1, 0, 2))


def local_step(x_saved, grad_out, x_next, w_up, w_down, gacc_up, gacc_down, master_up, master_down, mom1_up, mom1_down, mom2_up, mom2_down):
    core = jnp.reshape(lax.rem(lax.axis_index("fsdp"), 2), (1,))
    x_tokens = x_saved.reshape(LAYERS, -1, WIDTH)
    grad_last = grad_out.reshape(-1, WIDTH)
    x_last = x_tokens[LAYERS - 1]
    pre_act = jnp.dot(x_last, w_up[LAYERS - 1], preferred_element_type=F32)
    hidden_act, gelu_vjp = jax.vjp(gelu_fn, pre_act)
    act_last = hidden_act.astype(BF16)
    d_act = lax.dot_general(grad_last, w_down[LAYERS - 1], (((1,), (1,)), ((), ())), preferred_element_type=F32)
    d_last = gelu_vjp(d_act)[0].astype(BF16)
    d_sent, x_pair, g_pair = lax.optimization_barrier((d_last, swap_cores(x_last), swap_cores(grad_last)))
    sums = grad_sum(core, act_last, swap_cores(act_last), grad_last, g_pair, None, False)
    sums = grad_sum(core, x_last, x_pair, d_last, swap_cores(d_sent), sums, True)
    block = reduce_blocks(sums.reshape(RING, RING, RING, PAIR_ROWS, COLS), x_tokens[0], grad_last, d_last, w_up, w_down)

    new_block, *state = update_rows(
        block, rows_first(gacc_up), gacc_down, rows_first(master_up), master_down,
        rows_first(mom1_up), mom1_down, rows_first(mom2_up), mom2_down,
    )
    weights, hidden, act = gather_forward(new_block, x_next.reshape(-1, WIDTH))
    weights = weights.reshape(2, RING * RING, RING, N_MATRICES, BLOCK, COLS)
    hidden = last_product(act, weights, hidden)
    master_up, master_down, mom1_up, mom1_down, mom2_up, mom2_down = keep(state)
    return (hidden.reshape(x_next.shape), rows_first(master_up), master_down, rows_first(mom1_up), mom1_down, rows_first(mom2_up), mom2_down)


def solution(mesh):
    rows_spec = P(None, "fsdp")
    return jax.shard_map(local_step, mesh=mesh, in_specs=(rows_spec, P("fsdp"), P("fsdp"), P(), P(), rows_spec, rows_spec, rows_spec, rows_spec, rows_spec, rows_spec, rows_spec, rows_spec), out_specs=(P("fsdp"), rows_spec, rows_spec, rows_spec, rows_spec, rows_spec, rows_spec), check_vma=False)
```
